64 devices in a mesh: part: 4 (over x, y), dp: 16 (over z, core).
Axes of the slice: x: 2, y: 2, z: 8, core: 2. Of those that a mesh axis runs over, the one named last changes fastest.
The devices are a block of a 4x4x8 slice.
Arguments:
- x: bfloat16 [512, 1024], P(('part', 'dp')), parts along dimension 0
- positions: int32 [512], P(('part', 'dp')), parts along dimension 0
- k_cache: bfloat16 [2, 512, 128, 8, 128], P(None, ('part', 'dp')), parts along dimension 1
- v_cache: bfloat16 [2, 512, 128, 8, 128], P(None, ('part', 'dp')), parts along dimension 1
- attn_norm: bfloat16 [2, 1024], replicated
- w_q: bfloat16 [2, 1024, 2048], P(None, 'dp')
- w_k: bfloat16 [2, 1024, 1024], P(None, 'dp')
- w_v: bfloat16 [2, 1024, 1024], P(None, 'dp')
- q_norm: bfloat16 [2, 128], replicated
- k_norm: bfloat16 [2, 128], replicated
- w_o: bfloat16 [2, 2048, 1024], P(None, 'dp')
- mlp_norm: bfloat16 [2, 1024], replicated
- w_gate: bfloat16 [2, 1024, 3072], P(None, 'dp')
- w_up: bfloat16 [2, 1024, 3072], P(None, 'dp')
- w_down: bfloat16 [2, 3072, 1024], P(None, 'dp')
Outputs:
- output 1: bfloat16 [512, 1024], P(('part', 'dp')), parts along dimension 0
- output 2: bfloat16 [2, 512, 128, 8, 128], P(None, ('part', 'dp')), parts along dimension 1
- output 3: bfloat16 [2, 512, 128, 8, 128], P(None, ('part', 'dp')), parts along dimension 1
There are 4 independent parts. The reference program is written for one: setup_inputs(seed, part) draws one part's arguments, and reference() takes and returns one part's arrays. A program takes and returns all parts, laid end to end along the dimension named above; an argument that names none is the same for every part.
All inputs are finite; a program needn't handle non-finite values.
Results may differ from the reference program's by a relative error of at most 0.0179508.
Values are sent between devices in bfloat16 or wider.
A program may use at most 768 MiB of HBM per device.

```python
import jax
import jax.numpy as jnp
from jax import lax

TOK_DEV = 8
DP_SIZE = 16
CACHE_LEN = 128
D_MODEL = 1024
Q_HEADS = 16
KV_HEADS = 8
FF_DIM = 3072
HEAD_DIM = 128
LAYERS = 2
PART_BATCH = TOK_DEV * DP_SIZE
Q_PER_KV = Q_HEADS // KV_HEADS
RMS_EPS = 1e-6
ROPE_THETA = 1000000.0


def draw_normal(rng_key, shape, std_dev, offset):
    values = offset + std_dev * jax.random.normal(rng_key, shape, jnp.float32)
    return values.astype(jnp.bfloat16)


def setup_inputs(seed: int = 0, part: int = 0) -> dict:
    root_key = jax.random.key(seed)
    shared_keys = jax.random.split(root_key, 11)
    part_keys = jax.random.split(jax.random.fold_in(root_key, part), 4)
    q_width = Q_HEADS * HEAD_DIM
    kv_width = KV_HEADS * HEAD_DIM
    cache_shape = (LAYERS, PART_BATCH, CACHE_LEN, KV_HEADS, HEAD_DIM)
    row_ids = jnp.arange(PART_BATCH)
    positions = jax.random.randint(part_keys[1], (PART_BATCH,), 0, CACHE_LEN, dtype=jnp.int32)
    positions = jnp.where(row_ids == 0, CACHE_LEN - 1, positions)
    positions = jnp.where(row_ids == 1, 0, positions).astype(jnp.int32)
    return {
        "x": draw_normal(part_keys[0], (PART_BATCH, D_MODEL), 1.0, 0.0),
        "positions": positions,
        "k_cache": draw_normal(part_keys[2], cache_shape, 1.0, 0.0),
        "v_cache": draw_normal(part_keys[3], cache_shape, 1.0, 0.0),
        "attn_norm": draw_normal(shared_keys[0], (LAYERS, D_MODEL), 0.3, 1.0),
        "w_q": draw_normal(shared_keys[1], (LAYERS, D_MODEL, q_width), D_MODEL ** -0.5, 0.0),
        "w_k": draw_normal(shared_keys[2], (LAYERS, D_MODEL, kv_width), D_MODEL ** -0.5, 0.0),
        "w_v": draw_normal(shared_keys[3], (LAYERS, D_MODEL, kv_width), D_MODEL ** -0.5, 0.0),
        "q_norm": draw_normal(shared_keys[4], (LAYERS, HEAD_DIM), 0.3, 1.6),
        "k_norm": draw_normal(shared_keys[5], (LAYERS, HEAD_DIM), 1.2, 0.8),
        "w_o": draw_normal(shared_keys[6], (LAYERS, q_width, D_MODEL), q_width ** -0.5, 0.0),
        "mlp_norm": draw_normal(shared_keys[7], (LAYERS, D_MODEL), 0.3, 1.0),
        "w_gate": draw_normal(shared_keys[8], (LAYERS, D_MODEL, FF_DIM), D_MODEL ** -0.5, 0.0),
        "w_up": draw_normal(shared_keys[9], (LAYERS, D_MODEL, FF_DIM), D_MODEL ** -0.5, 0.0),
        "w_down": draw_normal(shared_keys[10], (LAYERS, FF_DIM, D_MODEL), FF_DIM ** -0.5, 0.0),
    }


def rms_norm(values, gain_vec):
    values = values.astype(jnp.float32)
    inv_rms = lax.rsqrt(jnp.mean(values * values, axis=-1, keepdims=True) + RMS_EPS)
    return values * inv_rms * gain_vec.astype(jnp.float32)


def apply_rope(values, positions):
    inv_freq = ROPE_THETA ** (-jnp.arange(0, HEAD_DIM, 2).astype(jnp.float32) / HEAD_DIM)
    angles = positions.astype(jnp.float32)[:, None] * inv_freq[None, :]
    angles = jnp.concatenate([angles, angles], axis=-1)[:, None, :]
    half_dim = HEAD_DIM // 2
    rotated = jnp.concatenate([-values[..., half_dim:], values[..., :half_dim]], axis=-1)
    return values * jnp.cos(angles) + rotated * jnp.sin(angles)


def attend_block(block_args):
    q_blk, k_blk, v_blk, pos_blk = block_args
    scores = jnp.einsum("nkgd,ntkd->nkgt", q_blk.astype(jnp.float32), k_blk.astype(jnp.float32)) * HEAD_DIM ** -0.5
    live_mask = jnp.arange(CACHE_LEN)[None, :] <= pos_blk[:, None]
    scores = jnp.where(live_mask[:, None, None, :], scores, -jnp.inf)
    attn_prob = jax.nn.softmax(scores, axis=-1).astype(jnp.bfloat16)
    attn_mix = jnp.einsum("nkgt,ntkd->nkgd", attn_prob.astype(jnp.float32), v_blk.astype(jnp.float32))
    return attn_mix.astype(jnp.bfloat16)


def decoder_layer(x, layer_args, positions):
    (k_layer, v_layer, attn_norm, w_q, w_k, w_v, q_norm, k_norm, w_o, mlp_norm, w_gate, w_up, w_down) = layer_args
    hidden = rms_norm(x, attn_norm).astype(jnp.bfloat16)
    q_proj = jnp.dot(hidden, w_q, preferred_element_type=jnp.float32).astype(jnp.bfloat16)
    k_proj = jnp.dot(hidden, w_k, preferred_element_type=jnp.float32).astype(jnp.bfloat16)
    v_proj = jnp.dot(hidden, w_v, preferred_element_type=jnp.float32).astype(jnp.bfloat16)
    q_rot = apply_rope(rms_norm(q_proj.reshape(PART_BATCH, Q_HEADS, HEAD_DIM), q_norm), positions).astype(jnp.bfloat16)
    k_rot = apply_rope(rms_norm(k_proj.reshape(PART_BATCH, KV_HEADS, HEAD_DIM), k_norm), positions).astype(jnp.bfloat16)
    v_new = v_proj.reshape(PART_BATCH, KV_HEADS, HEAD_DIM)
    slot_hit = (jnp.arange(CACHE_LEN)[None, :] == positions[:, None])[:, :, None, None]
    k_layer = jnp.where(slot_hit, k_rot[:, None], k_layer)
    v_layer = jnp.where(slot_hit, v_new[:, None], v_layer)
    blocks = (
        q_rot.reshape(DP_SIZE, TOK_DEV, KV_HEADS, Q_PER_KV, HEAD_DIM),
        k_layer.reshape(DP_SIZE, TOK_DEV, CACHE_LEN, KV_HEADS, HEAD_DIM),
        v_layer.reshape(DP_SIZE, TOK_DEV, CACHE_LEN, KV_HEADS, HEAD_DIM),
        positions.reshape(DP_SIZE, TOK_DEV),
    )
    attn_out = lax.map(attend_block, blocks).reshape(PART_BATCH, Q_HEADS * HEAD_DIM)
    x_mid = (x.astype(jnp.float32) + jnp.dot(attn_out, w_o, preferred_element_type=jnp.float32)).astype(jnp.bfloat16)
    hidden2 = rms_norm(x_mid, mlp_norm).astype(jnp.bfloat16)
    gate_val = jnp.dot(hidden2, w_gate, preferred_element_type=jnp.float32)
    up_val = jnp.dot(hidden2, w_up, preferred_element_type=jnp.float32)
    act_in = (jax.nn.silu(gate_val) * up_val).astype(jnp.bfloat16)
    layer_out = (x_mid.astype(jnp.float32) + jnp.dot(act_in, w_down, preferred_element_type=jnp.float32)).astype(jnp.bfloat16)
    return layer_out, (k_layer, v_layer)


def reference(x, positions, k_cache, v_cache, attn_norm, w_q, w_k, w_v, q_norm, k_norm, w_o, mlp_norm, w_gate, w_up, w_down):
    def scan_body(carry_x, layer_args):
        return decoder_layer(carry_x, layer_args, positions)
    y_out, (k_new, v_new) = lax.scan(scan_body, x, (k_cache, v_cache, attn_norm, w_q, w_k, w_v, q_norm, k_norm, w_o, mlp_norm, w_gate, w_up, w_down))
    return (y_out, k_new, v_new)
```

```python
import functools
import math

import jax
import jax.numpy as jnp
from jax import lax
from jax.experimental import pallas as pl
from jax.experimental.pallas import tpu as pltpu
from jax.sharding import PartitionSpec as P

HEAD_DIM = 128
RMS_EPS = 1e-6
ROPE_THETA = 1000000.0
POOL_MAX = 2
MESH = pl.DeviceIdType.MESH
F32 = jnp.float32
BF16 = jnp.bfloat16
NEG = float("-inf")


def rms(values, width):
    return values * lax.rsqrt(jnp.sum(values * values, axis=-1, keepdims=True) * (1.0 / width) + RMS_EPS)


def decode_kernel(cfg, pos_ref, x_ref, an_ref, qn_ref, kn_ref, mn_ref, wq_hbm, wk_hbm, wv_hbm, wo_hbm, wg_hbm, wu_hbm, wd_hbm, kc_hbm, vc_hbm,
                  y_ref, krow_ref, vrow_ref,
                  wqkv, wo, wgu, wd, kc, vc, xg, qkvs, qkvi, og, x1g, pbuf, ybuf, x1f, qs, ks, vs, os_, kro, vro, cs, sn,
                  z_send, z_recv, d_send, d_recv, y_send, y_recv, a_send, a_recv, down_send, down_recv, loc_sem, down_loc):
    layers, zn, pool, tok = cfg["layers"], cfg["zn"], cfg["pool"], cfg["tok"]
    qh, kh = cfg["qh"], cfg["kh"]
    dm = x_ref.shape[1]
    nq = zn * tok
    ctile = dm // zn
    idx = lax.axis_index("dp")
    z, c = idx // 2, idx % 2
    part = lax.axis_index("part")
    yi = part % pool
    mate = part + 1 - 2 * yi
    sib = {"dp": 2 * z + (1 - c)}
    nei = {"part": mate}
    qmine = c * pool + yi
    qother = c * pool + (pool - 1 - yi)

    order = []
    for r in range(zn // 2, 0, -1):
        order.append(r)
        if r != zn - r:
            order.append(zn - r)

    def peer(r):
        return lax.rem(z + r, zn)

    def peer_id(zt):
        return {"dp": 2 * zt + c}

    barrier = pltpu.get_barrier_semaphore()
    for r in order:
        pl.semaphore_signal(barrier, inc=1, device_id=peer_id(peer(r)), device_id_type=MESH)
    pl.semaphore_signal(barrier, inc=1, device_id=sib, device_id_type=MESH)
    if pool == 2:
        pl.semaphore_signal(barrier, inc=1, device_id=nei, device_id_type=MESH)

    def rcopy(src, dst, ss, rs, dev):
        return pltpu.make_async_remote_copy(src_ref=src, dst_ref=dst, send_sem=ss, recv_sem=rs, device_id=dev, device_id_type=MESH)

    def wait_bytes(ref, sem):
        pltpu.make_async_copy(ref, ref, sem).wait()

    groups = {
        "qkv": (wqkv, 0, [(wq_hbm, 0), (wk_hbm, 2 * HEAD_DIM), (wv_hbm, 3 * HEAD_DIM)]),
        "o": (wo, 1, [(wo_hbm, 0)]),
        "gu": (wgu, 2, [(wg_hbm, 0), (wu_hbm, wgu.shape[-1] // 2)]),
    }

    def pieces(l, name, zt):
        buf, gi, srcs = groups[name]
        rows = buf.shape[3]
        out = []
        for src, off in srcs:
            width = src.shape[2] // zn
            s = src.at[l, pl.ds(pl.multiple_of(yi * rows, rows), rows), pl.ds(pl.multiple_of(zt * width, 128), width)]
            d = buf.at[l, z, qmine, :, pl.ds(off, width)]
            out.append((s, d))
        return out, gi

    def w_local(l, name):
        ps, gi = pieces(l, name, z)
        for s, d in ps:
            pltpu.make_async_copy(s, d, loc_sem.at[l, gi]).start()

    def w_send(l, name):
        for r in order:
            zt = peer(r)
            ps, gi = pieces(l, name, zt)
            for s, d in ps:
                rcopy(s, d, z_send.at[l, gi], z_recv.at[l, gi], peer_id(zt)).start()

    def w_fwd1(l, name):
        buf, gi, _ = groups[name]
        wait_bytes(buf.at[l, 0:zn - 1, 0], z_recv.at[l, gi])
        wait_bytes(buf.at[l, 0, 0], loc_sem.at[l, gi])
        q = buf.at[l, :, qmine]
        if pool == 2:
            rcopy(q, q, y_send.at[l, gi], y_recv.at[l, gi], nei).start()
        rcopy(q, q, d_send.at[l, gi, 0], d_recv.at[l, gi, 0], sib).start()

    def w_fwd2(l, name):
        if pool == 2:
            buf, gi, _ = groups[name]
            q = buf.at[l, :, qother]
            wait_bytes(q, y_recv.at[l, gi])
            rcopy(q, q, d_send.at[l, gi, 1], d_recv.at[l, gi, 1], sib).start()

    def w_fin(l, name):
        buf, gi, _ = groups[name]
        wait_bytes(buf.at[l, :, 0], d_recv.at[l, gi, 0])
        if pool == 2:
            wait_bytes(buf.at[l, :, 0], d_recv.at[l, gi, 1])

    def w_drain(l, name):
        buf, gi, _ = groups[name]
        wait_bytes(buf.at[l, 0:zn - 1, 0], z_send.at[l, gi])
        wait_bytes(buf.at[l, :, 0], d_send.at[l, gi, 0])
        if pool == 2:
            wait_bytes(buf.at[l, :, 0], y_send.at[l, gi])
            wait_bytes(buf.at[l, :, 0], d_send.at[l, gi, 1])

    def spread(src_of, dst, l, ph):
        for r in order:
            zt = peer(r)
            rcopy(src_of(zt), dst, a_send.at[l, ph], a_recv.at[l, ph], peer_id(zt)).start()

    def arrived(buf, l, ph):
        wait_bytes(buf.at[l, 0:zn - 1], a_recv.at[l, ph])

    for l in range(layers):
        pltpu.make_async_copy(wd_hbm.at[l], wd.at[l, c], down_loc.at[l, 0]).start()
        for name in ("qkv", "o", "gu"):
            w_local(l, name)
        pltpu.make_async_copy(kc_hbm.at[l], kc.at[l], down_loc.at[l, 1]).start()
        pltpu.make_async_copy(vc_hbm.at[l], vc.at[l], down_loc.at[l, 2]).start()

    xg[0, z] = x_ref[...]

    pl.semaphore_wait(barrier, zn + pool - 1)

    spread(lambda zt: x_ref, xg.at[0, z], 0, 0)
    w_send(0, "qkv")
    for l in range(layers):
        rcopy(wd_hbm.at[l], wd.at[l, c], down_send.at[l], down_recv.at[l], sib).start()

    row_id = lax.broadcasted_iota(jnp.int32, (tok, HEAD_DIM), 0)
    lane_id = lax.broadcasted_iota(jnp.int32, (tok, HEAD_DIM), 1)
    pos = jnp.zeros((tok, HEAD_DIM), jnp.int32)
    for n in range(tok):
        pos = jnp.where(row_id == n, pos_ref[n], pos)
    half = HEAD_DIM // 2
    pair = jnp.where(lane_id >= half, lane_id - half, lane_id).astype(F32)
    inv_freq = jnp.exp(pair * (-2.0 * math.log(ROPE_THETA) / HEAD_DIM))
    ang = pos.astype(F32) * inv_freq
    cs[...] = jnp.cos(ang)
    sin_tab = jnp.sin(ang)
    sn[...] = jnp.where(lane_id >= half, sin_tab, -sin_tab)

    w_send(0, "o")

    def head_norm(v, gain):
        v = rms(v, HEAD_DIM) * gain
        return (v * cs[...] + pltpu.roll(v, half, 1) * sn[...]).astype(BF16).astype(F32)

    def gathered_x(l):
        return xg[l].astype(F32).reshape(nq, dm)

    def attention(l):
        qg = qn_ref[l:l + 1, :].astype(F32)
        kg = kn_ref[l:l + 1, :].astype(F32)
        for h in range(qh):
            v = qkvi[l, h // 2, :, (h % 2) * HEAD_DIM:(h % 2 + 1) * HEAD_DIM].astype(F32)
            qs[pl.ds(h, tok, stride=qh), :] = head_norm(v, qg)
        for h in range(kh):
            k = head_norm(qkvi[l, h, :, 2 * HEAD_DIM:3 * HEAD_DIM].astype(F32), kg)
            v = qkvi[l, h, :, 3 * HEAD_DIM:4 * HEAD_DIM].astype(F32)
            for g in range(2):
                ks[pl.ds(2 * h + g, tok, stride=qh), :] = k
                vs[pl.ds(2 * h + g, tok, stride=qh), :] = v
            kro[pl.ds(h, tok, stride=kh), :] = k
            vro[pl.ds(h, tok, stride=kh), :] = v
        krow_ref[l] = kro[...].astype(BF16)
        vrow_ref[l] = vro[...].astype(BF16)
        cols = kc.shape[2]
        lane = lax.broadcasted_iota(jnp.int32, (qh, cols), 1)
        row = lax.broadcasted_iota(jnp.int32, (qh, cols), 0)
        mine = lax.rem(lane, kh) == lax.shift_right_logical(row, 1)
        slot = jnp.where(mine, lax.div(lane, kh), cols)
        scale = HEAD_DIM ** -0.5
        for n in range(tok):
            q = qs[n * qh:(n + 1) * qh, :]
            s_new = jnp.sum(q * ks[n * qh:(n + 1) * qh, :], axis=-1, keepdims=True) * scale
            s = lax.dot_general(q.astype(BF16), kc[l, n], (((1,), (1,)), ((), ())), preferred_element_type=F32) * scale
            s = jnp.where(slot < pos_ref[n], s, NEG)
            m = jnp.maximum(jnp.max(s, axis=-1, keepdims=True), s_new)
            e = jnp.exp(s - m)
            e_new = jnp.exp(s_new - m)
            den = jnp.sum(e, axis=-1, keepdims=True) + e_new
            p = (e / den).astype(BF16)
            p_new = (e_new / den).astype(BF16).astype(F32)
            o = jnp.dot(p, vc[l, n], preferred_element_type=F32) + p_new * vs[n * qh:(n + 1) * qh, :]
            os_[n * qh:(n + 1) * qh, :] = o
        for h in range(qh):
            og[l, z, :, h * HEAD_DIM:(h + 1) * HEAD_DIM] = os_[pl.ds(h, tok, stride=qh), :].astype(BF16)

    for l in range(layers):
        last = l == layers - 1
        if l == 0:
            w_send(0, "gu")
        arrived(xg, l, 0)
        h = (rms(gathered_x(l), dm) * an_ref[l:l + 1, :].astype(F32)).astype(BF16)
        if l == 0:
            w_fwd1(l, "qkv")
            w_fwd2(l, "qkv")
        w_fin(l, "qkv")
        r = jnp.dot(h, wqkv[l].reshape(dm, wqkv.shape[-1]), preferred_element_type=F32)
        qkvs[l] = r.reshape(zn, tok, wqkv.shape[-1]).astype(BF16)
        qkvi[l, z] = qkvs[l, z]
        spread(lambda zt: qkvs.at[l, zt], qkvi.at[l, z], l, 1)
        w_fwd1(l, "o")
        if l == 0:
            for k in range(layers):
                wait_bytes(kc.at[k], down_loc.at[k, 1])
                wait_bytes(vc.at[k], down_loc.at[k, 2])
        arrived(qkvi, l, 1)
        attention(l)
        spread(lambda zt: og.at[l, z], og.at[l, z], l, 2)
        if not last:
            w_send(l + 1, "qkv")
        w_fwd2(l, "o")
        w_fwd1(l, "gu")
        w_fin(l, "o")
        arrived(og, l, 2)
        o_all = og[l].astype(F32).reshape(nq, og.shape[-1]).astype(BF16)
        r = jnp.dot(o_all, wo[l].reshape(og.shape[-1], ctile), preferred_element_type=F32)
        xc = xg[l, :, :, pl.ds(pl.multiple_of(z * ctile, ctile), ctile)].astype(F32).reshape(nq, ctile)
        x1g[l, z] = (xc + r).astype(BF16)
        spread(lambda zt: x1g.at[l, z], x1g.at[l, z], l, 3)
        if not last:
            w_send(l + 1, "o")
        w_fwd2(l, "gu")
        wait_bytes(wd.at[l, 0], down_loc.at[l, 0])
        wait_bytes(wd.at[l, 0], down_recv.at[l])
        w_fin(l, "gu")
        arrived(x1g, l, 3)
        x1 = jnp.concatenate([x1g[l, zz].astype(F32) for zz in range(zn)], axis=-1)
        x1f[...] = x1
        h2 = (rms(x1, dm) * mn_ref[l:l + 1, :].astype(F32)).astype(BF16)
        gu = jnp.dot(h2, wgu[l].reshape(dm, wgu.shape[-1]), preferred_element_type=F32)
        ffc = wgu.shape[-1] // 2
        g = gu[:, :ffc]
        a = (g * jax.nn.sigmoid(g) * gu[:, ffc:]).astype(BF16)
        pr = jnp.dot(a, wd[l].reshape(ffc, dm), preferred_element_type=F32)
        pbuf[l] = pr.reshape(zn, tok, dm)
        ybuf[l, z] = pbuf[l, z]
        spread(lambda zt: pbuf.at[l, zt], ybuf.at[l, z], l, 4)
        if not last:
            w_send(l + 1, "gu")
            w_fwd1(l + 1, "qkv")
            w_fwd2(l + 1, "qkv")
        arrived(ybuf, l, 4)
        total = ybuf[l, 0]
        for zz in range(1, zn):
            total = total + ybuf[l, zz]
        y = (x1f[pl.ds(pl.multiple_of(z * tok, tok), tok), :] + total).astype(BF16)
        if last:
            y_ref[...] = y
        else:
            xg[l + 1, z] = y
            spread(lambda zt: xg.at[l + 1, z], xg.at[l + 1, z], l + 1, 0)

    for l in range(layers):
        for name in ("qkv", "o", "gu"):
            w_drain(l, name)
        wait_bytes(wd.at[l, 0], down_send.at[l])
        for ph, buf in enumerate((xg, qkvi, og, x1g, ybuf)):
            wait_bytes(buf.at[l, 0:zn - 1], a_send.at[l, ph])


def solution(mesh):
    batch_axes = ("part", "dp")
    act_spec = P(batch_axes, None)
    cache_spec = P(None, batch_axes, None, None, None)
    mat_spec = P(None, "dp", None)
    gain_spec = P(None, None)
    in_specs = (act_spec, P(batch_axes), cache_spec, cache_spec, gain_spec, mat_spec, mat_spec, mat_spec, gain_spec, gain_spec, mat_spec, gain_spec, mat_spec, mat_spec, mat_spec)
    out_specs = (act_spec, cache_spec, cache_spec)
    zn = mesh.shape["dp"] // 2
    pool = POOL_MAX if mesh.shape["part"] % POOL_MAX == 0 else 1

    def device_fn(x, positions, k_cache, v_cache, attn_norm, w_q, w_k, w_v, q_norm, k_norm, w_o, mlp_norm, w_gate, w_up, w_down):
        layers, tok, slots, kh, hd = k_cache.shape
        dm = x.shape[1]
        qw, kw, ff = w_q.shape[2], w_k.shape[2], w_gate.shape[2]
        qh = qw // hd
        nq = 2 * pool
        qkvc = (qw + 2 * kw) // zn
        cfg = dict(layers=layers, zn=zn, pool=pool, tok=tok, qh=qh, kh=kh)
        vm = pl.BlockSpec(memory_space=pltpu.VMEM)
        hb = pl.BlockSpec(memory_space=pl.ANY)
        sm = pl.BlockSpec(memory_space=pltpu.SMEM)
        dma = pltpu.SemaphoreType.DMA
        flat = (layers, tok, slots * kh, hd)
        scratch = [
            pltpu.VMEM((layers, zn, nq, w_q.shape[1] // pool, qkvc), BF16),
            pltpu.VMEM((layers, zn, nq, w_o.shape[1] // pool, dm // zn), BF16),
            pltpu.VMEM((layers, zn, nq, w_gate.shape[1] // pool, 2 * ff // zn), BF16),
            pltpu.VMEM((layers, 2, w_down.shape[1], dm), BF16),
            pltpu.VMEM(flat, BF16),
            pltpu.VMEM(flat, BF16),
            pltpu.VMEM((layers, zn, tok, dm), BF16),
            pltpu.VMEM((layers, zn, tok, qkvc), BF16),
            pltpu.VMEM((layers, zn, tok, qkvc), BF16),
            pltpu.VMEM((layers, zn, tok, qw), BF16),
            pltpu.VMEM((layers, zn, zn * tok, dm // zn), BF16),
            pltpu.VMEM((layers, zn, tok, dm), F32),
            pltpu.VMEM((layers, zn, tok, dm), F32),
            pltpu.VMEM((zn * tok, dm), F32),
            pltpu.VMEM((tok * qh, hd), F32),
            pltpu.VMEM((tok * qh, hd), F32),
            pltpu.VMEM((tok * qh, hd), F32),
            pltpu.VMEM((tok * qh, hd), F32),
            pltpu.VMEM((tok * kh, hd), F32),
            pltpu.VMEM((tok * kh, hd), F32),
            pltpu.VMEM((tok, hd), F32),
            pltpu.VMEM((tok, hd), F32),
            dma((layers, 3)), dma((layers, 3)), dma((layers, 3, 2)), dma((layers, 3, 2)), dma((layers, 3)), dma((layers, 3)),
            dma((layers, 5)), dma((layers, 5)), dma((layers,)), dma((layers,)), dma((layers, 3)), dma((layers, 3)),
        ]
        y, krow, vrow = pl.pallas_call(
            functools.partial(decode_kernel, cfg),
            name="decode",
            out_shape=(jax.ShapeDtypeStruct((tok, dm), BF16), jax.ShapeDtypeStruct((layers, tok * kh, hd), BF16), jax.ShapeDtypeStruct((layers, tok * kh, hd), BF16)),
            in_specs=[sm, vm, vm, vm, vm, vm] + [hb] * 9,
            out_specs=(vm, vm, vm),
            scratch_shapes=scratch,
            compiler_params=pltpu.CompilerParams(collective_id=0, has_side_effects=True, vmem_limit_bytes=48 * 1024 * 1024),
        )(positions, x, attn_norm, q_norm, k_norm, mlp_norm, w_q, w_k, w_v, w_o, w_gate, w_up, w_down, k_cache.reshape(flat), v_cache.reshape(flat))
        slot_hit = (jnp.arange(slots)[None, :] == positions[:, None])[None, :, :, None, None]
        k_out = jnp.where(slot_hit, krow.reshape(layers, tok, 1, kh, hd), k_cache)
        v_out = jnp.where(slot_hit, vrow.reshape(layers, tok, 1, kh, hd), v_cache)
        return y, k_out, v_out

    return jax.shard_map(device_fn, mesh=mesh, in_specs=in_specs, out_specs=out_specs, check_vma=False)
```

```python
import functools
import math

import jax
import jax.numpy as jnp
from jax import lax
from jax.experimental import pallas as pl
from jax.experimental.pallas import tpu as pltpu
from jax.sharding import PartitionSpec as P

HEAD_DIM = 128
RMS_EPS = 1e-6
ROPE_THETA = 1000000.0
POOL_MAX = 2
VMEM_LIMIT = 67043328
MESH = pl.DeviceIdType.MESH
F32 = jnp.float32
BF16 = jnp.bfloat16
NEG = float("-inf")


def rms(values, width):
    return values * lax.rsqrt(jnp.sum(values * values, axis=-1, keepdims=True) * (1.0 / width) + RMS_EPS)


def decode_kernel(cfg, pos_hbm, x_hbm, an_hbm, qn_hbm, kn_hbm, mn_hbm, wq_hbm, wk_hbm, wv_hbm, wo_hbm, wg_hbm, wu_hbm, wd_hbm, kc_hbm, vc_hbm,
                  y_ref, krow_ref, vrow_ref,
                  wqkv, wo, wgu, wd, kc, vc, xg, qkvs, qkvi, og, x1g, pbuf, ybuf, x1f, qs, ks, vs, os_, kro, vro, cs, sn, pos_ref, an_ref, qn_ref, kn_ref, mn_ref,
                  z_send, z_recv, d_send, d_recv, y_send, y_recv, a_send, a_recv, down_send, down_recv, loc_sem, down_loc, in_sem):
    layers, zn, pool, tok = cfg["layers"], cfg["zn"], cfg["pool"], cfg["tok"]
    qh, kh = cfg["qh"], cfg["kh"]
    dm = x_hbm.shape[1]
    nq = zn * tok
    ctile = dm // zn
    idx = lax.axis_index("dp")
    z, c = idx // 2, idx % 2
    part = lax.axis_index("part")
    yi = part % pool
    mate = part + 1 - 2 * yi
    sib = {"dp": 2 * z + (1 - c)}
    nei = {"part": mate}
    qmine = c * pool + yi
    qother = c * pool + (pool - 1 - yi)

    order = []
    for r in range(zn // 2, 0, -1):
        order.append(r)
        if r != zn - r:
            order.append(zn - r)

    def peer(r):
        return lax.rem(z + r, zn)

    def peer_id(zt):
        return {"dp": 2 * zt + c}

    barrier = pltpu.get_barrier_semaphore()
    for r in order:
        pl.semaphore_signal(barrier, inc=1, device_id=peer_id(peer(r)), device_id_type=MESH)
    pl.semaphore_signal(barrier, inc=1, device_id=sib, device_id_type=MESH)
    if pool == 2:
        pl.semaphore_signal(barrier, inc=1, device_id=nei, device_id_type=MESH)

    def rcopy(src, dst, ss, rs, dev):
        return pltpu.make_async_remote_copy(src_ref=src, dst_ref=dst, send_sem=ss, recv_sem=rs, device_id=dev, device_id_type=MESH)

    def wait_bytes(ref, sem):
        pltpu.make_async_copy(ref, ref, sem).wait()

    groups = {
        "qkv": (wqkv, 0, [(wq_hbm, 0), (wk_hbm, 2 * HEAD_DIM), (wv_hbm, 3 * HEAD_DIM)]),
        "o": (wo, 1, [(wo_hbm, 0)]),
        "gu": (wgu, 2, [(wg_hbm, 0), (wu_hbm, wgu.shape[-1] // 2)]),
    }

    def pieces(l, name, zt):
        buf, gi, srcs = groups[name]
        rows = buf.shape[3]
        out = []
        for src, off in srcs:
            width = src.shape[2] // zn
            s = src.at[l, pl.ds(pl.multiple_of(yi * rows, rows), rows), pl.ds(pl.multiple_of(zt * width, 128), width)]
            d = buf.at[l, z, qmine, :, pl.ds(off, width)]
            out.append((s, d))
        return out, gi

    def w_local(l, name):
        ps, gi = pieces(l, name, z)
        for s, d in ps:
            pltpu.make_async_copy(s, d, loc_sem.at[l, gi]).start()

    def w_send(l, name):
        for r in order:
            zt = peer(r)
            ps, gi = pieces(l, name, zt)
            for s, d in ps:
                rcopy(s, d, z_send.at[l, gi], z_recv.at[l, gi], peer_id(zt)).start()

    def w_fwd1(l, name):
        buf, gi, _ = groups[name]
        wait_bytes(buf.at[l, 0:zn - 1, 0], z_recv.at[l, gi])
        wait_bytes(buf.at[l, 0, 0], loc_sem.at[l, gi])
        q = buf.at[l, :, qmine]
        if pool == 2:
            rcopy(q, q, y_send.at[l, gi], y_recv.at[l, gi], nei).start()
        rcopy(q, q, d_send.at[l, gi, 0], d_recv.at[l, gi, 0], sib).start()

    def w_fwd2(l, name):
        if pool == 2:
            buf, gi, _ = groups[name]
            q = buf.at[l, :, qother]
            wait_bytes(q, y_recv.at[l, gi])
            rcopy(q, q, d_send.at[l, gi, 1], d_recv.at[l, gi, 1], sib).start()

    def w_fin(l, name):
        buf, gi, _ = groups[name]
        wait_bytes(buf.at[l, :, 0], d_recv.at[l, gi, 0])
        if pool == 2:
            wait_bytes(buf.at[l, :, 0], d_recv.at[l, gi, 1])

    def w_drain(l, name):
        buf, gi, _ = groups[name]
        wait_bytes(buf.at[l, 0:zn - 1, 0], z_send.at[l, gi])
        wait_bytes(buf.at[l, :, 0], d_send.at[l, gi, 0])
        if pool == 2:
            wait_bytes(buf.at[l, :, 0], y_send.at[l, gi])
            wait_bytes(buf.at[l, :, 0], d_send.at[l, gi, 1])

    def spread(src_of, dst, l, ph):
        for r in order:
            zt = peer(r)
            rcopy(src_of(zt), dst, a_send.at[l, ph], a_recv.at[l, ph], peer_id(zt)).start()

    def arrived(buf, l, ph):
        wait_bytes(buf.at[l, 0:zn - 1], a_recv.at[l, ph])

    smalls = [(x_hbm, xg.at[0, z]), (pos_hbm, pos_ref), (an_hbm, an_ref), (qn_hbm, qn_ref), (kn_hbm, kn_ref), (mn_hbm, mn_ref)]
    small_copies = [pltpu.make_async_copy(s, d, in_sem.at[i]) for i, (s, d) in enumerate(smalls)]
    for cp in small_copies:
        cp.start()
    for l in range(layers):
        pltpu.make_async_copy(wd_hbm.at[l], wd.at[l, c], down_loc.at[l, 0]).start()
        for name in ("qkv", "o", "gu"):
            w_local(l, name)
        pltpu.make_async_copy(kc_hbm.at[l], kc.at[l], down_loc.at[l, 1]).start()
        pltpu.make_async_copy(vc_hbm.at[l], vc.at[l], down_loc.at[l, 2]).start()

    pl.semaphore_wait(barrier, zn + pool - 1)

    small_copies[0].wait()
    spread(lambda zt: xg.at[0, z], xg.at[0, z], 0, 0)
    w_send(0, "qkv")
    for l in range(layers):
        rcopy(wd_hbm.at[l], wd.at[l, c], down_send.at[l], down_recv.at[l], sib).start()

    for cp in small_copies[1:]:
        cp.wait()
    row_id = lax.broadcasted_iota(jnp.int32, (tok, HEAD_DIM), 0)
    lane_id = lax.broadcasted_iota(jnp.int32, (tok, HEAD_DIM), 1)
    pos = jnp.zeros((tok, HEAD_DIM), jnp.int32)
    for n in range(tok):
        pos = jnp.where(row_id == n, pos_ref[n], pos)
    half = HEAD_DIM // 2
    pair = jnp.where(lane_id >= half, lane_id - half, lane_id).astype(F32)
    inv_freq = jnp.exp(pair * (-2.0 * math.log(ROPE_THETA) / HEAD_DIM))
    ang = pos.astype(F32) * inv_freq
    cs[...] = jnp.cos(ang)
    sin_tab = jnp.sin(ang)
    sn[...] = jnp.where(lane_id >= half, sin_tab, -sin_tab)

    w_send(0, "o")

    def head_norm(v, gain):
        v = rms(v, HEAD_DIM) * gain
        return (v * cs[...] + pltpu.roll(v, half, 1) * sn[...]).astype(BF16).astype(F32)

    def gathered_x(l):
        return xg[l].astype(F32).reshape(nq, dm)

    def attention(l):
        qg = qn_ref[l:l + 1, :].astype(F32)
        kg = kn_ref[l:l + 1, :].astype(F32)
        for h in range(qh):
            v = qkvi[l, h // 2, :, (h % 2) * HEAD_DIM:(h % 2 + 1) * HEAD_DIM].astype(F32)
            qs[pl.ds(h, tok, stride=qh), :] = head_norm(v, qg)
        for h in range(kh):
            k = head_norm(qkvi[l, h, :, 2 * HEAD_DIM:3 * HEAD_DIM].astype(F32), kg)
            v = qkvi[l, h, :, 3 * HEAD_DIM:4 * HEAD_DIM].astype(F32)
            for g in range(2):
                ks[pl.ds(2 * h + g, tok, stride=qh), :] = k
                vs[pl.ds(2 * h + g, tok, stride=qh), :] = v
            kro[pl.ds(h, tok, stride=kh), :] = k
            vro[pl.ds(h, tok, stride=kh), :] = v
        krow_ref[l] = kro[...].astype(BF16)
        vrow_ref[l] = vro[...].astype(BF16)
        cols = kc.shape[2]
        lane = lax.broadcasted_iota(jnp.int32, (qh, cols), 1)
        row = lax.broadcasted_iota(jnp.int32, (qh, cols), 0)
        mine = lax.rem(lane, kh) == lax.shift_right_logical(row, 1)
        slot = jnp.where(mine, lax.div(lane, kh), cols)
        scale = HEAD_DIM ** -0.5
        for n in range(tok):
            q = qs[n * qh:(n + 1) * qh, :]
            s_new = jnp.sum(q * ks[n * qh:(n + 1) * qh, :], axis=-1, keepdims=True) * scale
            s = lax.dot_general(q.astype(BF16), kc[l, n], (((1,), (1,)), ((), ())), preferred_element_type=F32) * scale
            s = jnp.where(slot < pos_ref[n], s, NEG)
            m = jnp.maximum(jnp.max(s, axis=-1, keepdims=True), s_new)
            e = jnp.exp(s - m)
            e_new = jnp.exp(s_new - m)
            den = jnp.sum(e, axis=-1, keepdims=True) + e_new
            p = (e / den).astype(BF16)
            p_new = (e_new / den).astype(BF16).astype(F32)
            o = jnp.dot(p, vc[l, n], preferred_element_type=F32) + p_new * vs[n * qh:(n + 1) * qh, :]
            os_[n * qh:(n + 1) * qh, :] = o
        for h in range(qh):
            og[l, z, :, h * HEAD_DIM:(h + 1) * HEAD_DIM] = os_[pl.ds(h, tok, stride=qh), :].astype(BF16)

    for l in range(layers):
        last = l == layers - 1
        if l == 0:
            w_send(0, "gu")
        arrived(xg, l, 0)
        h = (rms(gathered_x(l), dm) * an_ref[l:l + 1, :].astype(F32)).astype(BF16)
        if l == 0:
            w_fwd1(l, "qkv")
            w_fwd2(l, "qkv")
        w_fin(l, "qkv")
        r = jnp.dot(h, wqkv[l].reshape(dm, wqkv.shape[-1]), preferred_element_type=F32)
        qkvs[l] = r.reshape(zn, tok, wqkv.shape[-1]).astype(BF16)
        qkvi[l, z] = qkvs[l, z]
        spread(lambda zt: qkvs.at[l, zt], qkvi.at[l, z], l, 1)
        w_fwd1(l, "o")
        if l == 0:
            for k in range(layers):
                wait_bytes(kc.at[k], down_loc.at[k, 1])
                wait_bytes(vc.at[k], down_loc.at[k, 2])
        arrived(qkvi, l, 1)
        attention(l)
        spread(lambda zt: og.at[l, z], og.at[l, z], l, 2)
        if not last:
            w_send(l + 1, "qkv")
        w_fwd2(l, "o")
        w_fwd1(l, "gu")
        w_fin(l, "o")
        arrived(og, l, 2)
        o_all = og[l].astype(F32).reshape(nq, og.shape[-1]).astype(BF16)
        r = jnp.dot(o_all, wo[l].reshape(og.shape[-1], ctile), preferred_element_type=F32)
        xc = xg[l, :, :, pl.ds(pl.multiple_of(z * ctile, ctile), ctile)].astype(F32).reshape(nq, ctile)
        x1g[l, z] = (xc + r).astype(BF16)
        spread(lambda zt: x1g.at[l, z], x1g.at[l, z], l, 3)
        if not last:
            w_send(l + 1, "o")
        w_fwd2(l, "gu")
        wait_bytes(wd.at[l, 0], down_loc.at[l, 0])
        wait_bytes(wd.at[l, 0], down_recv.at[l])
        w_fin(l, "gu")
        arrived(x1g, l, 3)
        x1 = jnp.concatenate([x1g[l, zz].astype(F32) for zz in range(zn)], axis=-1)
        x1f[...] = x1
        h2 = (rms(x1, dm) * mn_ref[l:l + 1, :].astype(F32)).astype(BF16)
        gu = jnp.dot(h2, wgu[l].reshape(dm, wgu.shape[-1]), preferred_element_type=F32)
        ffc = wgu.shape[-1] // 2
        g = gu[:, :ffc]
        a = (g * jax.nn.sigmoid(g) * gu[:, ffc:]).astype(BF16)
        pr = jnp.dot(a, wd[l].reshape(ffc, dm), preferred_element_type=F32)
        pbuf[l] = pr.reshape(zn, tok, dm)
        ybuf[l, z] = pbuf[l, z]
        spread(lambda zt: pbuf.at[l, zt], ybuf.at[l, z], l, 4)
        if not last:
            w_send(l + 1, "gu")
            w_fwd1(l + 1, "qkv")
            w_fwd2(l + 1, "qkv")
        arrived(ybuf, l, 4)
        total = ybuf[l, 0]
        for zz in range(1, zn):
            total = total + ybuf[l, zz]
        y = (x1f[pl.ds(pl.multiple_of(z * tok, tok), tok), :] + total).astype(BF16)
        if last:
            y_ref[...] = y
        else:
            xg[l + 1, z] = y
            spread(lambda zt: xg.at[l + 1, z], xg.at[l + 1, z], l + 1, 0)

    for l in range(layers):
        for name in ("qkv", "o", "gu"):
            w_drain(l, name)
        wait_bytes(wd.at[l, 0], down_send.at[l])
        for ph, buf in enumerate((xg, qkvi, og, x1g, ybuf)):
            wait_bytes(buf.at[l, 0:zn - 1], a_send.at[l, ph])


def solution(mesh):
    batch_axes = ("part", "dp")
    act_spec = P(batch_axes, None)
    cache_spec = P(None, batch_axes, None, None, None)
    mat_spec = P(None, "dp", None)
    gain_spec = P(None, None)
    in_specs = (act_spec, P(batch_axes), cache_spec, cache_spec, gain_spec, mat_spec, mat_spec, mat_spec, gain_spec, gain_spec, mat_spec, gain_spec, mat_spec, mat_spec, mat_spec)
    out_specs = (act_spec, cache_spec, cache_spec)
    zn = mesh.shape["dp"] // 2
    pool = POOL_MAX if mesh.shape["part"] % POOL_MAX == 0 else 1

    def device_fn(x, positions, k_cache, v_cache, attn_norm, w_q, w_k, w_v, q_norm, k_norm, w_o, mlp_norm, w_gate, w_up, w_down):
        layers, tok, slots, kh, hd = k_cache.shape
        dm = x.shape[1]
        qw, kw, ff = w_q.shape[2], w_k.shape[2], w_gate.shape[2]
        qh = qw // hd
        nq = 2 * pool
        qkvc = (qw + 2 * kw) // zn
        cfg = dict(layers=layers, zn=zn, pool=pool, tok=tok, qh=qh, kh=kh)
        vm = pl.BlockSpec(memory_space=pltpu.VMEM)
        hb = pl.BlockSpec(memory_space=pltpu.HBM)
        dma = pltpu.SemaphoreType.DMA
        flat = (layers, tok, slots * kh, hd)
        scratch = [
            pltpu.VMEM((layers, zn, nq, w_q.shape[1] // pool, qkvc), BF16),
            pltpu.VMEM((layers, zn, nq, w_o.shape[1] // pool, dm // zn), BF16),
            pltpu.VMEM((layers, zn, nq, w_gate.shape[1] // pool, 2 * ff // zn), BF16),
            pltpu.VMEM((layers, 2, w_down.shape[1], dm), BF16),
            pltpu.VMEM(flat, BF16),
            pltpu.VMEM(flat, BF16),
            pltpu.VMEM((layers, zn, tok, dm), BF16),
            pltpu.VMEM((layers, zn, tok, qkvc), BF16),
            pltpu.VMEM((layers, zn, tok, qkvc), BF16),
            pltpu.VMEM((layers, zn, tok, qw), BF16),
            pltpu.VMEM((layers, zn, zn * tok, dm // zn), BF16),
            pltpu.VMEM((layers, zn, tok, dm), F32),
            pltpu.VMEM((layers, zn, tok, dm), F32),
            pltpu.VMEM((zn * tok, dm), F32),
            pltpu.VMEM((tok * qh, hd), F32),
            pltpu.VMEM((tok * qh, hd), F32),
            pltpu.VMEM((tok * qh, hd), F32),
            pltpu.VMEM((tok * qh, hd), F32),
            pltpu.VMEM((tok * kh, hd), F32),
            pltpu.VMEM((tok * kh, hd), F32),
            pltpu.VMEM((tok, hd), F32),
            pltpu.VMEM((tok, hd), F32),
            pltpu.SMEM((tok,), jnp.int32),
            pltpu.VMEM((layers, dm), BF16),
            pltpu.VMEM((layers, hd), BF16),
            pltpu.VMEM((layers, hd), BF16),
            pltpu.VMEM((layers, dm), BF16),
            dma((layers, 3)), dma((layers, 3)), dma((layers, 3, 2)), dma((layers, 3, 2)), dma((layers, 3)), dma((layers, 3)),
            dma((layers, 5)), dma((layers, 5)), dma((layers,)), dma((layers,)), dma((layers, 3)), dma((layers, 3)), dma((6,)),
        ]
        y, krow, vrow = pl.pallas_call(
            functools.partial(decode_kernel, cfg),
            name="decode",
            out_shape=(jax.ShapeDtypeStruct((tok, dm), BF16), jax.ShapeDtypeStruct((layers, tok * kh, hd), BF16), jax.ShapeDtypeStruct((layers, tok * kh, hd), BF16)),
            in_specs=[hb] * 15,
            out_specs=(vm, vm, vm),
            scratch_shapes=scratch,
            compiler_params=pltpu.CompilerParams(collective_id=0, has_side_effects=True, vmem_limit_bytes=VMEM_LIMIT),
        )(positions, x, attn_norm, q_norm, k_norm, mlp_norm, w_q, w_k, w_v, w_o, w_gate, w_up, w_down, k_cache.reshape(flat), v_cache.reshape(flat))
        slot_hit = (jnp.arange(slots)[None, :] == positions[:, None])[None, :, :, None, None]
        k_out = jnp.where(slot_hit, krow.reshape(layers, tok, 1, kh, hd), k_cache)
        v_out = jnp.where(slot_hit, vrow.reshape(layers, tok, 1, kh, hd), v_cache)
        return y, k_out, v_out

    return jax.shard_map(device_fn, mesh=mesh, in_specs=in_specs, out_specs=out_specs, check_vma=False)
```

```python
import functools
import math

import jax
import jax.numpy as jnp
from jax import lax
from jax.experimental import pallas as pl
from jax.experimental.pallas import tpu as pltpu
from jax.sharding import PartitionSpec as P

HEAD_DIM = 128
RMS_EPS = 1e-6
ROPE_THETA = 1000000.0
VMEM_LIMIT = 58400000
MESH = pl.DeviceIdType.MESH
F32 = jnp.float32
BF16 = jnp.bfloat16
NEG = float("-inf")


def rms(values, width):
    return values * lax.rsqrt(jnp.sum(values * values, axis=-1, keepdims=True) * (1.0 / width) + RMS_EPS)


def decode_kernel(cfg, pos_hbm, x_hbm, an_hbm, qn_hbm, kn_hbm, mn_hbm, wq_hbm, wk_hbm, wv_hbm, wo_hbm, wg_hbm, wu_hbm, wd_hbm, kc_hbm, vc_hbm,
                  y_ref, krow_ref, vrow_ref,
                  wqkv, wo, wgu, wd, kc, vc, xg, qkvs, qkvi, og, x1g, pbuf, ybuf, x1f, qs, ks, vs, os_, kro, vro, cs, sn, pos_ref, an_ref, qn_ref, kn_ref, mn_ref,
                  z_send, z_recv, d_send, d_recv, p_send, p_recv, a_send, a_recv, down_send, down_recv, loc_sem, down_loc, in_sem):
    layers, zn, pool, tok = cfg["layers"], cfg["zn"], cfg["pool"], cfg["tok"]
    qh, kh, ny = cfg["qh"], cfg["kh"], cfg["ny"]
    dm = x_hbm.shape[1]
    nq = zn * tok
    ctile = dm // zn
    zh = zn // 2
    idx = lax.axis_index("dp")
    z, c = idx // 2, idx % 2
    part = lax.axis_index("part")
    sib = {"dp": 2 * z + (1 - c)}
    if pool == 4:
        px, py = (part // ny) % 2, (part % ny) % 2
        xnei = {"part": part + ny * (1 - 2 * px)}
        ynei = {"part": part + 1 - 2 * py}
    else:
        px, py = 0, 0
    quarter = px * 2 + py
    sub = c * pool + quarter
    subx = c * pool + (1 - px) * 2 + py
    suby = c * pool + px * 2 + 1 - py
    subd = c * pool + (1 - px) * 2 + 1 - py

    order = []
    for r in range(zn // 2, 0, -1):
        order.append(r)
        if r != zn - r:
            order.append(zn - r)

    def peer(r):
        return lax.rem(z + r, zn)

    def peer_id(zt):
        return {"dp": 2 * zt + c}

    barrier = pltpu.get_barrier_semaphore()
    for r in order:
        pl.semaphore_signal(barrier, inc=1, device_id=peer_id(peer(r)), device_id_type=MESH)
    pl.semaphore_signal(barrier, inc=1, device_id=sib, device_id_type=MESH)
    if pool == 4:
        pl.semaphore_signal(barrier, inc=1, device_id=xnei, device_id_type=MESH)
        pl.semaphore_signal(barrier, inc=1, device_id=ynei, device_id_type=MESH)

    def rcopy(src, dst, ss, rs, dev):
        return pltpu.make_async_remote_copy(src_ref=src, dst_ref=dst, send_sem=ss, recv_sem=rs, device_id=dev, device_id_type=MESH)

    def wait_bytes(ref, sem):
        pltpu.make_async_copy(ref, ref, sem).wait()

    groups = {
        "qkv": (wqkv, 0, [(wq_hbm, 0), (wk_hbm, 2 * HEAD_DIM), (wv_hbm, 3 * HEAD_DIM)]),
        "o": (wo, 1, [(wo_hbm, 0)]),
        "gu": (wgu, 2, [(wg_hbm, 0), (wu_hbm, wgu.shape[-1] // 2)]),
    }

    def pieces(l, name, zt):
        buf, gi, srcs = groups[name]
        rows = buf.shape[3]
        out = []
        for src, off in srcs:
            width = src.shape[2] // zn
            s = src.at[l, pl.ds(pl.multiple_of(quarter * rows, rows), rows), pl.ds(pl.multiple_of(zt * width, 128), width)]
            d = buf.at[l, z, sub, :, pl.ds(off, width)]
            out.append((s, d))
        return out, gi

    def w_local(l, name):
        ps, gi = pieces(l, name, z)
        for s, d in ps:
            pltpu.make_async_copy(s, d, loc_sem.at[l, gi]).start()

    def w_send(l, name):
        for r in order:
            zt = peer(r)
            ps, gi = pieces(l, name, zt)
            for s, d in ps:
                rcopy(s, d, z_send.at[l, gi], z_recv.at[l, gi], peer_id(zt)).start()

    def w_s1(l, name):
        buf, gi, _ = groups[name]
        wait_bytes(buf.at[l, 0:zn - 1, 0], z_recv.at[l, gi])
        wait_bytes(buf.at[l, 0, 0], loc_sem.at[l, gi])
        q = buf.at[l, :, sub]
        if pool == 4:
            rcopy(q, q, p_send.at[l, gi, 0], p_recv.at[l, gi, 0], xnei).start()
            rcopy(q, q, p_send.at[l, gi, 1], p_recv.at[l, gi, 1], ynei).start()
        rcopy(q, q, d_send.at[l, gi, 0], d_recv.at[l, gi, 0], sib).start()

    def w_s2(l, name):
        if pool == 4:
            buf, gi, _ = groups[name]
            qx, qy = buf.at[l, :, subx], buf.at[l, :, suby]
            hx, hy = buf.at[l, 0:zh, subx], buf.at[l, zh:zn, suby]
            wait_bytes(qx, p_recv.at[l, gi, 0])
            rcopy(hx, hx, p_send.at[l, gi, 2], p_recv.at[l, gi, 2], ynei).start()
            rcopy(qx, qx, d_send.at[l, gi, 1], d_recv.at[l, gi, 1], sib).start()
            wait_bytes(qy, p_recv.at[l, gi, 1])
            rcopy(hy, hy, p_send.at[l, gi, 3], p_recv.at[l, gi, 3], xnei).start()
            rcopy(qy, qy, d_send.at[l, gi, 2], d_recv.at[l, gi, 2], sib).start()

    def w_s3(l, name):
        if pool == 4:
            buf, gi, _ = groups[name]
            q = buf.at[l, :, subd]
            wait_bytes(buf.at[l, 0:zh, subd], p_recv.at[l, gi, 2])
            wait_bytes(buf.at[l, zh:zn, subd], p_recv.at[l, gi, 3])
            rcopy(q, q, d_send.at[l, gi, 3], d_recv.at[l, gi, 3], sib).start()

    def w_fin(l, name):
        buf, gi, _ = groups[name]
        for i in range(pool):
            wait_bytes(buf.at[l, :, 0], d_recv.at[l, gi, i])

    def w_drain(l, name):
        buf, gi, _ = groups[name]
        wait_bytes(buf.at[l, 0:zn - 1, 0], z_send.at[l, gi])
        for i in range(pool):
            wait_bytes(buf.at[l, :, 0], d_send.at[l, gi, i])
        if pool == 4:
            for i in range(4):
                wait_bytes(buf.at[l, :, 0] if i < 2 else buf.at[l, 0:zh, 0], p_send.at[l, gi, i])

    def spread(src_of, dst, l, ph):
        for r in order:
            zt = peer(r)
            rcopy(src_of(zt), dst, a_send.at[l, ph], a_recv.at[l, ph], peer_id(zt)).start()

    def arrived(buf, l, ph):
        wait_bytes(buf.at[l, 0:zn - 1], a_recv.at[l, ph])

    plan = {
        (0, "x_sent"): [(w_send, 0, "qkv")],
        (0, "x_in"): [(w_s1, 0, "qkv"), (w_send, 0, "o"), (w_send, 0, "gu"), (w_s2, 0, "qkv"), (w_send, 1, "qkv"), (w_s3, 0, "qkv")],
        (0, "qkv_sent"): [(w_s1, 0, "o")],
        (0, "qkv_in"): [(w_send, 1, "o"), (w_send, 1, "gu"), (w_s1, 0, "gu"), (w_s2, 0, "o")],
        (0, "o_sent"): [(w_s3, 0, "o"), (w_s2, 0, "gu"), (w_s1, 1, "qkv")],
        (0, "x1_sent"): [(w_s3, 0, "gu")],
        (0, "x1_in"): [(w_s2, 1, "qkv")],
        (0, "y_sent"): [(w_s3, 1, "qkv"), (w_s1, 1, "o")],
        (1, "x_sent"): [(w_s2, 1, "o"), (w_s1, 1, "gu")],
        (1, "qkv_sent"): [(w_s3, 1, "o"), (w_s2, 1, "gu")],
        (1, "qkv_in"): [(w_s3, 1, "gu")],
    }

    def background(l, point):
        for fn, wl, name in plan.get((l, point), ()):
            fn(wl, name)

    smalls = [(x_hbm, xg.at[0, z]), (pos_hbm, pos_ref), (an_hbm, an_ref), (qn_hbm, qn_ref), (kn_hbm, kn_ref), (mn_hbm, mn_ref)]
    small_copies = [pltpu.make_async_copy(s, d, in_sem.at[i]) for i, (s, d) in enumerate(smalls)]
    for cp in small_copies:
        cp.start()
    for l in range(layers):
        pltpu.make_async_copy(wd_hbm.at[l], wd.at[l, c], down_loc.at[l, 0]).start()
        for name in ("qkv", "o", "gu"):
            w_local(l, name)
        pltpu.make_async_copy(kc_hbm.at[l], kc.at[l], down_loc.at[l, 1]).start()
        pltpu.make_async_copy(vc_hbm.at[l], vc.at[l], down_loc.at[l, 2]).start()

    pl.semaphore_wait(barrier, zn + (2 if pool == 4 else 0))

    small_copies[0].wait()
    spread(lambda zt: xg.at[0, z], xg.at[0, z], 0, 0)
    background(0, "x_sent")
    for l in range(layers):
        rcopy(wd_hbm.at[l], wd.at[l, c], down_send.at[l], down_recv.at[l], sib).start()

    for cp in small_copies[1:]:
        cp.wait()
    row_id = lax.broadcasted_iota(jnp.int32, (tok, HEAD_DIM), 0)
    lane_id = lax.broadcasted_iota(jnp.int32, (tok, HEAD_DIM), 1)
    pos = jnp.zeros((tok, HEAD_DIM), jnp.int32)
    for n in range(tok):
        pos = jnp.where(row_id == n, pos_ref[n], pos)
    half = HEAD_DIM // 2
    pair = jnp.where(lane_id >= half, lane_id - half, lane_id).astype(F32)
    inv_freq = jnp.exp(pair * (-2.0 * math.log(ROPE_THETA) / HEAD_DIM))
    ang = pos.astype(F32) * inv_freq
    cs[...] = jnp.cos(ang)
    sin_tab = jnp.sin(ang)
    sn[...] = jnp.where(lane_id >= half, sin_tab, -sin_tab)

    def head_norm(v, gain):
        v = rms(v, HEAD_DIM) * gain
        return (v * cs[...] + pltpu.roll(v, half, 1) * sn[...]).astype(BF16).astype(F32)

    def gathered_x(l):
        return xg[l].astype(F32).reshape(nq, dm)

    def attention(l):
        qg = qn_ref[l:l + 1, :].astype(F32)
        kg = kn_ref[l:l + 1, :].astype(F32)
        for h in range(qh):
            v = qkvi[l, h // 2, :, (h % 2) * HEAD_DIM:(h % 2 + 1) * HEAD_DIM].astype(F32)
            qs[pl.ds(h, tok, stride=qh), :] = head_norm(v, qg)
        for h in range(kh):
            k = head_norm(qkvi[l, h, :, 2 * HEAD_DIM:3 * HEAD_DIM].astype(F32), kg)
            v = qkvi[l, h, :, 3 * HEAD_DIM:4 * HEAD_DIM].astype(F32)
            for g in range(2):
                ks[pl.ds(2 * h + g, tok, stride=qh), :] = k
                vs[pl.ds(2 * h + g, tok, stride=qh), :] = v
            kro[pl.ds(h, tok, stride=kh), :] = k
            vro[pl.ds(h, tok, stride=kh), :] = v
        krow_ref[l] = kro[...].astype(BF16)
        vrow_ref[l] = vro[...].astype(BF16)
        cols = kc.shape[2]
        lane = lax.broadcasted_iota(jnp.int32, (qh, cols), 1)
        row = lax.broadcasted_iota(jnp.int32, (qh, cols), 0)
        mine = lax.rem(lane, kh) == lax.shift_right_logical(row, 1)
        slot = jnp.where(mine, lax.div(lane, kh), cols)
        scale = HEAD_DIM ** -0.5
        for n0 in range(0, tok, 4):
            seqs = range(n0, n0 + 4)
            rows = [slice(n * qh, (n + 1) * qh) for n in seqs]
            q = [qs[r, :] for r in rows]
            s = [lax.dot_general(a.astype(BF16), kc[l, n], (((1,), (1,)), ((), ())), preferred_element_type=F32) * scale for a, n in zip(q, seqs)]
            s_new = [jnp.sum(a * ks[r, :], axis=-1, keepdims=True) * scale for a, r in zip(q, rows)]
            s = [jnp.where(slot < pos_ref[n], a, NEG) for a, n in zip(s, seqs)]
            m = [jnp.maximum(jnp.max(a, axis=-1, keepdims=True), b) for a, b in zip(s, s_new)]
            e = [jnp.exp(a - b) for a, b in zip(s, m)]
            e_new = [jnp.exp(a - b) for a, b in zip(s_new, m)]
            inv = [1.0 / (jnp.sum(a, axis=-1, keepdims=True) + b) for a, b in zip(e, e_new)]
            p = [(a * b).astype(BF16) for a, b in zip(e, inv)]
            p_new = [(a * b).astype(BF16).astype(F32) for a, b in zip(e_new, inv)]
            for a, b, r, n in zip(p, p_new, rows, seqs):
                os_[r, :] = jnp.dot(a, vc[l, n], preferred_element_type=F32) + b * vs[r, :]
        for h in range(qh):
            og[l, z, :, h * HEAD_DIM:(h + 1) * HEAD_DIM] = os_[pl.ds(h, tok, stride=qh), :].astype(BF16)

    for l in range(layers):
        last = l == layers - 1
        arrived(xg, l, 0)
        h = (rms(gathered_x(l), dm) * an_ref[l:l + 1, :].astype(F32)).astype(BF16)
        background(l, "x_in")
        w_fin(l, "qkv")
        r = jnp.dot(h, wqkv[l].reshape(dm, wqkv.shape[-1]), preferred_element_type=F32)
        qkvs[l] = r.reshape(zn, tok, wqkv.shape[-1]).astype(BF16)
        spread(lambda zt: qkvs.at[l, zt], qkvi.at[l, z], l, 1)
        qkvi[l, z] = qkvs[l, z]
        background(l, "qkv_sent")
        if l == 0:
            for k in range(layers):
                wait_bytes(kc.at[k], down_loc.at[k, 1])
                wait_bytes(vc.at[k], down_loc.at[k, 2])
        arrived(qkvi, l, 1)
        background(l, "qkv_in")
        attention(l)
        spread(lambda zt: og.at[l, z], og.at[l, z], l, 2)
        background(l, "o_sent")
        w_fin(l, "o")
        arrived(og, l, 2)
        o_all = og[l].astype(F32).reshape(nq, og.shape[-1]).astype(BF16)
        r = jnp.dot(o_all, wo[l].reshape(og.shape[-1], ctile), preferred_element_type=F32)
        xc = xg[l, :, :, pl.ds(pl.multiple_of(z * ctile, ctile), ctile)].astype(F32).reshape(nq, ctile)
        x1g[l, z] = (xc + r).astype(BF16)
        spread(lambda zt: x1g.at[l, z], x1g.at[l, z], l, 3)
        background(l, "x1_sent")
        wait_bytes(wd.at[l, 0], down_loc.at[l, 0])
        wait_bytes(wd.at[l, 0], down_recv.at[l])
        w_fin(l, "gu")
        arrived(x1g, l, 3)
        background(l, "x1_in")
        x1 = jnp.concatenate([x1g[l, zz].astype(F32) for zz in range(zn)], axis=-1)
        x1f[...] = x1
        h2 = (rms(x1, dm) * mn_ref[l:l + 1, :].astype(F32)).astype(BF16)
        gu = jnp.dot(h2, wgu[l].reshape(dm, wgu.shape[-1]), preferred_element_type=F32)
        ffc = wgu.shape[-1] // 2
        g = gu[:, :ffc]
        a = (g * jax.nn.sigmoid(g) * gu[:, ffc:]).astype(BF16)
        pr = jnp.dot(a, wd[l].reshape(ffc, dm), preferred_element_type=F32)
        pbuf[l] = pr.reshape(zn, tok, dm)
        spread(lambda zt: pbuf.at[l, zt], ybuf.at[l, z], l, 4)
        ybuf[l, z] = pbuf[l, z]
        background(l, "y_sent")
        arrived(ybuf, l, 4)
        total = ybuf[l, 0]
        for zz in range(1, zn):
            total = total + ybuf[l, zz]
        y = (x1f[pl.ds(pl.multiple_of(z * tok, tok), tok), :] + total).astype(BF16)
        if last:
            y_ref[...] = y
        else:
            xg[l + 1, z] = y
            spread(lambda zt: xg.at[l + 1, z], xg.at[l + 1, z], l + 1, 0)
            background(l + 1, "x_sent")

    for l in range(layers):
        for name in ("qkv", "o", "gu"):
            w_drain(l, name)
        wait_bytes(wd.at[l, 0], down_send.at[l])
        for ph, buf in enumerate((xg, qkvi, og, x1g, ybuf)):
            wait_bytes(buf.at[l, 0:zn - 1], a_send.at[l, ph])


def solution(mesh):
    batch_axes = ("part", "dp")
    act_spec = P(batch_axes, None)
    cache_spec = P(None, batch_axes, None, None, None)
    mat_spec = P(None, "dp", None)
    gain_spec = P(None, None)
    in_specs = (act_spec, P(batch_axes), cache_spec, cache_spec, gain_spec, mat_spec, mat_spec, mat_spec, gain_spec, gain_spec, mat_spec, gain_spec, mat_spec, mat_spec, mat_spec)
    out_specs = (act_spec, cache_spec, cache_spec)
    zn = mesh.shape["dp"] // 2
    ny = math.isqrt(mesh.shape["part"])
    pool = 4 if ny * ny == mesh.shape["part"] and ny % 2 == 0 else 1

    def device_fn(x, positions, k_cache, v_cache, attn_norm, w_q, w_k, w_v, q_norm, k_norm, w_o, mlp_norm, w_gate, w_up, w_down):
        layers, tok, slots, kh, hd = k_cache.shape
        dm = x.shape[1]
        qw, kw, ff = w_q.shape[2], w_k.shape[2], w_gate.shape[2]
        qh = qw // hd
        nq = 2 * pool
        qkvc = (qw + 2 * kw) // zn
        cfg = dict(layers=layers, zn=zn, pool=pool, ny=ny, tok=tok, qh=qh, kh=kh)
        vm = pl.BlockSpec(memory_space=pltpu.VMEM)
        hb = pl.BlockSpec(memory_space=pltpu.HBM)
        dma = pltpu.SemaphoreType.DMA
        flat = (layers, tok, slots * kh, hd)
        scratch = [
            pltpu.VMEM((layers, zn, nq, w_q.shape[1] // pool, qkvc), BF16),
            pltpu.VMEM((layers, zn, nq, w_o.shape[1] // pool, dm // zn), BF16),
            pltpu.VMEM((layers, zn, nq, w_gate.shape[1] // pool, 2 * ff // zn), BF16),
            pltpu.VMEM((layers, 2, w_down.shape[1], dm), BF16),
            pltpu.VMEM(flat, BF16),
            pltpu.VMEM(flat, BF16),
            pltpu.VMEM((layers, zn, tok, dm), BF16),
            pltpu.VMEM((layers, zn, tok, qkvc), BF16),
            pltpu.VMEM((layers, zn, tok, qkvc), BF16),
            pltpu.VMEM((layers, zn, tok, qw), BF16),
            pltpu.VMEM((layers, zn, zn * tok, dm // zn), BF16),
            pltpu.VMEM((layers, zn, tok, dm), F32),
            pltpu.VMEM((layers, zn, tok, dm), F32),
            pltpu.VMEM((zn * tok, dm), F32),
            pltpu.VMEM((tok * qh, hd), F32),
            pltpu.VMEM((tok * qh, hd), F32),
            pltpu.VMEM((tok * qh, hd), F32),
            pltpu.VMEM((tok * qh, hd), F32),
            pltpu.VMEM((tok * kh, hd), F32),
            pltpu.VMEM((tok * kh, hd), F32),
            pltpu.VMEM((tok, hd), F32),
            pltpu.VMEM((tok, hd), F32),
            pltpu.SMEM((tok,), jnp.int32),
            pltpu.VMEM((layers, dm), BF16),
            pltpu.VMEM((layers, hd), BF16),
            pltpu.VMEM((layers, hd), BF16),
            pltpu.VMEM((layers, dm), BF16),
            dma((layers, 3)), dma((layers, 3)), dma((layers, 3, pool)), dma((layers, 3, pool)), dma((layers, 3, 4)), dma((layers, 3, 4)),
            dma((layers, 5)), dma((layers, 5)), dma((layers,)), dma((layers,)), dma((layers, 3)), dma((layers, 3)), dma((6,)),
        ]
        y, krow, vrow = pl.pallas_call(
            functools.partial(decode_kernel, cfg),
            name="decode",
            out_shape=(jax.ShapeDtypeStruct((tok, dm), BF16), jax.ShapeDtypeStruct((layers, tok * kh, hd), BF16), jax.ShapeDtypeStruct((layers, tok * kh, hd), BF16)),
            in_specs=[hb] * 15,
            out_specs=(vm, vm, vm),
            scratch_shapes=scratch,
            compiler_params=pltpu.CompilerParams(collective_id=0, has_side_effects=True, vmem_limit_bytes=VMEM_LIMIT),
        )(positions, x, attn_norm, q_norm, k_norm, mlp_norm, w_q, w_k, w_v, w_o, w_gate, w_up, w_down, k_cache.reshape(flat), v_cache.reshape(flat))
        slot_hit = (jnp.arange(slots)[None, :] == positions[:, None])[None, :, :, None, None]
        k_out = jnp.where(slot_hit, krow.reshape(layers, tok, 1, kh, hd), k_cache)
        v_out = jnp.where(slot_hit, vrow.reshape(layers, tok, 1, kh, hd), v_cache)
        return y, k_out, v_out

    return jax.shard_map(device_fn, mesh=mesh, in_specs=in_specs, out_specs=out_specs, check_vma=False)
```

```python
import functools
import math

import jax
import jax.numpy as jnp
from jax import lax
from jax.experimental import pallas as pl
from jax.experimental.pallas import tpu as pltpu
from jax.sharding import PartitionSpec as P

HEAD_DIM = 128
RMS_EPS = 1e-6
ROPE_THETA = 1000000.0
VMEM_LIMIT = 58400000
PLACE_LIMIT = 8 * 1024 * 1024
RES_BLOCKS = 4096

MESH = pl.DeviceIdType.MESH
F32 = jnp.float32
BF16 = jnp.bfloat16
NEG = float("-inf")


def rms(values, width):
    return values * lax.rsqrt(jnp.sum(values * values, axis=-1, keepdims=True) * (1.0 / width) + RMS_EPS)


def decode_kernel(cfg, pos_hbm, x_hbm, an_hbm, qn_hbm, kn_hbm, mn_hbm, wq_hbm, wk_hbm, wv_hbm, wo_hbm, wg_hbm, wu_hbm, wd_hbm, kc_hbm, vc_hbm,
                  res_hbm,
                  wq, wkv, wo, wgu, wd, kc, vc, xg, qkvs, qkvi, og, x1g, pbuf, ybuf, x1f, qs, ks, vs, os_, kro, vro, cs, sn, pos_ref, an_ref, qn_ref, kn_ref, mn_ref, y_ref, krow_ref, vrow_ref,
                  z_send, z_recv, d_send, d_recv, p_send, p_recv, a_send, a_recv, down_send, down_recv, loc_sem, down_loc, in_sem, out_sem):
    layers, zn, pool, tok = cfg["layers"], cfg["zn"], cfg["pool"], cfg["tok"]
    qh, kh, ny = cfg["qh"], cfg["kh"], cfg["ny"]
    dm = x_hbm.shape[1]
    nq = zn * tok
    ctile = dm // zn
    zh = zn // 2
    idx = lax.axis_index("dp")
    z, c = idx // 2, idx % 2
    part = lax.axis_index("part")
    sib = {"dp": 2 * z + (1 - c)}
    if pool == 4:
        px, py = (part // ny) % 2, (part % ny) % 2
        xnei = {"part": part + ny * (1 - 2 * px)}
        ynei = {"part": part + 1 - 2 * py}
    else:
        px, py = 0, 0
    quarter = px * 2 + py
    sub = c * pool + quarter
    subx = c * pool + (1 - px) * 2 + py
    suby = c * pool + px * 2 + 1 - py
    subd = c * pool + (1 - px) * 2 + 1 - py

    order = []
    for r in range(zn // 2, 0, -1):
        order.append(r)
        if r != zn - r:
            order.append(zn - r)

    def peer(r):
        return lax.rem(z + r, zn)

    def peer_id(zt):
        return {"dp": 2 * zt + c}

    barrier = pltpu.get_barrier_semaphore()
    for r in order:
        pl.semaphore_signal(barrier, inc=1, device_id=peer_id(peer(r)), device_id_type=MESH)
    pl.semaphore_signal(barrier, inc=1, device_id=sib, device_id_type=MESH)
    if pool == 4:
        pl.semaphore_signal(barrier, inc=1, device_id=xnei, device_id_type=MESH)
        pl.semaphore_signal(barrier, inc=1, device_id=ynei, device_id_type=MESH)

    def rcopy(src, dst, ss, rs, dev):
        return pltpu.make_async_remote_copy(src_ref=src, dst_ref=dst, send_sem=ss, recv_sem=rs, device_id=dev, device_id_type=MESH)

    def wait_bytes(ref, sem):
        pltpu.make_async_copy(ref, ref, sem).wait()

    groups = {
        "q": (wq, 0, [(wq_hbm, 0)]),
        "kv": (wkv, 1, [(wk_hbm, 0), (wv_hbm, wkv.shape[-1] // 2)]),
        "o": (wo, 2, [(wo_hbm, 0)]),
        "gu": (wgu, 3, [(wg_hbm, 0), (wu_hbm, wgu.shape[-1] // 2)]),
    }

    def pieces(l, name, zt):
        buf, gi, srcs = groups[name]
        rows = buf.shape[3]
        out = []
        for src, off in srcs:
            width = src.shape[2] // zn
            s = src.at[l, pl.ds(pl.multiple_of(quarter * rows, rows), rows), pl.ds(pl.multiple_of(zt * width, 128), width)]
            d = buf.at[l, z, sub, :, pl.ds(off, width)]
            out.append((s, d))
        return out, gi

    def w_local(l, name):
        ps, gi = pieces(l, name, z)
        for s, d in ps:
            pltpu.make_async_copy(s, d, loc_sem.at[l, gi]).start()

    def w_send(l, name):
        for r in order:
            zt = peer(r)
            ps, gi = pieces(l, name, zt)
            for s, d in ps:
                rcopy(s, d, z_send.at[l, gi], z_recv.at[l, gi], peer_id(zt)).start()

    def w_s1(l, name):
        buf, gi, _ = groups[name]
        wait_bytes(buf.at[l, 0:zn - 1, 0], z_recv.at[l, gi])
        wait_bytes(buf.at[l, 0, 0], loc_sem.at[l, gi])
        q = buf.at[l, :, sub]
        if pool == 4:
            rcopy(q, q, p_send.at[l, gi, 0], p_recv.at[l, gi, 0], xnei).start()
            rcopy(q, q, p_send.at[l, gi, 1], p_recv.at[l, gi, 1], ynei).start()
        rcopy(q, q, d_send.at[l, gi, 0], d_recv.at[l, gi, 0], sib).start()

    def w_s2(l, name):
        if pool == 4:
            buf, gi, _ = groups[name]
            qx, qy = buf.at[l, :, subx], buf.at[l, :, suby]
            hx, hy = buf.at[l, 0:zh, subx], buf.at[l, zh:zn, suby]
            wait_bytes(qx, p_recv.at[l, gi, 0])
            rcopy(hx, hx, p_send.at[l, gi, 2], p_recv.at[l, gi, 2], ynei).start()
            rcopy(qx, qx, d_send.at[l, gi, 1], d_recv.at[l, gi, 1], sib).start()
            wait_bytes(qy, p_recv.at[l, gi, 1])
            rcopy(hy, hy, p_send.at[l, gi, 3], p_recv.at[l, gi, 3], xnei).start()
            rcopy(qy, qy, d_send.at[l, gi, 2], d_recv.at[l, gi, 2], sib).start()

    def w_s3(l, name):
        if pool == 4:
            buf, gi, _ = groups[name]
            q = buf.at[l, :, subd]
            wait_bytes(buf.at[l, 0:zh, subd], p_recv.at[l, gi, 2])
            wait_bytes(buf.at[l, zh:zn, subd], p_recv.at[l, gi, 3])
            rcopy(q, q, d_send.at[l, gi, 3], d_recv.at[l, gi, 3], sib).start()

    def w_fin(l, name):
        buf, gi, _ = groups[name]
        for i in range(pool):
            wait_bytes(buf.at[l, :, 0], d_recv.at[l, gi, i])

    def w_drain(l, name):
        buf, gi, _ = groups[name]
        wait_bytes(buf.at[l, 0:zn - 1, 0], z_send.at[l, gi])
        for i in range(pool):
            wait_bytes(buf.at[l, :, 0], d_send.at[l, gi, i])
        if pool == 4:
            for i in range(4):
                wait_bytes(buf.at[l, :, 0] if i < 2 else buf.at[l, 0:zh, 0], p_send.at[l, gi, i])

    def spread(src_of, dst, l, ph):
        for r in order:
            zt = peer(r)
            rcopy(src_of(zt), dst, a_send.at[l, ph], a_recv.at[l, ph], peer_id(zt)).start()

    def arrived(buf, l, ph):
        wait_bytes(buf.at[l, 0:zn - 1], a_recv.at[l, ph])

    plan = {
        (0, "entry"): [(w_send, 0, "q"), (w_send, 0, "kv")],
        (0, "x_in"): [(w_s1, 0, "q"), (w_send, 0, "o"), (w_s1, 0, "kv"), (w_send, 0, "gu"), (w_s2, 0, "q"), (w_s2, 0, "kv"), (w_s3, 0, "q"), (w_s3, 0, "kv")],
        (0, "qkv_sent"): [(w_send, 1, "q"), (w_send, 1, "kv"), (w_send, 1, "o"), (w_s1, 0, "o")],
        (0, "qkv_in"): [(w_s1, 0, "gu"), (w_s2, 0, "o")],
        (0, "o_sent"): [(w_s3, 0, "o"), (w_s2, 0, "gu"), (w_s1, 1, "q"), (w_s1, 1, "kv")],
        (0, "x1_sent"): [(w_send, 1, "gu"), (w_s3, 0, "gu")],
        (0, "x1_in"): [(w_s2, 1, "q"), (w_s2, 1, "kv"), (w_s1, 1, "o")],
        (0, "y_sent"): [(w_s3, 1, "q"), (w_s3, 1, "kv"), (w_s2, 1, "o")],
        (1, "x_sent"): [(w_s3, 1, "o"), (w_s1, 1, "gu")],
        (1, "qkv_sent"): [(w_s2, 1, "gu")],
        (1, "o_sent"): [(w_s3, 1, "gu")],
    }

    def background(l, point):
        for fn, wl, name in plan.get((l, point), ()):
            fn(wl, name)

    smalls = [(x_hbm, xg.at[0, z]), (pos_hbm, pos_ref), (an_hbm, an_ref), (qn_hbm, qn_ref), (kn_hbm, kn_ref), (mn_hbm, mn_ref)]
    small_copies = [pltpu.make_async_copy(s, d, in_sem.at[i]) for i, (s, d) in enumerate(smalls)]
    for cp in small_copies:
        cp.start()
    for l in range(layers):
        pltpu.make_async_copy(wd_hbm.at[l], wd.at[l, c], down_loc.at[l, 0]).start()
        for name in groups:
            w_local(l, name)
        pltpu.make_async_copy(kc_hbm.at[l], kc.at[l], down_loc.at[l, 1]).start()
        pltpu.make_async_copy(vc_hbm.at[l], vc.at[l], down_loc.at[l, 2]).start()

    pl.semaphore_wait(barrier, zn + (2 if pool == 4 else 0))

    background(0, "entry")
    small_copies[0].wait()
    spread(lambda zt: xg.at[0, z], xg.at[0, z], 0, 0)
    for l in range(layers):
        rcopy(wd_hbm.at[l], wd.at[l, c], down_send.at[l], down_recv.at[l], sib).start()

    for cp in small_copies[1:]:
        cp.wait()
    row_id = lax.broadcasted_iota(jnp.int32, (tok, HEAD_DIM), 0)
    lane_id = lax.broadcasted_iota(jnp.int32, (tok, HEAD_DIM), 1)
    pos = jnp.zeros((tok, HEAD_DIM), jnp.int32)
    for n in range(tok):
        pos = jnp.where(row_id == n, pos_ref[n], pos)
    half = HEAD_DIM // 2
    pair = jnp.where(lane_id >= half, lane_id - half, lane_id).astype(F32)
    inv_freq = jnp.exp(pair * (-2.0 * math.log(ROPE_THETA) / HEAD_DIM))
    ang = pos.astype(F32) * inv_freq
    cs[...] = jnp.cos(ang)
    sin_tab = jnp.sin(ang)
    sn[...] = jnp.where(lane_id >= half, sin_tab, -sin_tab)

    outs = []

    def head_norm(v, gain):
        v = rms(v, HEAD_DIM) * gain
        return (v * cs[...] + pltpu.roll(v, half, 1) * sn[...]).astype(BF16).astype(F32)

    def gathered_x(l):
        return xg[l].astype(F32).reshape(nq, dm)

    def attention(l):
        qg = qn_ref[l:l + 1, :].astype(F32)
        kg = kn_ref[l:l + 1, :].astype(F32)
        for h in range(qh):
            v = qkvi[l, h // 2, :, (h % 2) * HEAD_DIM:(h % 2 + 1) * HEAD_DIM].astype(F32)
            qs[pl.ds(h, tok, stride=qh), :] = head_norm(v, qg)
        for h in range(kh):
            k = head_norm(qkvi[l, h, :, 2 * HEAD_DIM:3 * HEAD_DIM].astype(F32), kg)
            v = qkvi[l, h, :, 3 * HEAD_DIM:4 * HEAD_DIM].astype(F32)
            for g in range(2):
                ks[pl.ds(2 * h + g, tok, stride=qh), :] = k
                vs[pl.ds(2 * h + g, tok, stride=qh), :] = v
            kro[pl.ds(h, tok, stride=kh), :] = k
            vro[pl.ds(h, tok, stride=kh), :] = v
        krow_ref[l] = kro[...].astype(BF16)
        vrow_ref[l] = vro[...].astype(BF16)
        outs.append(pltpu.make_async_copy(krow_ref.at[l], res_hbm.at[1 + 2 * l], out_sem.at[1 + 2 * l]))
        outs.append(pltpu.make_async_copy(vrow_ref.at[l], res_hbm.at[2 + 2 * l], out_sem.at[2 + 2 * l]))
        outs[-2].start()
        outs[-1].start()
        cols = kc.shape[2]
        lane = lax.broadcasted_iota(jnp.int32, (qh, cols), 1)
        row = lax.broadcasted_iota(jnp.int32, (qh, cols), 0)
        mine = lax.rem(lane, kh) == lax.shift_right_logical(row, 1)
        slot = jnp.where(mine, lax.div(lane, kh), cols)
        scale = HEAD_DIM ** -0.5
        for n0 in range(0, tok, 4):
            seqs = range(n0, n0 + 4)
            rows = [slice(n * qh, (n + 1) * qh) for n in seqs]
            q = [qs[r, :] for r in rows]
            s = [lax.dot_general(a.astype(BF16), kc[l, n], (((1,), (1,)), ((), ())), preferred_element_type=F32) * scale for a, n in zip(q, seqs)]
            s_new = [jnp.sum(a * ks[r, :], axis=-1, keepdims=True) * scale for a, r in zip(q, rows)]
            s = [jnp.where(slot < pos_ref[n], a, NEG) for a, n in zip(s, seqs)]
            m = [jnp.maximum(jnp.max(a, axis=-1, keepdims=True), b) for a, b in zip(s, s_new)]
            e = [jnp.exp(a - b) for a, b in zip(s, m)]
            e_new = [jnp.exp(a - b) for a, b in zip(s_new, m)]
            inv = [1.0 / (jnp.sum(a, axis=-1, keepdims=True) + b) for a, b in zip(e, e_new)]
            p = [(a * b).astype(BF16) for a, b in zip(e, inv)]
            p_new = [(a * b).astype(BF16).astype(F32) for a, b in zip(e_new, inv)]
            for a, b, r, n in zip(p, p_new, rows, seqs):
                os_[r, :] = jnp.dot(a, vc[l, n], preferred_element_type=F32) + b * vs[r, :]
        for h in range(qh):
            og[l, z, :, h * HEAD_DIM:(h + 1) * HEAD_DIM] = os_[pl.ds(h, tok, stride=qh), :].astype(BF16)

    for l in range(layers):
        last = l == layers - 1
        arrived(xg, l, 0)
        h = (rms(gathered_x(l), dm) * an_ref[l:l + 1, :].astype(F32)).astype(BF16)
        background(l, "x_in")
        for name, lo in (("q", 0), ("kv", wq.shape[-1])):
            w_fin(l, name)
            buf = groups[name][0]
            cols = buf.shape[-1]
            r = jnp.dot(h, buf[l].reshape(dm, cols), preferred_element_type=F32)
            qkvs[l, :, :, lo:lo + cols] = r.reshape(zn, tok, cols).astype(BF16)
        spread(lambda zt: qkvs.at[l, zt], qkvi.at[l, z], l, 1)
        qkvi[l, z] = qkvs[l, z]
        background(l, "qkv_sent")
        if l == 0:
            for k in range(layers):
                wait_bytes(kc.at[k], down_loc.at[k, 1])
                wait_bytes(vc.at[k], down_loc.at[k, 2])
        arrived(qkvi, l, 1)
        background(l, "qkv_in")
        attention(l)
        spread(lambda zt: og.at[l, z], og.at[l, z], l, 2)
        background(l, "o_sent")
        w_fin(l, "o")
        arrived(og, l, 2)
        o_all = og[l].astype(F32).reshape(nq, og.shape[-1]).astype(BF16)
        r = jnp.dot(o_all, wo[l].reshape(og.shape[-1], ctile), preferred_element_type=F32)
        xc = xg[l, :, :, pl.ds(pl.multiple_of(z * ctile, ctile), ctile)].astype(F32).reshape(nq, ctile)
        x1g[l, z] = (xc + r).astype(BF16)
        spread(lambda zt: x1g.at[l, z], x1g.at[l, z], l, 3)
        background(l, "x1_sent")
        wait_bytes(wd.at[l, 0], down_loc.at[l, 0])
        wait_bytes(wd.at[l, 0], down_recv.at[l])
        w_fin(l, "gu")
        arrived(x1g, l, 3)
        background(l, "x1_in")
        x1 = jnp.concatenate([x1g[l, zz].astype(F32) for zz in range(zn)], axis=-1)
        x1f[...] = x1
        h2 = (rms(x1, dm) * mn_ref[l:l + 1, :].astype(F32)).astype(BF16)
        gu = jnp.dot(h2, wgu[l].reshape(dm, wgu.shape[-1]), preferred_element_type=F32)
        ffc = wgu.shape[-1] // 2
        g = gu[:, :ffc]
        a = (g * jax.nn.sigmoid(g) * gu[:, ffc:]).astype(BF16)
        pr = jnp.dot(a, wd[l].reshape(ffc, dm), preferred_element_type=F32)
        pbuf[l] = pr.reshape(zn, tok, dm)
        spread(lambda zt: pbuf.at[l, zt], ybuf.at[l, z], l, 4)
        ybuf[l, z] = pbuf[l, z]
        background(l, "y_sent")
        arrived(ybuf, l, 4)
        total = ybuf[l, 0]
        for zz in range(1, zn):
            total = total + ybuf[l, zz]
        y = x1f[pl.ds(pl.multiple_of(z * tok, tok), tok), :] + total
        if last:
            y_ref[...] = jnp.concatenate([y[:, t * HEAD_DIM:(t + 1) * HEAD_DIM] for t in range(dm // HEAD_DIM)], axis=0).astype(BF16)
            outs.append(pltpu.make_async_copy(y_ref, res_hbm.at[0], out_sem.at[0]))
            outs[-1].start()
        else:
            xg[l + 1, z] = y.astype(BF16)
            spread(lambda zt: xg.at[l + 1, z], xg.at[l + 1, z], l + 1, 0)
            background(l + 1, "x_sent")

    for l in range(layers):
        for name in groups:
            w_drain(l, name)
        wait_bytes(wd.at[l, 0], down_send.at[l])
        for ph, buf in enumerate((xg, qkvi, og, x1g, ybuf)):
            wait_bytes(buf.at[l, 0:zn - 1], a_send.at[l, ph])
    for cp in outs:
        cp.wait()


def place_rows(layers, tok, kh, pos_hbm, res_hbm, kin, vin, y_out, kout, vout, pos_ref, res, in_sem, y_sem, bulk_sem, row_sem):
    small = [pltpu.make_async_copy(pos_hbm, pos_ref, in_sem.at[0]), pltpu.make_async_copy(res_hbm.at[0:1 + 2 * layers], res, in_sem.at[1])]
    for cp in small:
        cp.start()
    pairs = ((kin, kout), (vin, vout))
    bulk = [[[pltpu.make_async_copy(src.at[l, n], dst.at[l, n], bulk_sem.at[i, l, n]) for n in range(tok)] for l in range(layers)] for i, (src, dst) in enumerate(pairs)]
    for l in range(layers):
        for n in range(tok):
            for i in range(2):
                bulk[i][l][n].start()
    for cp in small:
        cp.wait()
    done = [pltpu.make_async_copy(res.at[0, pl.ds(t * tok, tok)], y_out.at[:, pl.ds(t * HEAD_DIM, HEAD_DIM)], y_sem.at[t]) for t in range(y_out.shape[1] // HEAD_DIM)]
    for cp in done:
        cp.start()
    for l in range(layers):
        for n in range(tok):
            at = pl.ds(pl.multiple_of(pos_ref[n] * kh, kh), kh)
            for i, (_, dst) in enumerate(pairs):
                bulk[i][l][n].wait()
                cp = pltpu.make_async_copy(res.at[1 + 2 * l + i, pl.ds(n * kh, kh)], dst.at[l, n, at], row_sem.at[i, l, n])
                cp.start()
                done.append(cp)
    for cp in done:
        cp.wait()


def solution(mesh):
    batch_axes = ("part", "dp")
    act_spec = P(batch_axes, None)
    cache_spec = P(None, batch_axes, None, None, None)
    mat_spec = P(None, "dp", None)
    gain_spec = P(None, None)
    in_specs = (act_spec, P(batch_axes), cache_spec, cache_spec, gain_spec, mat_spec, mat_spec, mat_spec, gain_spec, gain_spec, mat_spec, gain_spec, mat_spec, mat_spec, mat_spec)
    out_specs = (act_spec, cache_spec, cache_spec)
    zn = mesh.shape["dp"] // 2
    ny = math.isqrt(mesh.shape["part"])
    pool = 4 if ny * ny == mesh.shape["part"] and ny % 2 == 0 else 1

    def device_fn(x, positions, k_cache, v_cache, attn_norm, w_q, w_k, w_v, q_norm, k_norm, w_o, mlp_norm, w_gate, w_up, w_down):
        layers, tok, slots, kh, hd = k_cache.shape
        dm = x.shape[1]
        qw, kw, ff = w_q.shape[2], w_k.shape[2], w_gate.shape[2]
        qh = qw // hd
        nq = 2 * pool
        qkvc = (qw + 2 * kw) // zn
        cfg = dict(layers=layers, zn=zn, pool=pool, ny=ny, tok=tok, qh=qh, kh=kh)
        hb = pl.BlockSpec(memory_space=pltpu.HBM)
        dma = pltpu.SemaphoreType.DMA
        flat = (layers, tok, slots * kh, hd)
        scratch = [
            pltpu.VMEM((layers, zn, nq, w_q.shape[1] // pool, qw // zn), BF16),
            pltpu.VMEM((layers, zn, nq, w_k.shape[1] // pool, 2 * kw // zn), BF16),
            pltpu.VMEM((layers, zn, nq, w_o.shape[1] // pool, dm // zn), BF16),
            pltpu.VMEM((layers, zn, nq, w_gate.shape[1] // pool, 2 * ff // zn), BF16),
            pltpu.VMEM((layers, 2, w_down.shape[1], dm), BF16),
            pltpu.VMEM(flat, BF16),
            pltpu.VMEM(flat, BF16),
            pltpu.VMEM((layers, zn, tok, dm), BF16),
            pltpu.VMEM((layers, zn, tok, qkvc), BF16),
            pltpu.VMEM((layers, zn, tok, qkvc), BF16),
            pltpu.VMEM((layers, zn, tok, qw), BF16),
            pltpu.VMEM((layers, zn, zn * tok, dm // zn), BF16),
            pltpu.VMEM((layers, zn, tok, dm), F32),
            pltpu.VMEM((layers, zn, tok, dm), F32),
            pltpu.VMEM((zn * tok, dm), F32),
            pltpu.VMEM((tok * qh, hd), F32),
            pltpu.VMEM((tok * qh, hd), F32),
            pltpu.VMEM((tok * qh, hd), F32),
            pltpu.VMEM((tok * qh, hd), F32),
            pltpu.VMEM((tok * kh, hd), F32),
            pltpu.VMEM((tok * kh, hd), F32),
            pltpu.VMEM((tok, hd), F32),
            pltpu.VMEM((tok, hd), F32),
            pltpu.SMEM((tok,), jnp.int32),
            pltpu.VMEM((layers, dm), BF16),
            pltpu.VMEM((layers, hd), BF16),
            pltpu.VMEM((layers, hd), BF16),
            pltpu.VMEM((layers, dm), BF16),
            pltpu.VMEM((tok * kh, hd), BF16),
            pltpu.VMEM((layers, tok * kh, hd), BF16),
            pltpu.VMEM((layers, tok * kh, hd), BF16),
            dma((layers, 4)), dma((layers, 4)), dma((layers, 4, pool)), dma((layers, 4, pool)), dma((layers, 4, 4)), dma((layers, 4, 4)),
            dma((layers, 5)), dma((layers, 5)), dma((layers,)), dma((layers,)), dma((layers, 4)), dma((layers, 3)), dma((6,)), dma((1 + 2 * layers,)),
        ]
        res = pl.pallas_call(
            functools.partial(decode_kernel, cfg),
            name="decode",
            out_shape=jax.ShapeDtypeStruct((RES_BLOCKS, tok * kh, hd), BF16),
            in_specs=[hb] * 15,
            out_specs=hb,
            scratch_shapes=scratch,
            compiler_params=pltpu.CompilerParams(collective_id=0, has_side_effects=True, vmem_limit_bytes=VMEM_LIMIT),
        )(positions, x, attn_norm, q_norm, k_norm, mlp_norm, w_q, w_k, w_v, w_o, w_gate, w_up, w_down, k_cache.reshape(flat), v_cache.reshape(flat))
        anys = pl.BlockSpec(memory_space=pl.ANY)
        rows = (1 + 2 * layers, tok * kh, hd)
        y, k_out, v_out = pl.pallas_call(
            functools.partial(place_rows, layers, tok, kh),
            name="place",
            out_shape=(jax.ShapeDtypeStruct((tok, dm), BF16), jax.ShapeDtypeStruct(flat, BF16), jax.ShapeDtypeStruct(flat, BF16)),
            in_specs=[anys] * 4,
            out_specs=(anys,) * 3,
            scratch_shapes=[pltpu.SMEM((tok,), jnp.int32), pltpu.VMEM(rows, BF16), dma((2,)), dma((dm // hd,)), dma((2, layers, tok)), dma((2, layers, tok))],
            compiler_params=pltpu.CompilerParams(vmem_limit_bytes=PLACE_LIMIT),
        )(positions, res, k_cache.reshape(flat), v_cache.reshape(flat))
        k_out = k_out.reshape(k_cache.shape)
        v_out = v_out.reshape(v_cache.shape)
        return y, k_out, v_out

    return jax.shard_map(device_fn, mesh=mesh, in_specs=in_specs, out_specs=out_specs, check_vma=False)
```

```python
import functools
import math

import jax
import jax.numpy as jnp
from jax import lax
from jax.experimental import pallas as pl
from jax.experimental.pallas import tpu as pltpu
from jax.sharding import PartitionSpec as P

HEAD_DIM = 128
RMS_EPS = 1e-6
ROPE_THETA = 1000000.0
VMEM_LIMIT = 58400000
PLACE_LIMIT = 8 * 1024 * 1024
RES_BLOCKS = 4096

MESH = pl.DeviceIdType.MESH
F32 = jnp.float32
BF16 = jnp.bfloat16
NEG = float("-inf")


def rms(values, width):
    return values * lax.rsqrt(jnp.sum(values * values, axis=-1, keepdims=True) * (1.0 / width) + RMS_EPS)


def decode_kernel(cfg, pos_hbm, x_hbm, an_hbm, qn_hbm, kn_hbm, mn_hbm, wq_hbm, wk_hbm, wv_hbm, wo_hbm, wg_hbm, wu_hbm, wd_hbm, kc_hbm, vc_hbm,
                  res_hbm,
                  wq, wkv, wo, wgu, wd, kc, vc, xg, qkvs, qkvi, og, x1g, pbuf, ybuf, x1f, qs, ks, vs, os_, kro, vro, cs, sn, pos_ref, an_ref, qn_ref, kn_ref, mn_ref, y_ref, krow_ref, vrow_ref,
                  z_send, z_recv, d_send, d_recv, p_send, p_recv, a_send, a_recv, down_send, down_recv, loc_sem, down_loc, in_sem, out_sem, diag_send, diag_recv, diag_loc):
    layers, zn, pool, tok = cfg["layers"], cfg["zn"], cfg["pool"], cfg["tok"]
    qh, kh, ny = cfg["qh"], cfg["kh"], cfg["ny"]
    dm = x_hbm.shape[1]
    nq = zn * tok
    ctile = dm // zn
    zh = zn // 2
    idx = lax.axis_index("dp")
    z, c = idx // 2, idx % 2
    part = lax.axis_index("part")
    sib = {"dp": 2 * z + (1 - c)}
    if pool == 4:
        px, py = (part // ny) % 2, (part % ny) % 2
        xnei = {"part": part + ny * (1 - 2 * px)}
        ynei = {"part": part + 1 - 2 * py}
    else:
        px, py = 0, 0
    quarter = px * 2 + py
    sub = c * pool + quarter
    subx = c * pool + (1 - px) * 2 + py
    suby = c * pool + px * 2 + 1 - py
    subd = c * pool + (1 - px) * 2 + 1 - py

    order = []
    for r in range(zn // 2, 0, -1):
        order.append(r)
        if r != zn - r:
            order.append(zn - r)

    def peer(r):
        return lax.rem(z + r, zn)

    def peer_id(zt):
        return {"dp": 2 * zt + c}

    barrier = pltpu.get_barrier_semaphore()
    for r in order:
        pl.semaphore_signal(barrier, inc=1, device_id=peer_id(peer(r)), device_id_type=MESH)
    pl.semaphore_signal(barrier, inc=1, device_id=sib, device_id_type=MESH)
    if pool == 4:
        pl.semaphore_signal(barrier, inc=1, device_id=xnei, device_id_type=MESH)
        pl.semaphore_signal(barrier, inc=1, device_id=ynei, device_id_type=MESH)

    def rcopy(src, dst, ss, rs, dev):
        return pltpu.make_async_remote_copy(src_ref=src, dst_ref=dst, send_sem=ss, recv_sem=rs, device_id=dev, device_id_type=MESH)

    def wait_bytes(ref, sem):
        pltpu.make_async_copy(ref, ref, sem).wait()

    groups = {
        "q": (wq, 0, [(wq_hbm, 0)]),
        "kv": (wkv, 1, [(wk_hbm, 0), (wv_hbm, wkv.shape[-1] // 2)]),
        "o": (wo, 2, [(wo_hbm, 0)]),
        "gu": (wgu, 3, [(wg_hbm, 0), (wu_hbm, wgu.shape[-1] // 2)]),
    }

    direct = {(0, "q"), (0, "kv")} if pool == 4 else set()

    def pieces(l, name, zt, diag=False):
        buf, gi, srcs = groups[name]
        quart, to = (3 - quarter, subd) if diag else (quarter, sub)
        rows = buf.shape[3]
        out = []
        for src, off in srcs:
            width = src.shape[2] // zn
            s = src.at[l, pl.ds(pl.multiple_of(quart * rows, rows), rows), pl.ds(pl.multiple_of(zt * width, 128), width)]
            d = buf.at[l, z, to, :, pl.ds(off, width)]
            out.append((s, d))
        return out, gi

    def w_local(l, name):
        ps, gi = pieces(l, name, z)
        for s, d in ps:
            pltpu.make_async_copy(s, d, loc_sem.at[l, gi]).start()
        if (l, name) in direct:
            for s, d in pieces(l, name, z, True)[0]:
                pltpu.make_async_copy(s, d, diag_loc.at[gi]).start()

    def w_send(l, name):
        for r in order:
            zt = peer(r)
            ps, gi = pieces(l, name, zt)
            for s, d in ps:
                rcopy(s, d, z_send.at[l, gi], z_recv.at[l, gi], peer_id(zt)).start()

    def w_diag(l, name):
        if (l, name) in direct:
            for r in order:
                zt = peer(r)
                ps, gi = pieces(l, name, zt, True)
                for s, d in ps:
                    rcopy(s, d, diag_send.at[gi], diag_recv.at[gi], peer_id(zt)).start()

    def w_s1(l, name):
        buf, gi, _ = groups[name]
        wait_bytes(buf.at[l, 0:zn - 1, 0], z_recv.at[l, gi])
        wait_bytes(buf.at[l, 0, 0], loc_sem.at[l, gi])
        q = buf.at[l, :, sub]
        if pool == 4:
            rcopy(q, q, p_send.at[l, gi, 0], p_recv.at[l, gi, 0], xnei).start()
            rcopy(q, q, p_send.at[l, gi, 1], p_recv.at[l, gi, 1], ynei).start()
        rcopy(q, q, d_send.at[l, gi, 0], d_recv.at[l, gi, 0], sib).start()

    def w_s2(l, name):
        if pool == 4:
            buf, gi, _ = groups[name]
            qx, qy = buf.at[l, :, subx], buf.at[l, :, suby]
            hx, hy = buf.at[l, 0:zh, subx], buf.at[l, zh:zn, suby]
            wait_bytes(qx, p_recv.at[l, gi, 0])
            if (l, name) not in direct:
                rcopy(hx, hx, p_send.at[l, gi, 2], p_recv.at[l, gi, 2], ynei).start()
            rcopy(qx, qx, d_send.at[l, gi, 1], d_recv.at[l, gi, 1], sib).start()
            wait_bytes(qy, p_recv.at[l, gi, 1])
            if (l, name) not in direct:
                rcopy(hy, hy, p_send.at[l, gi, 3], p_recv.at[l, gi, 3], xnei).start()
            rcopy(qy, qy, d_send.at[l, gi, 2], d_recv.at[l, gi, 2], sib).start()

    def w_s3(l, name):
        if pool == 4:
            buf, gi, _ = groups[name]
            q = buf.at[l, :, subd]
            if (l, name) in direct:
                wait_bytes(buf.at[l, 0:zn - 1, 0], diag_recv.at[gi])
                wait_bytes(buf.at[l, 0, 0], diag_loc.at[gi])
            else:
                wait_bytes(buf.at[l, 0:zh, subd], p_recv.at[l, gi, 2])
                wait_bytes(buf.at[l, zh:zn, subd], p_recv.at[l, gi, 3])
            rcopy(q, q, d_send.at[l, gi, 3], d_recv.at[l, gi, 3], sib).start()

    def w_fin(l, name):
        buf, gi, _ = groups[name]
        for i in range(pool):
            wait_bytes(buf.at[l, :, 0], d_recv.at[l, gi, i])

    def w_drain(l, name):
        buf, gi, _ = groups[name]
        wait_bytes(buf.at[l, 0:zn - 1, 0], z_send.at[l, gi])
        for i in range(pool):
            wait_bytes(buf.at[l, :, 0], d_send.at[l, gi, i])
        if (l, name) in direct:
            wait_bytes(buf.at[l, 0:zn - 1, 0], diag_send.at[gi])
        if pool == 4:
            for i in range(2 if (l, name) in direct else 4):
                wait_bytes(buf.at[l, :, 0] if i < 2 else buf.at[l, 0:zh, 0], p_send.at[l, gi, i])

    def spread(src_of, dst, l, ph):
        for r in order:
            zt = peer(r)
            rcopy(src_of(zt), dst, a_send.at[l, ph], a_recv.at[l, ph], peer_id(zt)).start()

    def arrived(buf, l, ph):
        wait_bytes(buf.at[l, 0:zn - 1], a_recv.at[l, ph])

    plan = {
        (0, "entry"): [(w_send, 0, "q"), (w_send, 0, "kv"), (w_diag, 0, "q"), (w_diag, 0, "kv")],
        (0, "x_wait"): [(w_s1, 0, "q"), (w_s1, 0, "kv"), (w_send, 0, "o"), (w_send, 0, "gu"), (w_s2, 0, "q"), (w_s3, 0, "q"), (w_s2, 0, "kv"), (w_s3, 0, "kv")],
        (0, "qkv_sent"): [(w_send, 1, "q"), (w_send, 1, "kv"), (w_send, 1, "o"), (w_s1, 0, "o")],
        (0, "qkv_in"): [(w_s1, 0, "gu"), (w_s2, 0, "o")],
        (0, "o_sent"): [(w_s3, 0, "o"), (w_s2, 0, "gu"), (w_s1, 1, "q"), (w_s1, 1, "kv")],
        (0, "x1_sent"): [(w_send, 1, "gu"), (w_s3, 0, "gu")],
        (0, "x1_in"): [(w_s2, 1, "q"), (w_s2, 1, "kv"), (w_s1, 1, "o")],
        (0, "y_sent"): [(w_s3, 1, "q"), (w_s3, 1, "kv"), (w_s2, 1, "o")],
        (1, "x_sent"): [(w_s3, 1, "o"), (w_s1, 1, "gu")],
        (1, "qkv_sent"): [(w_s2, 1, "gu")],
        (1, "o_sent"): [(w_s3, 1, "gu")],
    }

    def background(l, point):
        for fn, wl, name in plan.get((l, point), ()):
            fn(wl, name)

    smalls = [(x_hbm, xg.at[0, z]), (pos_hbm, pos_ref), (an_hbm, an_ref), (qn_hbm, qn_ref), (kn_hbm, kn_ref), (mn_hbm, mn_ref)]
    small_copies = [pltpu.make_async_copy(s, d, in_sem.at[i]) for i, (s, d) in enumerate(smalls)]
    for cp in small_copies:
        cp.start()
    for l in range(layers):
        pltpu.make_async_copy(wd_hbm.at[l], wd.at[l, c], down_loc.at[l, 0]).start()
        for name in groups:
            w_local(l, name)
        pltpu.make_async_copy(kc_hbm.at[l], kc.at[l], down_loc.at[l, 1]).start()
        pltpu.make_async_copy(vc_hbm.at[l], vc.at[l], down_loc.at[l, 2]).start()

    pl.semaphore_wait(barrier, zn + (2 if pool == 4 else 0))

    background(0, "entry")
    small_copies[0].wait()
    spread(lambda zt: xg.at[0, z], xg.at[0, z], 0, 0)
    for l in range(layers):
        rcopy(wd_hbm.at[l], wd.at[l, c], down_send.at[l], down_recv.at[l], sib).start()

    for cp in small_copies[1:]:
        cp.wait()
    row_id = lax.broadcasted_iota(jnp.int32, (tok, HEAD_DIM), 0)
    lane_id = lax.broadcasted_iota(jnp.int32, (tok, HEAD_DIM), 1)
    pos = jnp.zeros((tok, HEAD_DIM), jnp.int32)
    for n in range(tok):
        pos = jnp.where(row_id == n, pos_ref[n], pos)
    half = HEAD_DIM // 2
    pair = jnp.where(lane_id >= half, lane_id - half, lane_id).astype(F32)
    inv_freq = jnp.exp(pair * (-2.0 * math.log(ROPE_THETA) / HEAD_DIM))
    ang = pos.astype(F32) * inv_freq
    cs[...] = jnp.cos(ang)
    sin_tab = jnp.sin(ang)
    sn[...] = jnp.where(lane_id >= half, sin_tab, -sin_tab)

    outs = []

    def head_norm(v, gain):
        v = rms(v, HEAD_DIM) * gain
        return (v * cs[...] + pltpu.roll(v, half, 1) * sn[...]).astype(BF16).astype(F32)

    def gathered_x(l):
        return xg[l].astype(F32).reshape(nq, dm)

    def attention(l):
        qg = qn_ref[l:l + 1, :].astype(F32)
        kg = kn_ref[l:l + 1, :].astype(F32)
        for h in range(qh):
            v = qkvi[l, h // 2, :, (h % 2) * HEAD_DIM:(h % 2 + 1) * HEAD_DIM].astype(F32)
            qs[pl.ds(h, tok, stride=qh), :] = head_norm(v, qg)
        for h in range(kh):
            k = head_norm(qkvi[l, h, :, 2 * HEAD_DIM:3 * HEAD_DIM].astype(F32), kg)
            v = qkvi[l, h, :, 3 * HEAD_DIM:4 * HEAD_DIM].astype(F32)
            for g in range(2):
                ks[pl.ds(2 * h + g, tok, stride=qh), :] = k
                vs[pl.ds(2 * h + g, tok, stride=qh), :] = v
            kro[pl.ds(h, tok, stride=kh), :] = k
            vro[pl.ds(h, tok, stride=kh), :] = v
        krow_ref[l] = kro[...].astype(BF16)
        vrow_ref[l] = vro[...].astype(BF16)
        outs.append(pltpu.make_async_copy(krow_ref.at[l], res_hbm.at[1 + 2 * l], out_sem.at[1 + 2 * l]))
        outs.append(pltpu.make_async_copy(vrow_ref.at[l], res_hbm.at[2 + 2 * l], out_sem.at[2 + 2 * l]))
        outs[-2].start()
        outs[-1].start()
        cols = kc.shape[2]
        lane = lax.broadcasted_iota(jnp.int32, (qh, cols), 1)
        row = lax.broadcasted_iota(jnp.int32, (qh, cols), 0)
        mine = lax.rem(lane, kh) == lax.shift_right_logical(row, 1)
        slot = jnp.where(mine, lax.div(lane, kh), cols)
        scale = HEAD_DIM ** -0.5
        for n0 in range(0, tok, 4):
            seqs = range(n0, n0 + 4)
            rows = [slice(n * qh, (n + 1) * qh) for n in seqs]
            q = [qs[r, :] for r in rows]
            s = [lax.dot_general(a.astype(BF16), kc[l, n], (((1,), (1,)), ((), ())), preferred_element_type=F32) * scale for a, n in zip(q, seqs)]
            s_new = [jnp.sum(a * ks[r, :], axis=-1, keepdims=True) * scale for a, r in zip(q, rows)]
            s = [jnp.where(slot < pos_ref[n], a, NEG) for a, n in zip(s, seqs)]
            m = [jnp.maximum(jnp.max(a, axis=-1, keepdims=True), b) for a, b in zip(s, s_new)]
            e = [jnp.exp(a - b) for a, b in zip(s, m)]
            e_new = [jnp.exp(a - b) for a, b in zip(s_new, m)]
            inv = [1.0 / (jnp.sum(a, axis=-1, keepdims=True) + b) for a, b in zip(e, e_new)]
            p = [(a * b).astype(BF16) for a, b in zip(e, inv)]
            p_new = [(a * b).astype(BF16).astype(F32) for a, b in zip(e_new, inv)]
            for a, b, r, n in zip(p, p_new, rows, seqs):
                os_[r, :] = jnp.dot(a, vc[l, n], preferred_element_type=F32) + b * vs[r, :]
        for h in range(qh):
            og[l, z, :, h * HEAD_DIM:(h + 1) * HEAD_DIM] = os_[pl.ds(h, tok, stride=qh), :].astype(BF16)

    for l in range(layers):
        last = l == layers - 1
        background(l, "x_wait")
        arrived(xg, l, 0)
        h = (rms(gathered_x(l), dm) * an_ref[l:l + 1, :].astype(F32)).astype(BF16)
        background(l, "x_in")
        w_fin(l, "q")
        w_fin(l, "kv")
        for name, lo in (("q", 0), ("kv", wq.shape[-1])):
            buf = groups[name][0]
            cols = buf.shape[-1]
            r = jnp.dot(h, buf[l].reshape(dm, cols), preferred_element_type=F32)
            qkvs[l, :, :, lo:lo + cols] = r.reshape(zn, tok, cols).astype(BF16)
        spread(lambda zt: qkvs.at[l, zt], qkvi.at[l, z], l, 1)
        qkvi[l, z] = qkvs[l, z]
        background(l, "qkv_sent")
        if l == 0:
            for k in range(layers):
                wait_bytes(kc.at[k], down_loc.at[k, 1])
                wait_bytes(vc.at[k], down_loc.at[k, 2])
        arrived(qkvi, l, 1)
        background(l, "qkv_in")
        attention(l)
        spread(lambda zt: og.at[l, z], og.at[l, z], l, 2)
        background(l, "o_sent")
        w_fin(l, "o")
        arrived(og, l, 2)
        o_all = og[l].astype(F32).reshape(nq, og.shape[-1]).astype(BF16)
        r = jnp.dot(o_all, wo[l].reshape(og.shape[-1], ctile), preferred_element_type=F32)
        xc = xg[l, :, :, pl.ds(pl.multiple_of(z * ctile, ctile), ctile)].astype(F32).reshape(nq, ctile)
        x1g[l, z] = (xc + r).astype(BF16)
        spread(lambda zt: x1g.at[l, z], x1g.at[l, z], l, 3)
        background(l, "x1_sent")
        wait_bytes(wd.at[l, 0], down_loc.at[l, 0])
        wait_bytes(wd.at[l, 0], down_recv.at[l])
        w_fin(l, "gu")
        arrived(x1g, l, 3)
        background(l, "x1_in")
        x1 = jnp.concatenate([x1g[l, zz].astype(F32) for zz in range(zn)], axis=-1)
        x1f[...] = x1
        h2 = (rms(x1, dm) * mn_ref[l:l + 1, :].astype(F32)).astype(BF16)
        gu = jnp.dot(h2, wgu[l].reshape(dm, wgu.shape[-1]), preferred_element_type=F32)
        ffc = wgu.shape[-1] // 2
        g = gu[:, :ffc]
        a = (g * jax.nn.sigmoid(g) * gu[:, ffc:]).astype(BF16)
        pr = jnp.dot(a, wd[l].reshape(ffc, dm), preferred_element_type=F32)
        pbuf[l] = pr.reshape(zn, tok, dm)
        spread(lambda zt: pbuf.at[l, zt], ybuf.at[l, z], l, 4)
        ybuf[l, z] = pbuf[l, z]
        background(l, "y_sent")
        arrived(ybuf, l, 4)
        total = ybuf[l, 0]
        for zz in range(1, zn):
            total = total + ybuf[l, zz]
        y = x1f[pl.ds(pl.multiple_of(z * tok, tok), tok), :] + total
        if last:
            y_ref[...] = jnp.concatenate([y[:, t * HEAD_DIM:(t + 1) * HEAD_DIM] for t in range(dm // HEAD_DIM)], axis=0).astype(BF16)
            outs.append(pltpu.make_async_copy(y_ref, res_hbm.at[0], out_sem.at[0]))
            outs[-1].start()
        else:
            xg[l + 1, z] = y.astype(BF16)
            spread(lambda zt: xg.at[l + 1, z], xg.at[l + 1, z], l + 1, 0)
            background(l + 1, "x_sent")

    for l in range(layers):
        for name in groups:
            w_drain(l, name)
        wait_bytes(wd.at[l, 0], down_send.at[l])
        for ph, buf in enumerate((xg, qkvi, og, x1g, ybuf)):
            wait_bytes(buf.at[l, 0:zn - 1], a_send.at[l, ph])
    for cp in outs:
        cp.wait()


def place_rows(layers, tok, kh, pos_hbm, res_hbm, kin, vin, y_out, kout, vout, pos_ref, res, in_sem, y_sem, bulk_sem, row_sem):
    small = [pltpu.make_async_copy(pos_hbm, pos_ref, in_sem.at[0]), pltpu.make_async_copy(res_hbm.at[0:1 + 2 * layers], res, in_sem.at[1])]
    for cp in small:
        cp.start()
    pairs = ((kin, kout), (vin, vout))
    bulk = [[[pltpu.make_async_copy(src.at[l, n], dst.at[l, n], bulk_sem.at[i, l, n]) for n in range(tok)] for l in range(layers)] for i, (src, dst) in enumerate(pairs)]
    for l in range(layers):
        for n in range(tok):
            for i in range(2):
                bulk[i][l][n].start()
    for cp in small:
        cp.wait()
    done = [pltpu.make_async_copy(res.at[0, pl.ds(t * tok, tok)], y_out.at[:, pl.ds(t * HEAD_DIM, HEAD_DIM)], y_sem.at[t]) for t in range(y_out.shape[1] // HEAD_DIM)]
    for cp in done:
        cp.start()
    for l in range(layers):
        for n in range(tok):
            at = pl.ds(pl.multiple_of(pos_ref[n] * kh, kh), kh)
            for i, (_, dst) in enumerate(pairs):
                bulk[i][l][n].wait()
                cp = pltpu.make_async_copy(res.at[1 + 2 * l + i, pl.ds(n * kh, kh)], dst.at[l, n, at], row_sem.at[i, l, n])
                cp.start()
                done.append(cp)
    for cp in done:
        cp.wait()


def solution(mesh):
    batch_axes = ("part", "dp")
    act_spec = P(batch_axes, None)
    cache_spec = P(None, batch_axes, None, None, None)
    mat_spec = P(None, "dp", None)
    gain_spec = P(None, None)
    in_specs = (act_spec, P(batch_axes), cache_spec, cache_spec, gain_spec, mat_spec, mat_spec, mat_spec, gain_spec, gain_spec, mat_spec, gain_spec, mat_spec, mat_spec, mat_spec)
    out_specs = (act_spec, cache_spec, cache_spec)
    zn = mesh.shape["dp"] // 2
    ny = math.isqrt(mesh.shape["part"])
    pool = 4 if ny * ny == mesh.shape["part"] and ny % 2 == 0 else 1

    def device_fn(x, positions, k_cache, v_cache, attn_norm, w_q, w_k, w_v, q_norm, k_norm, w_o, mlp_norm, w_gate, w_up, w_down):
        layers, tok, slots, kh, hd = k_cache.shape
        dm = x.shape[1]
        qw, kw, ff = w_q.shape[2], w_k.shape[2], w_gate.shape[2]
        qh = qw // hd
        nq = 2 * pool
        qkvc = (qw + 2 * kw) // zn
        cfg = dict(layers=layers, zn=zn, pool=pool, ny=ny, tok=tok, qh=qh, kh=kh)
        hb = pl.BlockSpec(memory_space=pltpu.HBM)
        dma = pltpu.SemaphoreType.DMA
        flat = (layers, tok, slots * kh, hd)
        scratch = [
            pltpu.VMEM((layers, zn, nq, w_q.shape[1] // pool, qw // zn), BF16),
            pltpu.VMEM((layers, zn, nq, w_k.shape[1] // pool, 2 * kw // zn), BF16),
            pltpu.VMEM((layers, zn, nq, w_o.shape[1] // pool, dm // zn), BF16),
            pltpu.VMEM((layers, zn, nq, w_gate.shape[1] // pool, 2 * ff // zn), BF16),
            pltpu.VMEM((layers, 2, w_down.shape[1], dm), BF16),
            pltpu.VMEM(flat, BF16),
            pltpu.VMEM(flat, BF16),
            pltpu.VMEM((layers, zn, tok, dm), BF16),
            pltpu.VMEM((layers, zn, tok, qkvc), BF16),
            pltpu.VMEM((layers, zn, tok, qkvc), BF16),
            pltpu.VMEM((layers, zn, tok, qw), BF16),
            pltpu.VMEM((layers, zn, zn * tok, dm // zn), BF16),
            pltpu.VMEM((layers, zn, tok, dm), F32),
            pltpu.VMEM((layers, zn, tok, dm), F32),
            pltpu.VMEM((zn * tok, dm), F32),
            pltpu.VMEM((tok * qh, hd), F32),
            pltpu.VMEM((tok * qh, hd), F32),
            pltpu.VMEM((tok * qh, hd), F32),
            pltpu.VMEM((tok * qh, hd), F32),
            pltpu.VMEM((tok * kh, hd), F32),
            pltpu.VMEM((tok * kh, hd), F32),
            pltpu.VMEM((tok, hd), F32),
            pltpu.VMEM((tok, hd), F32),
            pltpu.SMEM((tok,), jnp.int32),
            pltpu.VMEM((layers, dm), BF16),
            pltpu.VMEM((layers, hd), BF16),
            pltpu.VMEM((layers, hd), BF16),
            pltpu.VMEM((layers, dm), BF16),
            pltpu.VMEM((tok * kh, hd), BF16),
            pltpu.VMEM((layers, tok * kh, hd), BF16),
            pltpu.VMEM((layers, tok * kh, hd), BF16),
            dma((layers, 4)), dma((layers, 4)), dma((layers, 4, pool)), dma((layers, 4, pool)), dma((layers, 4, 4)), dma((layers, 4, 4)),
            dma((layers, 5)), dma((layers, 5)), dma((layers,)), dma((layers,)), dma((layers, 4)), dma((layers, 3)), dma((6,)), dma((1 + 2 * layers,)), dma((2,)), dma((2,)), dma((2,)),
        ]
        res = pl.pallas_call(
            functools.partial(decode_kernel, cfg),
            name="decode",
            out_shape=jax.ShapeDtypeStruct((RES_BLOCKS, tok * kh, hd), BF16),
            in_specs=[hb] * 15,
            out_specs=hb,
            scratch_shapes=scratch,
            compiler_params=pltpu.CompilerParams(collective_id=0, has_side_effects=True, vmem_limit_bytes=VMEM_LIMIT),
        )(positions, x, attn_norm, q_norm, k_norm, mlp_norm, w_q, w_k, w_v, w_o, w_gate, w_up, w_down, k_cache.reshape(flat), v_cache.reshape(flat))
        anys = pl.BlockSpec(memory_space=pl.ANY)
        rows = (1 + 2 * layers, tok * kh, hd)
        y, k_out, v_out = pl.pallas_call(
            functools.partial(place_rows, layers, tok, kh),
            name="place",
            out_shape=(jax.ShapeDtypeStruct((tok, dm), BF16), jax.ShapeDtypeStruct(flat, BF16), jax.ShapeDtypeStruct(flat, BF16)),
            in_specs=[anys] * 4,
            out_specs=(anys,) * 3,
            scratch_shapes=[pltpu.SMEM((tok,), jnp.int32), pltpu.VMEM(rows, BF16), dma((2,)), dma((dm // hd,)), dma((2, layers, tok)), dma((2, layers, tok))],
            compiler_params=pltpu.CompilerParams(vmem_limit_bytes=PLACE_LIMIT),
        )(positions, res, k_cache.reshape(flat), v_cache.reshape(flat))
        k_out = k_out.reshape(k_cache.shape)
        v_out = v_out.reshape(v_cache.shape)
        return y, k_out, v_out

    return jax.shard_map(device_fn, mesh=mesh, in_specs=in_specs, out_specs=out_specs, check_vma=False)
```

```python
import functools
import math

import jax
import jax.numpy as jnp
from jax import lax
from jax.experimental import pallas as pl
from jax.experimental.pallas import tpu as pltpu
from jax.sharding import PartitionSpec as P

HEAD_DIM = 128
RMS_EPS = 1e-6
ROPE_THETA = 1000000.0
VMEM_LIMIT = 58400000
PLACE_LIMIT = 8 * 1024 * 1024
RES_BLOCKS = 4096

MESH = pl.DeviceIdType.MESH
F32 = jnp.float32
BF16 = jnp.bfloat16
NEG = float("-inf")


def rms(values, width):
    return values * lax.rsqrt(jnp.sum(values * values, axis=-1, keepdims=True) * (1.0 / width) + RMS_EPS)


def decode_kernel(cfg, pos_hbm, x_hbm, an_hbm, qn_hbm, kn_hbm, mn_hbm, wq_hbm, wk_hbm, wv_hbm, wo_hbm, wg_hbm, wu_hbm, wd_hbm, kc_hbm, vc_hbm,
                  res_hbm,
                  wq, wkv, wo, wof, wgu, wd, kc, vc, xg, qkvs, qkvi, og, x1g, x1r, pbuf, ybuf, x1f, qs, ks, vs, os_, kro, vro, cs, sn, pos_ref, an_ref, qn_ref, kn_ref, mn_ref, y_ref, krow_ref, vrow_ref,
                  z_send, z_recv, d_send, d_recv, p_send, p_recv, a_send, a_recv, down_send, down_recv, loc_sem, down_loc, in_sem, out_sem, diag_send, diag_recv, diag_loc, ring_send, ring_recv, of_send, of_recv, of_sib):
    layers, zn, pool, tok = cfg["layers"], cfg["zn"], cfg["pool"], cfg["tok"]
    qh, kh, ny = cfg["qh"], cfg["kh"], cfg["ny"]
    dm = x_hbm.shape[1]
    nq = zn * tok
    ctile = dm // zn
    zh = zn // 2
    idx = lax.axis_index("dp")
    z, c = idx // 2, idx % 2
    part = lax.axis_index("part")
    sib = {"dp": 2 * z + (1 - c)}
    if pool == 4:
        px, py = (part // ny) % 2, (part % ny) % 2
        xnei = {"part": part + ny * (1 - 2 * px)}
        ynei = {"part": part + 1 - 2 * py}
    else:
        px, py = 0, 0
    quarter = px * 2 + py
    sub = c * pool + quarter
    subx = c * pool + (1 - px) * 2 + py
    suby = c * pool + px * 2 + 1 - py
    subd = c * pool + (1 - px) * 2 + 1 - py

    order = []
    for r in range(zn // 2, 0, -1):
        order.append(r)
        if r != zn - r:
            order.append(zn - r)

    def peer(r):
        return lax.rem(z + r, zn)

    def peer_id(zt):
        return {"dp": 2 * zt + c}

    barrier = pltpu.get_barrier_semaphore()
    for r in order:
        pl.semaphore_signal(barrier, inc=1, device_id=peer_id(peer(r)), device_id_type=MESH)
    pl.semaphore_signal(barrier, inc=1, device_id=sib, device_id_type=MESH)
    if pool == 4:
        pl.semaphore_signal(barrier, inc=1, device_id=xnei, device_id_type=MESH)
        pl.semaphore_signal(barrier, inc=1, device_id=ynei, device_id_type=MESH)

    def rcopy(src, dst, ss, rs, dev):
        return pltpu.make_async_remote_copy(src_ref=src, dst_ref=dst, send_sem=ss, recv_sem=rs, device_id=dev, device_id_type=MESH)

    def wait_bytes(ref, sem):
        pltpu.make_async_copy(ref, ref, sem).wait()

    groups = {
        "q": (wq, 0, [(wq_hbm, 0)]),
        "kv": (wkv, 1, [(wk_hbm, 0), (wv_hbm, wkv.shape[-1] // 2)]),
        "o": (wo, 2, [(wo_hbm, 0)]),
        "gu": (wgu, 3, [(wg_hbm, 0), (wu_hbm, wgu.shape[-1] // 2)]),
    }

    full_o = {layers - 1} if pool == 4 else set()

    def skip(l, name):
        return l in full_o and name == "o"

    half_rows = wof.shape[3] // 2
    right, left = peer_id(peer(1)), peer_id(peer(zn - 1))

    def r_block(d, which=None):
        return wof.at[0, lax.rem(z + zn + d, zn), sub if which is None else which]

    def signed(d):
        return (d,) if d in (0, zh) else (d, -d)

    def of_own(l, d):
        if d == 0:
            wait_bytes(r_block(0), loc_sem.at[l, 2])
        elif d == zh:
            ring(l, zh)
        for b in signed(d):
            q = r_block(b)
            rcopy(q, q, of_send.at[0], of_recv.at[0, d], xnei).start()
            rcopy(q, q, of_send.at[1], of_recv.at[1, d], ynei).start()
            rcopy(q, q, of_send.at[2], of_sib.at[0], sib).start()

    def of_relay(l, d):
        for i, which, to in ((0, subx, ynei), (1, suby, xnei)):
            wait_bytes(wof.at[0, 0:len(signed(d)), 0], of_recv.at[i, d])
            for b in signed(d):
                q = r_block(b, which)
                if (b > 0 if i == 0 else b <= 0):
                    rcopy(q, q, of_send.at[3], of_recv.at[2, d], to).start()
                rcopy(q, q, of_send.at[4 + i], of_sib.at[1 + i], sib).start()

    def of_last(l, d):
        wait_bytes(wof.at[0, 0:len(signed(d)), 0], of_recv.at[2, d])
        for b in signed(d):
            q = r_block(b, subd)
            rcopy(q, q, of_send.at[6], of_sib.at[3], sib).start()

    def of_fin():
        for i in range(4):
            wait_bytes(wof.at[0, :, 0], of_sib.at[i])

    def of_drain():
        for i in range(7):
            wait_bytes(wof.at[0, :, 0], of_send.at[i])
        for i in range(2):
            for step in range(zh):
                wait_bytes(r_block(0) if step < zh - 1 else r_halves(0)[0], ring_send.at[i, step])

    def r_halves(d):
        blk = lax.rem(z + zn + d, zn)
        return wof.at[0, blk, sub, 0:half_rows], wof.at[0, blk, sub, half_rows:2 * half_rows]

    def ring(l, step):
        if step == 0:
            src = wo_hbm.at[l, pl.ds(pl.multiple_of(quarter * 2 * half_rows, 2 * half_rows), 2 * half_rows)]
            pltpu.make_async_copy(src, r_block(0), loc_sem.at[l, 2]).start()
            rcopy(src, r_block(0), ring_send.at[0, 0], ring_recv.at[0, 0], right).start()
            rcopy(src, r_block(0), ring_send.at[1, 0], ring_recv.at[1, 0], left).start()
        elif step < zh - 1:
            for i, d, to in ((0, -step, right), (1, step, left)):
                wait_bytes(r_block(d), ring_recv.at[i, step - 1])
                rcopy(r_block(d), r_block(d), ring_send.at[i, step], ring_recv.at[i, step], to).start()
        elif step == zh - 1:
            for i, d, to in ((0, -step, right), (1, step, left)):
                wait_bytes(r_block(d), ring_recv.at[i, step - 1])
                h = r_halves(d)[i]
                rcopy(h, h, ring_send.at[i, step], ring_recv.at[i, step], to).start()
        else:
            for i in range(2):
                wait_bytes(r_halves(zh)[i], ring_recv.at[i, zh - 1])

    direct = {(0, "q"), (0, "kv")} if pool == 4 else set()

    def pieces(l, name, zt, diag=False):
        buf, gi, srcs = groups[name]
        quart, to = (3 - quarter, subd) if diag else (quarter, sub)
        rows = buf.shape[3]
        out = []
        for src, off in srcs:
            width = src.shape[2] // zn
            s = src.at[l, pl.ds(pl.multiple_of(quart * rows, rows), rows), pl.ds(pl.multiple_of(zt * width, 128), width)]
            d = buf.at[l, z, to, :, pl.ds(off, width)]
            out.append((s, d))
        return out, gi

    def w_local(l, name):
        ps, gi = pieces(l, name, z)
        for s, d in ps:
            pltpu.make_async_copy(s, d, loc_sem.at[l, gi]).start()
        if (l, name) in direct:
            for s, d in pieces(l, name, z, True)[0]:
                pltpu.make_async_copy(s, d, diag_loc.at[gi]).start()

    def w_send(l, name):
        for r in order:
            zt = peer(r)
            ps, gi = pieces(l, name, zt)
            for s, d in ps:
                rcopy(s, d, z_send.at[l, gi], z_recv.at[l, gi], peer_id(zt)).start()

    def w_diag(l, name):
        if (l, name) in direct:
            for r in order:
                zt = peer(r)
                ps, gi = pieces(l, name, zt, True)
                for s, d in ps:
                    rcopy(s, d, diag_send.at[gi], diag_recv.at[gi], peer_id(zt)).start()

    def w_s1(l, name):
        buf, gi, _ = groups[name]
        buf = buf.at[l]
        wait_bytes(buf.at[0:zn - 1, 0], z_recv.at[l, gi])
        wait_bytes(buf.at[0, 0], loc_sem.at[l, gi])
        q = buf.at[:, sub]
        if pool == 4:
            rcopy(q, q, p_send.at[l, gi, 0], p_recv.at[l, gi, 0], xnei).start()
            rcopy(q, q, p_send.at[l, gi, 1], p_recv.at[l, gi, 1], ynei).start()
        rcopy(q, q, d_send.at[l, gi, 0], d_recv.at[l, gi, 0], sib).start()

    def w_s2(l, name):
        if pool == 4:
            buf, gi, _ = groups[name]
            buf = buf.at[l]
            qx, qy = buf.at[:, subx], buf.at[:, suby]
            hx, hy = buf.at[0:zh, subx], buf.at[zh:zn, suby]
            wait_bytes(qx, p_recv.at[l, gi, 0])
            if (l, name) not in direct:
                rcopy(hx, hx, p_send.at[l, gi, 2], p_recv.at[l, gi, 2], ynei).start()
            rcopy(qx, qx, d_send.at[l, gi, 1], d_recv.at[l, gi, 1], sib).start()
            wait_bytes(qy, p_recv.at[l, gi, 1])
            if (l, name) not in direct:
                rcopy(hy, hy, p_send.at[l, gi, 3], p_recv.at[l, gi, 3], xnei).start()
            rcopy(qy, qy, d_send.at[l, gi, 2], d_recv.at[l, gi, 2], sib).start()

    def w_s3(l, name):
        if pool == 4:
            buf, gi, _ = groups[name]
            buf = buf.at[l]
            q = buf.at[:, subd]
            if (l, name) in direct:
                wait_bytes(buf.at[0:zn - 1, 0], diag_recv.at[gi])
                wait_bytes(buf.at[0, 0], diag_loc.at[gi])
            else:
                wait_bytes(buf.at[0:zh, subd], p_recv.at[l, gi, 2])
                wait_bytes(buf.at[zh:zn, subd], p_recv.at[l, gi, 3])
            rcopy(q, q, d_send.at[l, gi, 3], d_recv.at[l, gi, 3], sib).start()

    def w_fin(l, name):
        buf, gi, _ = groups[name]
        buf = buf.at[l]
        for i in range(pool):
            wait_bytes(buf.at[:, 0], d_recv.at[l, gi, i])

    def w_drain(l, name):
        buf, gi, _ = groups[name]
        buf = buf.at[l]
        wait_bytes(buf.at[0:zn - 1, 0], z_send.at[l, gi])
        for i in range(pool):
            wait_bytes(buf.at[:, 0], d_send.at[l, gi, i])
        if (l, name) in direct:
            wait_bytes(buf.at[0:zn - 1, 0], diag_send.at[gi])
        if pool == 4:
            for i in range(2 if (l, name) in direct else 4):
                wait_bytes(buf.at[:, 0] if i < 2 else buf.at[0:zh, 0], p_send.at[l, gi, i])

    def spread(src_of, dst, l, ph):
        for r in order:
            zt = peer(r)
            rcopy(src_of(zt), dst, a_send.at[l, ph], a_recv.at[l, ph], peer_id(zt)).start()

    def arrived(buf, l, ph):
        if l is None:
            wait_bytes(buf.at[0:zn - 1], a_recv.at[layers - 1, ph])
        else:
            wait_bytes(buf.at[l, 0:zn - 1], a_recv.at[l, ph])

    end = layers - 1
    plan = {
        (0, "entry"): [(w_send, 0, "q"), (w_send, 0, "kv"), (w_diag, 0, "q"), (w_diag, 0, "kv")],
        (0, "x_wait"): [(ring, end, 0), (w_s1, 0, "q"), (w_s1, 0, "kv"), (w_send, 0, "o"), (w_send, 0, "gu"), (w_s2, 0, "q"), (w_s3, 0, "q"), (w_s2, 0, "kv"), (w_s3, 0, "kv")],
        (0, "qkv_sent"): [(ring, end, 1), (w_send, 1, "q"), (w_send, 1, "kv"), (w_s1, 0, "o"), (of_own, end, 0), (of_own, end, 1)],
        (0, "qkv_in"): [(w_s2, 0, "o"), (w_s1, 0, "gu")],
        (0, "o_sent"): [(ring, end, 2), (w_s3, 0, "o"), (w_s2, 0, "gu"), (w_s1, 1, "q"), (w_s1, 1, "kv"), (of_relay, end, 0), (of_own, end, 2)],
        (0, "x1_sent"): [(ring, end, 3), (w_send, 1, "gu"), (w_s3, 0, "gu"), (of_own, end, 3)],
        (0, "x1_in"): [(w_s2, 1, "q"), (w_s2, 1, "kv")],
        (0, "y_sent"): [(of_relay, end, 1), (of_relay, end, 2), (w_s1, 1, "gu"), (w_s3, 1, "q"), (w_s3, 1, "kv"), (of_own, end, zh)],
        (1, "x_sent"): [(of_relay, end, 3), (of_relay, end, zh), (of_last, end, 0), (of_last, end, 1), (of_last, end, 2)],
        (1, "qkv_sent"): [(w_s2, 1, "gu"), (of_last, end, 3), (of_last, end, zh)],
        (1, "x1_sent"): [(w_s3, 1, "gu")],
    } if full_o else {
        (0, "entry"): [(w_send, 0, "q"), (w_send, 0, "kv"), (w_send, 0, "o"), (w_send, 0, "gu")],
        (0, "x_wait"): [(w_s1, 0, "q"), (w_s1, 0, "kv")],
        (0, "qkv_sent"): [(w_s1, 0, "o"), (w_send, 1, "q"), (w_send, 1, "kv"), (w_send, 1, "o")],
        (0, "o_sent"): [(w_s1, 0, "gu")],
        (0, "x1_sent"): [(w_send, 1, "gu"), (w_s1, 1, "q"), (w_s1, 1, "kv")],
        (0, "y_sent"): [(w_s1, 1, "o")],
        (1, "qkv_sent"): [(w_s1, 1, "gu")],
    }

    def background(l, point):
        for fn, wl, name in plan.get((l, point), ()):
            fn(wl, name)

    smalls = [(x_hbm, xg.at[0, z]), (pos_hbm, pos_ref), (an_hbm, an_ref), (qn_hbm, qn_ref), (kn_hbm, kn_ref), (mn_hbm, mn_ref)]
    small_copies = [pltpu.make_async_copy(s, d, in_sem.at[i]) for i, (s, d) in enumerate(smalls)]
    for cp in small_copies:
        cp.start()
    for l in range(layers):
        pltpu.make_async_copy(wd_hbm.at[l], wd.at[l, c], down_loc.at[l, 0]).start()
        for name in ("q", "kv", "o", "gu"):
            if not skip(l, name):
                w_local(l, name)
        pltpu.make_async_copy(kc_hbm.at[l], kc.at[l], down_loc.at[l, 1]).start()
        pltpu.make_async_copy(vc_hbm.at[l], vc.at[l], down_loc.at[l, 2]).start()

    pl.semaphore_wait(barrier, zn + (2 if pool == 4 else 0))

    background(0, "entry")
    small_copies[0].wait()
    spread(lambda zt: xg.at[0, z], xg.at[0, z], 0, 0)
    for l in range(layers):
        rcopy(wd_hbm.at[l], wd.at[l, c], down_send.at[l], down_recv.at[l], sib).start()

    for cp in small_copies[1:]:
        cp.wait()
    row_id = lax.broadcasted_iota(jnp.int32, (tok, HEAD_DIM), 0)
    lane_id = lax.broadcasted_iota(jnp.int32, (tok, HEAD_DIM), 1)
    pos = jnp.zeros((tok, HEAD_DIM), jnp.int32)
    for n in range(tok):
        pos = jnp.where(row_id == n, pos_ref[n], pos)
    half = HEAD_DIM // 2
    pair = jnp.where(lane_id >= half, lane_id - half, lane_id).astype(F32)
    inv_freq = jnp.exp(pair * (-2.0 * math.log(ROPE_THETA) / HEAD_DIM))
    ang = pos.astype(F32) * inv_freq
    cs[...] = jnp.cos(ang)
    sin_tab = jnp.sin(ang)
    sn[...] = jnp.where(lane_id >= half, sin_tab, -sin_tab)

    outs = []

    def head_norm(v, gain):
        v = rms(v, HEAD_DIM) * gain
        return (v * cs[...] + pltpu.roll(v, half, 1) * sn[...]).astype(BF16).astype(F32)

    def gathered_x(l):
        return xg[l].astype(F32).reshape(nq, dm)

    def attention(l):
        qg = qn_ref[l:l + 1, :].astype(F32)
        kg = kn_ref[l:l + 1, :].astype(F32)
        for h in range(qh):
            v = qkvi[l, h // 2, :, (h % 2) * HEAD_DIM:(h % 2 + 1) * HEAD_DIM].astype(F32)
            qs[pl.ds(h, tok, stride=qh), :] = head_norm(v, qg)
        for h in range(kh):
            k = head_norm(qkvi[l, h, :, 2 * HEAD_DIM:3 * HEAD_DIM].astype(F32), kg)
            v = qkvi[l, h, :, 3 * HEAD_DIM:4 * HEAD_DIM].astype(F32)
            for g in range(2):
                ks[pl.ds(2 * h + g, tok, stride=qh), :] = k
                vs[pl.ds(2 * h + g, tok, stride=qh), :] = v
            kro[pl.ds(h, tok, stride=kh), :] = k
            vro[pl.ds(h, tok, stride=kh), :] = v
        krow_ref[l] = kro[...].astype(BF16)
        vrow_ref[l] = vro[...].astype(BF16)
        outs.append(pltpu.make_async_copy(krow_ref.at[l], res_hbm.at[1 + 2 * l], out_sem.at[1 + 2 * l]))
        outs.append(pltpu.make_async_copy(vrow_ref.at[l], res_hbm.at[2 + 2 * l], out_sem.at[2 + 2 * l]))
        outs[-2].start()
        outs[-1].start()
        cols = kc.shape[2]
        lane = lax.broadcasted_iota(jnp.int32, (qh, cols), 1)
        row = lax.broadcasted_iota(jnp.int32, (qh, cols), 0)
        mine = lax.rem(lane, kh) == lax.shift_right_logical(row, 1)
        slot = jnp.where(mine, lax.div(lane, kh), cols)
        scale = HEAD_DIM ** -0.5
        for n0 in range(0, tok, 4):
            seqs = range(n0, n0 + 4)
            rows = [slice(n * qh, (n + 1) * qh) for n in seqs]
            q = [qs[r, :] for r in rows]
            s = [lax.dot_general(a.astype(BF16), kc[l, n], (((1,), (1,)), ((), ())), preferred_element_type=F32) * scale for a, n in zip(q, seqs)]
            s_new = [jnp.sum(a * ks[r, :], axis=-1, keepdims=True) * scale for a, r in zip(q, rows)]
            s = [jnp.where(slot < pos_ref[n], a, NEG) for a, n in zip(s, seqs)]
            m = [jnp.maximum(jnp.max(a, axis=-1, keepdims=True), b) for a, b in zip(s, s_new)]
            e = [jnp.exp(a - b) for a, b in zip(s, m)]
            e_new = [jnp.exp(a - b) for a, b in zip(s_new, m)]
            inv = [1.0 / (jnp.sum(a, axis=-1, keepdims=True) + b) for a, b in zip(e, e_new)]
            p = [(a * b).astype(BF16) for a, b in zip(e, inv)]
            p_new = [(a * b).astype(BF16).astype(F32) for a, b in zip(e_new, inv)]
            for a, b, r, n in zip(p, p_new, rows, seqs):
                os_[r, :] = jnp.dot(a, vc[l, n], preferred_element_type=F32) + b * vs[r, :]
        for h in range(qh):
            og[l, z, :, h * HEAD_DIM:(h + 1) * HEAD_DIM] = os_[pl.ds(h, tok, stride=qh), :].astype(BF16)

    def own_rows(l):
        of_fin()
        r = jnp.dot(og[l, z], wof[0].reshape(og.shape[-1], dm), preferred_element_type=F32)
        x1r[z] = (xg[l, z].astype(F32) + r).astype(BF16)
        spread(lambda zt: x1r.at[z], x1r.at[z], l, 3)
        background(l, "x1_sent")
        wait_bytes(wd.at[l, 0], down_loc.at[l, 0])
        wait_bytes(wd.at[l, 0], down_recv.at[l])
        w_fin(l, "gu")
        arrived(x1r, None, 3)
        return x1r[...].astype(F32).reshape(nq, dm)

    def gathered_rows(l):
        spread(lambda zt: og.at[l, z], og.at[l, z], l, 2)
        background(l, "o_sent")
        w_fin(l, "o")
        arrived(og, l, 2)
        o_all = og[l].astype(F32).reshape(nq, og.shape[-1]).astype(BF16)
        r = jnp.dot(o_all, wo[l].reshape(og.shape[-1], ctile), preferred_element_type=F32)
        xc = xg[l, :, :, pl.ds(pl.multiple_of(z * ctile, ctile), ctile)].astype(F32).reshape(nq, ctile)
        x1g[l, z] = (xc + r).astype(BF16)
        spread(lambda zt: x1g.at[l, z], x1g.at[l, z], l, 3)
        background(l, "x1_sent")
        wait_bytes(wd.at[l, 0], down_loc.at[l, 0])
        wait_bytes(wd.at[l, 0], down_recv.at[l])
        w_fin(l, "gu")
        arrived(x1g, l, 3)
        background(l, "x1_in")
        return jnp.concatenate([x1g[l, zz].astype(F32) for zz in range(zn)], axis=-1)

    for l in range(layers):
        last = l == layers - 1
        background(l, "x_wait")
        arrived(xg, l, 0)
        h = (rms(gathered_x(l), dm) * an_ref[l:l + 1, :].astype(F32)).astype(BF16)
        background(l, "x_in")
        w_fin(l, "q")
        w_fin(l, "kv")
        for name, lo in (("q", 0), ("kv", wq.shape[-1])):
            buf = groups[name][0]
            cols = buf.shape[-1]
            r = jnp.dot(h, buf[l].reshape(dm, cols), preferred_element_type=F32)
            qkvs[l, :, :, lo:lo + cols] = r.reshape(zn, tok, cols).astype(BF16)
        spread(lambda zt: qkvs.at[l, zt], qkvi.at[l, z], l, 1)
        qkvi[l, z] = qkvs[l, z]
        background(l, "qkv_sent")
        if l == 0:
            for k in range(layers):
                wait_bytes(kc.at[k], down_loc.at[k, 1])
                wait_bytes(vc.at[k], down_loc.at[k, 2])
        arrived(qkvi, l, 1)
        background(l, "qkv_in")
        attention(l)
        x1 = own_rows(l) if l in full_o else gathered_rows(l)
        x1f[...] = x1
        h2 = (rms(x1, dm) * mn_ref[l:l + 1, :].astype(F32)).astype(BF16)
        gu = jnp.dot(h2, wgu[l].reshape(dm, wgu.shape[-1]), preferred_element_type=F32)
        ffc = wgu.shape[-1] // 2
        g = gu[:, :ffc]
        a = (g * jax.nn.sigmoid(g) * gu[:, ffc:]).astype(BF16)
        pr = jnp.dot(a, wd[l].reshape(ffc, dm), preferred_element_type=F32)
        pbuf[l] = pr.reshape(zn, tok, dm)
        spread(lambda zt: pbuf.at[l, zt], ybuf.at[l, z], l, 4)
        ybuf[l, z] = pbuf[l, z]
        background(l, "y_sent")
        arrived(ybuf, l, 4)
        total = ybuf[l, 0]
        for zz in range(1, zn):
            total = total + ybuf[l, zz]
        y = x1f[pl.ds(pl.multiple_of(z * tok, tok), tok), :] + total
        if last:
            y_ref[...] = jnp.concatenate([y[:, t * HEAD_DIM:(t + 1) * HEAD_DIM] for t in range(dm // HEAD_DIM)], axis=0).astype(BF16)
            outs.append(pltpu.make_async_copy(y_ref, res_hbm.at[0], out_sem.at[0]))
            outs[-1].start()
        else:
            xg[l + 1, z] = y.astype(BF16)
            spread(lambda zt: xg.at[l + 1, z], xg.at[l + 1, z], l + 1, 0)
            background(l + 1, "x_sent")

    for l in range(layers):
        for name in groups:
            if not skip(l, name):
                w_drain(l, name)
        if l in full_o:
            of_drain()
        wait_bytes(wd.at[l, 0], down_send.at[l])
        for ph, buf in enumerate((xg, qkvi, og, x1g, ybuf)):
            if ph != 2 or l not in full_o:
                wait_bytes(buf.at[l, 0:zn - 1], a_send.at[l, ph])
    for cp in outs:
        cp.wait()


def place_rows(layers, tok, kh, pos_hbm, res_hbm, kin, vin, y_out, kout, vout, pos_ref, res, in_sem, y_sem, bulk_sem, row_sem):
    small = [pltpu.make_async_copy(pos_hbm, pos_ref, in_sem.at[0]), pltpu.make_async_copy(res_hbm.at[0:1 + 2 * layers], res, in_sem.at[1])]
    for cp in small:
        cp.start()
    pairs = ((kin, kout), (vin, vout))
    bulk = [[[pltpu.make_async_copy(src.at[l, n], dst.at[l, n], bulk_sem.at[i, l, n]) for n in range(tok)] for l in range(layers)] for i, (src, dst) in enumerate(pairs)]
    for l in range(layers):
        for n in range(tok):
            for i in range(2):
                bulk[i][l][n].start()
    for cp in small:
        cp.wait()
    done = [pltpu.make_async_copy(res.at[0, pl.ds(t * tok, tok)], y_out.at[:, pl.ds(t * HEAD_DIM, HEAD_DIM)], y_sem.at[t]) for t in range(y_out.shape[1] // HEAD_DIM)]
    for cp in done:
        cp.start()
    for l in range(layers):
        for n in range(tok):
            at = pl.ds(pl.multiple_of(pos_ref[n] * kh, kh), kh)
            for i, (_, dst) in enumerate(pairs):
                bulk[i][l][n].wait()
                cp = pltpu.make_async_copy(res.at[1 + 2 * l + i, pl.ds(n * kh, kh)], dst.at[l, n, at], row_sem.at[i, l, n])
                cp.start()
                done.append(cp)
    for cp in done:
        cp.wait()


def solution(mesh):
    batch_axes = ("part", "dp")
    act_spec = P(batch_axes, None)
    cache_spec = P(None, batch_axes, None, None, None)
    mat_spec = P(None, "dp", None)
    gain_spec = P(None, None)
    in_specs = (act_spec, P(batch_axes), cache_spec, cache_spec, gain_spec, mat_spec, mat_spec, mat_spec, gain_spec, gain_spec, mat_spec, gain_spec, mat_spec, mat_spec, mat_spec)
    out_specs = (act_spec, cache_spec, cache_spec)
    zn = mesh.shape["dp"] // 2
    ny = math.isqrt(mesh.shape["part"])
    pool = 4 if ny * ny == mesh.shape["part"] and ny % 2 == 0 else 1

    def device_fn(x, positions, k_cache, v_cache, attn_norm, w_q, w_k, w_v, q_norm, k_norm, w_o, mlp_norm, w_gate, w_up, w_down):
        layers, tok, slots, kh, hd = k_cache.shape
        dm = x.shape[1]
        qw, kw, ff = w_q.shape[2], w_k.shape[2], w_gate.shape[2]
        qh = qw // hd
        nq = 2 * pool
        qkvc = (qw + 2 * kw) // zn
        cfg = dict(layers=layers, zn=zn, pool=pool, ny=ny, tok=tok, qh=qh, kh=kh)
        hb = pl.BlockSpec(memory_space=pltpu.HBM)
        dma = pltpu.SemaphoreType.DMA
        flat = (layers, tok, slots * kh, hd)
        scratch = [
            pltpu.VMEM((layers, zn, nq, w_q.shape[1] // pool, qw // zn), BF16),
            pltpu.VMEM((layers, zn, nq, w_k.shape[1] // pool, 2 * kw // zn), BF16),
            pltpu.VMEM((layers, zn, nq, w_o.shape[1] // pool, dm // zn), BF16),
            pltpu.VMEM((1, zn, nq, w_o.shape[1] // pool, dm), BF16),
            pltpu.VMEM((layers, zn, nq, w_gate.shape[1] // pool, 2 * ff // zn), BF16),
            pltpu.VMEM((layers, 2, w_down.shape[1], dm), BF16),
            pltpu.VMEM(flat, BF16),
            pltpu.VMEM(flat, BF16),
            pltpu.VMEM((layers, zn, tok, dm), BF16),
            pltpu.VMEM((layers, zn, tok, qkvc), BF16),
            pltpu.VMEM((layers, zn, tok, qkvc), BF16),
            pltpu.VMEM((layers, zn, tok, qw), BF16),
            pltpu.VMEM((layers, zn, zn * tok, dm // zn), BF16),
            pltpu.VMEM((zn, tok, dm), BF16),
            pltpu.VMEM((layers, zn, tok, dm), F32),
            pltpu.VMEM((layers, zn, tok, dm), F32),
            pltpu.VMEM((zn * tok, dm), F32),
            pltpu.VMEM((tok * qh, hd), F32),
            pltpu.VMEM((tok * qh, hd), F32),
            pltpu.VMEM((tok * qh, hd), F32),
            pltpu.VMEM((tok * qh, hd), F32),
            pltpu.VMEM((tok * kh, hd), F32),
            pltpu.VMEM((tok * kh, hd), F32),
            pltpu.VMEM((tok, hd), F32),
            pltpu.VMEM((tok, hd), F32),
            pltpu.SMEM((tok,), jnp.int32),
            pltpu.VMEM((layers, dm), BF16),
            pltpu.VMEM((layers, hd), BF16),
            pltpu.VMEM((layers, hd), BF16),
            pltpu.VMEM((layers, dm), BF16),
            pltpu.VMEM((tok * kh, hd), BF16),
            pltpu.VMEM((layers, tok * kh, hd), BF16),
            pltpu.VMEM((layers, tok * kh, hd), BF16),
            dma((layers, 4)), dma((layers, 4)), dma((layers, 4, pool)), dma((layers, 4, pool)), dma((layers, 4, 4)), dma((layers, 4, 4)),
            dma((layers, 5)), dma((layers, 5)), dma((layers,)), dma((layers,)), dma((layers, 4)), dma((layers, 3)), dma((6,)), dma((1 + 2 * layers,)), dma((2,)), dma((2,)), dma((2,)), dma((2, zn // 2)), dma((2, zn // 2)), dma((7,)), dma((3, zn // 2 + 1)), dma((4,)),
        ]
        res = pl.pallas_call(
            functools.partial(decode_kernel, cfg),
            name="decode",
            out_shape=jax.ShapeDtypeStruct((RES_BLOCKS, tok * kh, hd), BF16),
            in_specs=[hb] * 15,
            out_specs=hb,
            scratch_shapes=scratch,
            compiler_params=pltpu.CompilerParams(collective_id=0, has_side_effects=True, vmem_limit_bytes=VMEM_LIMIT),
        )(positions, x, attn_norm, q_norm, k_norm, mlp_norm, w_q, w_k, w_v, w_o, w_gate, w_up, w_down, k_cache.reshape(flat), v_cache.reshape(flat))
        anys = pl.BlockSpec(memory_space=pl.ANY)
        rows = (1 + 2 * layers, tok * kh, hd)
        y, k_out, v_out = pl.pallas_call(
            functools.partial(place_rows, layers, tok, kh),
            name="place",
            out_shape=(jax.ShapeDtypeStruct((tok, dm), BF16), jax.ShapeDtypeStruct(flat, BF16), jax.ShapeDtypeStruct(flat, BF16)),
            in_specs=[anys] * 4,
            out_specs=(anys,) * 3,
            scratch_shapes=[pltpu.SMEM((tok,), jnp.int32), pltpu.VMEM(rows, BF16), dma((2,)), dma((dm // hd,)), dma((2, layers, tok)), dma((2, layers, tok))],
            compiler_params=pltpu.CompilerParams(vmem_limit_bytes=PLACE_LIMIT),
        )(positions, res, k_cache.reshape(flat), v_cache.reshape(flat))
        k_out = k_out.reshape(k_cache.shape)
        v_out = v_out.reshape(v_cache.shape)
        return y, k_out, v_out

    return jax.shard_map(device_fn, mesh=mesh, in_specs=in_specs, out_specs=out_specs, check_vma=False)
```

```python
import functools
import math

import jax
import jax.numpy as jnp
from jax import lax
from jax.experimental import pallas as pl
from jax.experimental.pallas import tpu as pltpu
from jax.sharding import PartitionSpec as P

HEAD_DIM = 128
RMS_EPS = 1e-6
ROPE_THETA = 1000000.0
VMEM_LIMIT = 58400000
PLACE_LIMIT = 8 * 1024 * 1024
RES_BLOCKS = 4096

MESH = pl.DeviceIdType.MESH
F32 = jnp.float32
BF16 = jnp.bfloat16
NEG = float("-inf")


def rms(values, width):
    return values * lax.rsqrt(jnp.sum(values * values, axis=-1, keepdims=True) * (1.0 / width) + RMS_EPS)


def decode_kernel(cfg, pos_hbm, x_hbm, an_hbm, qn_hbm, kn_hbm, mn_hbm, wq_hbm, wk_hbm, wv_hbm, wo_hbm, wg_hbm, wu_hbm, wd_hbm, kc_hbm, vc_hbm,
                  res_hbm,
                  wq, wkv, wo, wof, wg, wu, wd, kc, vc, xg, qkvs, qkvi, og, x1g, x1r, pbuf, ybuf, x1f, qs, ks, vs, os_, kro, vro, cs, sn, pos_ref, an_ref, qn_ref, kn_ref, mn_ref, y_ref, krow_ref, vrow_ref,
                  z_send, z_recv, d_send, d_recv, p_send, p_recv, a_send, a_recv, down_send, down_recv, loc_sem, down_loc, in_sem, out_sem, diag_send, diag_recv, diag_loc, ring_send, ring_recv, of_send, of_recv, of_sib):
    layers, zn, pool, tok = cfg["layers"], cfg["zn"], cfg["pool"], cfg["tok"]
    qh, kh, ny = cfg["qh"], cfg["kh"], cfg["ny"]
    dm = x_hbm.shape[1]
    nq = zn * tok
    ctile = dm // zn
    zh = zn // 2
    idx = lax.axis_index("dp")
    z, c = idx // 2, idx % 2
    part = lax.axis_index("part")
    sib = {"dp": 2 * z + (1 - c)}
    if pool == 4:
        px, py = (part // ny) % 2, (part % ny) % 2
        xnei = {"part": part + ny * (1 - 2 * px)}
        ynei = {"part": part + 1 - 2 * py}
    else:
        px, py = 0, 0
    quarter = px * 2 + py
    sub = c * pool + quarter
    subx = c * pool + (1 - px) * 2 + py
    suby = c * pool + px * 2 + 1 - py
    subd = c * pool + (1 - px) * 2 + 1 - py

    order = []
    for r in range(zn // 2, 0, -1):
        order.append(r)
        if r != zn - r:
            order.append(zn - r)

    def peer(r):
        return lax.rem(z + r, zn)

    def peer_id(zt):
        return {"dp": 2 * zt + c}

    barrier = pltpu.get_barrier_semaphore()
    for r in order:
        pl.semaphore_signal(barrier, inc=1, device_id=peer_id(peer(r)), device_id_type=MESH)
    pl.semaphore_signal(barrier, inc=1, device_id=sib, device_id_type=MESH)
    if pool == 4:
        pl.semaphore_signal(barrier, inc=1, device_id=xnei, device_id_type=MESH)
        pl.semaphore_signal(barrier, inc=1, device_id=ynei, device_id_type=MESH)

    def rcopy(src, dst, ss, rs, dev):
        return pltpu.make_async_remote_copy(src_ref=src, dst_ref=dst, send_sem=ss, recv_sem=rs, device_id=dev, device_id_type=MESH)

    def wait_bytes(ref, sem):
        pltpu.make_async_copy(ref, ref, sem).wait()

    groups = {
        "q": (wq, 0, [(wq_hbm, 0)]),
        "kv": (wkv, 1, [(wk_hbm, 0), (wv_hbm, wkv.shape[-1] // 2)]),
        "o": (wo, 2, [(wo_hbm, 0)]),
        "g": (wg, 3, [(wg_hbm, 0)]),
        "u": (wu, 4, [(wu_hbm, 0)]),
    }

    full_o = {layers - 1} if pool == 4 else set()

    def skip(l, name):
        return l in full_o and name == "o"

    half_rows = wof.shape[3] // 2
    right, left = peer_id(peer(1)), peer_id(peer(zn - 1))

    def r_block(d, which=None):
        return wof.at[0, lax.rem(z + zn + d, zn), sub if which is None else which]

    def signed(d):
        return (d,) if d in (0, zh) else (d, -d)

    def of_own(l, d):
        if d == 0:
            wait_bytes(r_block(0), loc_sem.at[l, 2])
        elif d == zh:
            ring(l, zh)
        for b in signed(d):
            q = r_block(b)
            rcopy(q, q, of_send, of_recv.at[0, d], xnei).start()
            rcopy(q, q, of_send, of_recv.at[1, d], ynei).start()
            rcopy(q, q, of_send, of_sib, sib).start()

    def of_relay(l, d):
        for i, which, to in ((0, subx, ynei), (1, suby, xnei)):
            wait_bytes(wof.at[0, 0:len(signed(d)), 0], of_recv.at[i, d])
            for b in signed(d):
                q = r_block(b, which)
                if (b > 0 if i == 0 else b <= 0):
                    rcopy(q, q, of_send, of_recv.at[2, d], to).start()
                rcopy(q, q, of_send, of_sib, sib).start()

    def of_last(l, d):
        wait_bytes(wof.at[0, 0:len(signed(d)), 0], of_recv.at[2, d])
        for b in signed(d):
            q = r_block(b, subd)
            rcopy(q, q, of_send, of_sib, sib).start()

    def of_fin():
        wait_bytes(wof.at[0, :, 0:4], of_sib)

    def of_drain():
        wait_bytes(wof.at[0, :, 0:7], of_send)
        wait_bytes(wof.at[0, 0:zn - 1, 0], ring_send)

    def r_halves(d):
        blk = lax.rem(z + zn + d, zn)
        return wof.at[0, blk, sub, 0:half_rows], wof.at[0, blk, sub, half_rows:2 * half_rows]

    def ring(l, step):
        if step == 0:
            src = wo_hbm.at[l, pl.ds(pl.multiple_of(quarter * 2 * half_rows, 2 * half_rows), 2 * half_rows)]
            pltpu.make_async_copy(src, r_block(0), loc_sem.at[l, 2]).start()
            rcopy(src, r_block(0), ring_send, ring_recv.at[0, 0], right).start()
            rcopy(src, r_block(0), ring_send, ring_recv.at[1, 0], left).start()
        elif step < zh - 1:
            for i, d, to in ((0, -step, right), (1, step, left)):
                wait_bytes(r_block(d), ring_recv.at[i, step - 1])
                rcopy(r_block(d), r_block(d), ring_send, ring_recv.at[i, step], to).start()
        elif step == zh - 1:
            for i, d, to in ((0, -step, right), (1, step, left)):
                wait_bytes(r_block(d), ring_recv.at[i, step - 1])
                h = r_halves(d)[i]
                rcopy(h, h, ring_send, ring_recv.at[i, step], to).start()
        else:
            for i in range(2):
                wait_bytes(r_halves(zh)[i], ring_recv.at[i, zh - 1])

    direct = {(0, "q"), (0, "kv")} if pool == 4 else set()

    def pieces(l, name, zt, diag=False):
        buf, gi, srcs = groups[name]
        quart, to = (3 - quarter, subd) if diag else (quarter, sub)
        rows = buf.shape[3]
        out = []
        for src, off in srcs:
            width = src.shape[2] // zn
            s = src.at[l, pl.ds(pl.multiple_of(quart * rows, rows), rows), pl.ds(pl.multiple_of(zt * width, 128), width)]
            d = buf.at[l, z, to, :, pl.ds(off, width)]
            out.append((s, d))
        return out, gi

    def w_local(l, name):
        ps, gi = pieces(l, name, z)
        for s, d in ps:
            pltpu.make_async_copy(s, d, loc_sem.at[l, gi]).start()
        if (l, name) in direct:
            for s, d in pieces(l, name, z, True)[0]:
                pltpu.make_async_copy(s, d, diag_loc.at[l, gi]).start()

    def w_send(l, name):
        for r in order:
            zt = peer(r)
            ps, gi = pieces(l, name, zt)
            for s, d in ps:
                rcopy(s, d, z_send.at[l, gi], z_recv.at[l, gi], peer_id(zt)).start()

    def w_diag(l, name):
        if (l, name) in direct:
            for r in order:
                zt = peer(r)
                ps, gi = pieces(l, name, zt, True)
                for s, d in ps:
                    rcopy(s, d, diag_send.at[l, gi], diag_recv.at[l, gi], peer_id(zt)).start()

    def w_s1(l, name):
        buf, gi, _ = groups[name]
        buf = buf.at[l]
        wait_bytes(buf.at[0:zn - 1, 0], z_recv.at[l, gi])
        wait_bytes(buf.at[0, 0], loc_sem.at[l, gi])
        q = buf.at[:, sub]
        if pool == 4:
            rcopy(q, q, p_send.at[l, gi], p_recv.at[l, gi, 0], xnei).start()
            rcopy(q, q, p_send.at[l, gi], p_recv.at[l, gi, 1], ynei).start()
        rcopy(q, q, d_send.at[l, gi], d_recv.at[l, gi], sib).start()

    def w_s2(l, name):
        if pool == 4:
            buf, gi, _ = groups[name]
            buf = buf.at[l]
            qx, qy = buf.at[:, subx], buf.at[:, suby]
            hx, hy = buf.at[0:zh, subx], buf.at[zh:zn, suby]
            wait_bytes(qx, p_recv.at[l, gi, 0])
            if (l, name) not in direct:
                rcopy(hx, hx, p_send.at[l, gi], p_recv.at[l, gi, 2], ynei).start()
            rcopy(qx, qx, d_send.at[l, gi], d_recv.at[l, gi], sib).start()
            wait_bytes(qy, p_recv.at[l, gi, 1])
            if (l, name) not in direct:
                rcopy(hy, hy, p_send.at[l, gi], p_recv.at[l, gi, 3], xnei).start()
            rcopy(qy, qy, d_send.at[l, gi], d_recv.at[l, gi], sib).start()

    def w_s3(l, name):
        if pool == 4:
            buf, gi, _ = groups[name]
            buf = buf.at[l]
            q = buf.at[:, subd]
            if (l, name) in direct:
                wait_bytes(buf.at[0:zn - 1, 0], diag_recv.at[l, gi])
                wait_bytes(buf.at[0, 0], diag_loc.at[l, gi])
            else:
                wait_bytes(buf.at[0:zh, subd], p_recv.at[l, gi, 2])
                wait_bytes(buf.at[zh:zn, subd], p_recv.at[l, gi, 3])
            rcopy(q, q, d_send.at[l, gi], d_recv.at[l, gi], sib).start()

    def w_fin(l, name):
        buf, gi, _ = groups[name]
        buf = buf.at[l]
        wait_bytes(buf.at[:, 0:pool], d_recv.at[l, gi])

    def w_drain(l, name):
        buf, gi, _ = groups[name]
        buf = buf.at[l]
        wait_bytes(buf.at[0:zn - 1, 0], z_send.at[l, gi])
        wait_bytes(buf.at[:, 0:pool], d_send.at[l, gi])
        if (l, name) in direct:
            wait_bytes(buf.at[0:zn - 1, 0], diag_send.at[l, gi])
        if pool == 4:
            wait_bytes(buf.at[:, 0:2 if (l, name) in direct else 3], p_send.at[l, gi])

    def spread(src_of, dst, l, ph):
        for r in order:
            zt = peer(r)
            rcopy(src_of(zt), dst, a_send.at[l, ph], a_recv.at[l, ph], peer_id(zt)).start()

    def arrived(buf, l, ph):
        if l is None:
            wait_bytes(buf.at[0:zn - 1], a_recv.at[layers - 1, ph])
        else:
            wait_bytes(buf.at[l, 0:zn - 1], a_recv.at[l, ph])

    end = layers - 1
    plan = {
        (0, "entry"): [(w_send, 0, "q"), (w_send, 0, "kv"), (w_diag, 0, "q"), (w_diag, 0, "kv")],
        (0, "x_wait"): [(w_s1, 0, "q"), (w_s1, 0, "kv"), (w_send, 0, "o"), (w_send, 0, "g"), (w_s2, 0, "q"), (w_s3, 0, "q"), (w_s2, 0, "kv"), (w_s3, 0, "kv")],
        (0, "qkv_sent"): [(w_send, 0, "u"), (ring, end, 0), (w_s1, 0, "o"), (of_own, end, 0), (w_s1, 0, "g")],
        (0, "o_sent"): [(w_s2, 0, "o"), (w_s1, 0, "u"), (ring, end, 1), (w_s3, 0, "o"), (w_s2, 0, "g"), (of_own, end, 1), (of_relay, end, 0)],
        (0, "x1_sent"): [(w_s2, 0, "u"), (ring, end, 2), (w_send, 1, "q"), (w_send, 1, "kv"), (w_s3, 0, "g"), (of_own, end, 2), (w_s3, 0, "u"), (of_relay, end, 1)],
        (0, "y_sent"): [(ring, end, 3), (w_send, 1, "g"), (w_s1, 1, "q"), (w_s1, 1, "kv"), (of_own, end, 3), (of_relay, end, 2)],
        (1, "x_sent"): [(w_s2, 1, "q"), (w_s2, 1, "kv"), (w_send, 1, "u"), (of_own, end, zh), (of_relay, end, 3), (w_s3, 1, "q"), (w_s3, 1, "kv"), (of_last, end, 0), (of_last, end, 1), (w_s1, 1, "g")],
        (1, "qkv_sent"): [(of_relay, end, zh), (w_s1, 1, "u"), (of_last, end, 2), (w_s2, 1, "g"), (of_last, end, 3), (of_last, end, zh)],
        (1, "x1_sent"): [(w_s2, 1, "u"), (w_s3, 1, "g"), (w_s3, 1, "u")],
    } if full_o else {
        (0, "entry"): [(w_send, 0, "q"), (w_send, 0, "kv"), (w_send, 0, "o"), (w_send, 0, "g"), (w_send, 0, "u")],
        (0, "x_wait"): [(w_s1, 0, "q"), (w_s1, 0, "kv")],
        (0, "qkv_sent"): [(w_s1, 0, "o"), (w_send, 1, "q"), (w_send, 1, "kv"), (w_send, 1, "o")],
        (0, "o_sent"): [(w_s1, 0, "g"), (w_s1, 0, "u")],
        (0, "x1_sent"): [(w_send, 1, "g"), (w_send, 1, "u"), (w_s1, 1, "q"), (w_s1, 1, "kv")],
        (0, "y_sent"): [(w_s1, 1, "o")],
        (1, "qkv_sent"): [(w_s1, 1, "g"), (w_s1, 1, "u")],
    }

    def background(l, point):
        for fn, wl, name in plan.get((l, point), ()):
            fn(wl, name)

    smalls = [(x_hbm, xg.at[0, z]), (pos_hbm, pos_ref), (an_hbm, an_ref), (qn_hbm, qn_ref), (kn_hbm, kn_ref), (mn_hbm, mn_ref)]
    small_copies = [pltpu.make_async_copy(s, d, in_sem.at[i]) for i, (s, d) in enumerate(smalls)]
    for cp in small_copies:
        cp.start()
    for l in range(layers):
        pltpu.make_async_copy(wd_hbm.at[l], wd.at[l, c], down_loc.at[l, 0]).start()
        for name in ("q", "kv", "o", "g", "u"):
            if not skip(l, name):
                w_local(l, name)
        pltpu.make_async_copy(kc_hbm.at[l], kc.at[l], down_loc.at[l, 1]).start()
        pltpu.make_async_copy(vc_hbm.at[l], vc.at[l], down_loc.at[l, 2]).start()

    pl.semaphore_wait(barrier, zn + (2 if pool == 4 else 0))

    background(0, "entry")
    small_copies[0].wait()
    spread(lambda zt: xg.at[0, z], xg.at[0, z], 0, 0)
    for l in range(layers):
        rcopy(wd_hbm.at[l], wd.at[l, c], down_send.at[l], down_recv.at[l], sib).start()

    for cp in small_copies[1:]:
        cp.wait()
    row_id = lax.broadcasted_iota(jnp.int32, (tok, HEAD_DIM), 0)
    lane_id = lax.broadcasted_iota(jnp.int32, (tok, HEAD_DIM), 1)
    pos = jnp.zeros((tok, HEAD_DIM), jnp.int32)
    for n in range(tok):
        pos = jnp.where(row_id == n, pos_ref[n], pos)
    half = HEAD_DIM // 2
    pair = jnp.where(lane_id >= half, lane_id - half, lane_id).astype(F32)
    inv_freq = jnp.exp(pair * (-2.0 * math.log(ROPE_THETA) / HEAD_DIM))
    ang = pos.astype(F32) * inv_freq
    cs[...] = jnp.cos(ang)
    sin_tab = jnp.sin(ang)
    sn[...] = jnp.where(lane_id >= half, sin_tab, -sin_tab)

    outs = []

    def head_norm(v, gain):
        v = rms(v, HEAD_DIM) * gain
        return (v * cs[...] + pltpu.roll(v, half, 1) * sn[...]).astype(BF16).astype(F32)

    def gathered_x(l):
        return xg[l].astype(F32).reshape(nq, dm)

    def attention(l):
        qg = qn_ref[l:l + 1, :].astype(F32)
        kg = kn_ref[l:l + 1, :].astype(F32)
        for h in range(qh):
            v = qkvi[l, h // 2, :, (h % 2) * HEAD_DIM:(h % 2 + 1) * HEAD_DIM].astype(F32)
            qs[pl.ds(h, tok, stride=qh), :] = head_norm(v, qg)
        for h in range(kh):
            k = head_norm(qkvi[l, h, :, 2 * HEAD_DIM:3 * HEAD_DIM].astype(F32), kg)
            v = qkvi[l, h, :, 3 * HEAD_DIM:4 * HEAD_DIM].astype(F32)
            for g in range(2):
                ks[pl.ds(2 * h + g, tok, stride=qh), :] = k
                vs[pl.ds(2 * h + g, tok, stride=qh), :] = v
            kro[pl.ds(h, tok, stride=kh), :] = k
            vro[pl.ds(h, tok, stride=kh), :] = v
        krow_ref[l] = kro[...].astype(BF16)
        vrow_ref[l] = vro[...].astype(BF16)
        outs.append(pltpu.make_async_copy(krow_ref.at[l], res_hbm.at[1 + 2 * l], out_sem.at[1 + 2 * l]))
        outs.append(pltpu.make_async_copy(vrow_ref.at[l], res_hbm.at[2 + 2 * l], out_sem.at[2 + 2 * l]))
        outs[-2].start()
        outs[-1].start()
        cols = kc.shape[2]
        lane = lax.broadcasted_iota(jnp.int32, (qh, cols), 1)
        row = lax.broadcasted_iota(jnp.int32, (qh, cols), 0)
        mine = lax.rem(lane, kh) == lax.shift_right_logical(row, 1)
        slot = jnp.where(mine, lax.div(lane, kh), cols)
        scale = HEAD_DIM ** -0.5
        for n0 in range(0, tok, 4):
            seqs = range(n0, n0 + 4)
            rows = [slice(n * qh, (n + 1) * qh) for n in seqs]
            q = [qs[r, :] for r in rows]
            s = [lax.dot_general(a.astype(BF16), kc[l, n], (((1,), (1,)), ((), ())), preferred_element_type=F32) * scale for a, n in zip(q, seqs)]
            s_new = [jnp.sum(a * ks[r, :], axis=-1, keepdims=True) * scale for a, r in zip(q, rows)]
            s = [jnp.where(slot < pos_ref[n], a, NEG) for a, n in zip(s, seqs)]
            m = [jnp.maximum(jnp.max(a, axis=-1, keepdims=True), b) for a, b in zip(s, s_new)]
            e = [jnp.exp(a - b) for a, b in zip(s, m)]
            e_new = [jnp.exp(a - b) for a, b in zip(s_new, m)]
            inv = [1.0 / (jnp.sum(a, axis=-1, keepdims=True) + b) for a, b in zip(e, e_new)]
            p = [(a * b).astype(BF16) for a, b in zip(e, inv)]
            p_new = [(a * b).astype(BF16).astype(F32) for a, b in zip(e_new, inv)]
            for a, b, r, n in zip(p, p_new, rows, seqs):
                os_[r, :] = jnp.dot(a, vc[l, n], preferred_element_type=F32) + b * vs[r, :]
        for h in range(qh):
            og[l, z, :, h * HEAD_DIM:(h + 1) * HEAD_DIM] = os_[pl.ds(h, tok, stride=qh), :].astype(BF16)

    def own_rows(l):
        of_fin()
        r = jnp.dot(og[l, z], wof[0].reshape(og.shape[-1], dm), preferred_element_type=F32)
        x1r[z] = (xg[l, z].astype(F32) + r).astype(BF16)
        spread(lambda zt: x1r.at[z], x1r.at[z], l, 3)
        background(l, "x1_sent")
        wait_bytes(wd.at[l, 0], down_loc.at[l, 0])
        wait_bytes(wd.at[l, 0], down_recv.at[l])
        w_fin(l, "g")
        w_fin(l, "u")
        arrived(x1r, None, 3)
        return x1r[...].astype(F32).reshape(nq, dm)

    def gathered_rows(l):
        spread(lambda zt: og.at[l, z], og.at[l, z], l, 2)
        background(l, "o_sent")
        w_fin(l, "o")
        arrived(og, l, 2)
        o_all = og[l].astype(F32).reshape(nq, og.shape[-1]).astype(BF16)
        r = jnp.dot(o_all, wo[l].reshape(og.shape[-1], ctile), preferred_element_type=F32)
        xc = xg[l, :, :, pl.ds(pl.multiple_of(z * ctile, ctile), ctile)].astype(F32).reshape(nq, ctile)
        x1g[l, z] = (xc + r).astype(BF16)
        spread(lambda zt: x1g.at[l, z], x1g.at[l, z], l, 3)
        background(l, "x1_sent")
        wait_bytes(wd.at[l, 0], down_loc.at[l, 0])
        wait_bytes(wd.at[l, 0], down_recv.at[l])
        w_fin(l, "g")
        w_fin(l, "u")
        arrived(x1g, l, 3)
        background(l, "x1_in")
        return jnp.concatenate([x1g[l, zz].astype(F32) for zz in range(zn)], axis=-1)

    for l in range(layers):
        last = l == layers - 1
        background(l, "x_wait")
        arrived(xg, l, 0)
        h = (rms(gathered_x(l), dm) * an_ref[l:l + 1, :].astype(F32)).astype(BF16)
        background(l, "x_in")
        w_fin(l, "q")
        w_fin(l, "kv")
        for name, lo in (("q", 0), ("kv", wq.shape[-1])):
            buf = groups[name][0]
            cols = buf.shape[-1]
            r = jnp.dot(h, buf[l].reshape(dm, cols), preferred_element_type=F32)
            qkvs[l, :, :, lo:lo + cols] = r.reshape(zn, tok, cols).astype(BF16)
        spread(lambda zt: qkvs.at[l, zt], qkvi.at[l, z], l, 1)
        qkvi[l, z] = qkvs[l, z]
        background(l, "qkv_sent")
        if l == 0:
            for k in range(layers):
                wait_bytes(kc.at[k], down_loc.at[k, 1])
                wait_bytes(vc.at[k], down_loc.at[k, 2])
        arrived(qkvi, l, 1)
        background(l, "qkv_in")
        attention(l)
        x1 = own_rows(l) if l in full_o else gathered_rows(l)
        x1f[...] = x1
        h2 = (rms(x1, dm) * mn_ref[l:l + 1, :].astype(F32)).astype(BF16)
        ffc = wg.shape[-1]
        g = jnp.dot(h2, wg[l].reshape(dm, ffc), preferred_element_type=F32)
        u = jnp.dot(h2, wu[l].reshape(dm, ffc), preferred_element_type=F32)
        a = (g * jax.nn.sigmoid(g) * u).astype(BF16)
        pr = jnp.dot(a, wd[l].reshape(ffc, dm), preferred_element_type=F32)
        pbuf[l] = pr.reshape(zn, tok, dm)
        spread(lambda zt: pbuf.at[l, zt], ybuf.at[l, z], l, 4)
        ybuf[l, z] = pbuf[l, z]
        background(l, "y_sent")
        arrived(ybuf, l, 4)
        total = ybuf[l, 0]
        for zz in range(1, zn):
            total = total + ybuf[l, zz]
        y = x1f[pl.ds(pl.multiple_of(z * tok, tok), tok), :] + total
        if last:
            y_ref[...] = jnp.concatenate([y[:, t * HEAD_DIM:(t + 1) * HEAD_DIM] for t in range(dm // HEAD_DIM)], axis=0).astype(BF16)
            outs.append(pltpu.make_async_copy(y_ref, res_hbm.at[0], out_sem.at[0]))
            outs[-1].start()
        else:
            xg[l + 1, z] = y.astype(BF16)
            spread(lambda zt: xg.at[l + 1, z], xg.at[l + 1, z], l + 1, 0)
            background(l + 1, "x_sent")

    for l in range(layers):
        for name in groups:
            if not skip(l, name):
                w_drain(l, name)
        if l in full_o:
            of_drain()
        wait_bytes(wd.at[l, 0], down_send.at[l])
        for ph, buf in enumerate((xg, qkvi, og, x1g, ybuf)):
            if ph != 2 or l not in full_o:
                wait_bytes(buf.at[l, 0:zn - 1], a_send.at[l, ph])
    for cp in outs:
        cp.wait()


def place_rows(layers, tok, kh, pos_hbm, res_hbm, kin, vin, y_out, kout, vout, pos_ref, res, in_sem, y_sem, bulk_sem, row_sem):
    small = [pltpu.make_async_copy(pos_hbm, pos_ref, in_sem.at[0]), pltpu.make_async_copy(res_hbm.at[0:1 + 2 * layers], res, in_sem.at[1])]
    for cp in small:
        cp.start()
    pairs = ((kin, kout), (vin, vout))
    bulk = [[[pltpu.make_async_copy(src.at[l, n], dst.at[l, n], bulk_sem.at[i, l, n]) for n in range(tok)] for l in range(layers)] for i, (src, dst) in enumerate(pairs)]
    for l in range(layers):
        for n in range(tok):
            for i in range(2):
                bulk[i][l][n].start()
    for cp in small:
        cp.wait()
    done = [pltpu.make_async_copy(res.at[0, pl.ds(t * tok, tok)], y_out.at[:, pl.ds(t * HEAD_DIM, HEAD_DIM)], y_sem.at[t]) for t in range(y_out.shape[1] // HEAD_DIM)]
    for cp in done:
        cp.start()
    for l in range(layers):
        for n in range(tok):
            at = pl.ds(pl.multiple_of(pos_ref[n] * kh, kh), kh)
            for i, (_, dst) in enumerate(pairs):
                bulk[i][l][n].wait()
                cp = pltpu.make_async_copy(res.at[1 + 2 * l + i, pl.ds(n * kh, kh)], dst.at[l, n, at], row_sem.at[i, l, n])
                cp.start()
                done.append(cp)
    for cp in done:
        cp.wait()


def solution(mesh):
    batch_axes = ("part", "dp")
    act_spec = P(batch_axes, None)
    cache_spec = P(None, batch_axes, None, None, None)
    mat_spec = P(None, "dp", None)
    gain_spec = P(None, None)
    in_specs = (act_spec, P(batch_axes), cache_spec, cache_spec, gain_spec, mat_spec, mat_spec, mat_spec, gain_spec, gain_spec, mat_spec, gain_spec, mat_spec, mat_spec, mat_spec)
    out_specs = (act_spec, cache_spec, cache_spec)
    zn = mesh.shape["dp"] // 2
    ny = math.isqrt(mesh.shape["part"])
    pool = 4 if ny * ny == mesh.shape["part"] and ny % 2 == 0 else 1

    def device_fn(x, positions, k_cache, v_cache, attn_norm, w_q, w_k, w_v, q_norm, k_norm, w_o, mlp_norm, w_gate, w_up, w_down):
        layers, tok, slots, kh, hd = k_cache.shape
        dm = x.shape[1]
        qw, kw, ff = w_q.shape[2], w_k.shape[2], w_gate.shape[2]
        qh = qw // hd
        nq = 2 * pool
        qkvc = (qw + 2 * kw) // zn
        cfg = dict(layers=layers, zn=zn, pool=pool, ny=ny, tok=tok, qh=qh, kh=kh)
        hb = pl.BlockSpec(memory_space=pltpu.HBM)
        dma = pltpu.SemaphoreType.DMA
        flat = (layers, tok, slots * kh, hd)
        scratch = [
            pltpu.VMEM((layers, zn, nq, w_q.shape[1] // pool, qw // zn), BF16),
            pltpu.VMEM((layers, zn, nq, w_k.shape[1] // pool, 2 * kw // zn), BF16),
            pltpu.VMEM((layers, zn, nq, w_o.shape[1] // pool, dm // zn), BF16),
            pltpu.VMEM((1, zn, nq, w_o.shape[1] // pool, dm), BF16),
            pltpu.VMEM((layers, zn, nq, w_gate.shape[1] // pool, ff // zn), BF16),
            pltpu.VMEM((layers, zn, nq, w_up.shape[1] // pool, ff // zn), BF16),
            pltpu.VMEM((layers, 2, w_down.shape[1], dm), BF16),
            pltpu.VMEM(flat, BF16),
            pltpu.VMEM(flat, BF16),
            pltpu.VMEM((layers, zn, tok, dm), BF16),
            pltpu.VMEM((layers, zn, tok, qkvc), BF16),
            pltpu.VMEM((layers, zn, tok, qkvc), BF16),
            pltpu.VMEM((layers, zn, tok, qw), BF16),
            pltpu.VMEM((layers, zn, zn * tok, dm // zn), BF16),
            pltpu.VMEM((zn, tok, dm), BF16),
            pltpu.VMEM((layers, zn, tok, dm), F32),
            pltpu.VMEM((layers, zn, tok, dm), F32),
            pltpu.VMEM((zn * tok, dm), F32),
            pltpu.VMEM((tok * qh, hd), F32),
            pltpu.VMEM((tok * qh, hd), F32),
            pltpu.VMEM((tok * qh, hd), F32),
            pltpu.VMEM((tok * qh, hd), F32),
            pltpu.VMEM((tok * kh, hd), F32),
            pltpu.VMEM((tok * kh, hd), F32),
            pltpu.VMEM((tok, hd), F32),
            pltpu.VMEM((tok, hd), F32),
            pltpu.SMEM((tok,), jnp.int32),
            pltpu.VMEM((layers, dm), BF16),
            pltpu.VMEM((layers, hd), BF16),
            pltpu.VMEM((layers, hd), BF16),
            pltpu.VMEM((layers, dm), BF16),
            pltpu.VMEM((tok * kh, hd), BF16),
            pltpu.VMEM((layers, tok * kh, hd), BF16),
            pltpu.VMEM((layers, tok * kh, hd), BF16),
            dma((layers, 5)), dma((layers, 5)), dma((layers, 5)), dma((layers, 5)), dma((layers, 5)), dma((layers, 5, 4)),
            dma((layers, 5)), dma((layers, 5)), dma((layers,)), dma((layers,)), dma((layers, 5)), dma((layers, 3)), dma((6,)), dma((1 + 2 * layers,)), dma((1, 2)), dma((1, 2)), dma((1, 2)), dma, dma((2, zn // 2)), dma, dma((3, zn // 2 + 1)), dma,
        ]
        res = pl.pallas_call(
            functools.partial(decode_kernel, cfg),
            name="decode",
            out_shape=jax.ShapeDtypeStruct((RES_BLOCKS, tok * kh, hd), BF16),
            in_specs=[hb] * 15,
            out_specs=hb,
            scratch_shapes=scratch,
            compiler_params=pltpu.CompilerParams(collective_id=0, has_side_effects=True, vmem_limit_bytes=VMEM_LIMIT),
        )(positions, x, attn_norm, q_norm, k_norm, mlp_norm, w_q, w_k, w_v, w_o, w_gate, w_up, w_down, k_cache.reshape(flat), v_cache.reshape(flat))
        anys = pl.BlockSpec(memory_space=pl.ANY)
        rows = (1 + 2 * layers, tok * kh, hd)
        y, k_out, v_out = pl.pallas_call(
            functools.partial(place_rows, layers, tok, kh),
            name="place",
            out_shape=(jax.ShapeDtypeStruct((tok, dm), BF16), jax.ShapeDtypeStruct(flat, BF16), jax.ShapeDtypeStruct(flat, BF16)),
            in_specs=[anys] * 4,
            out_specs=(anys,) * 3,
            scratch_shapes=[pltpu.SMEM((tok,), jnp.int32), pltpu.VMEM(rows, BF16), dma((2,)), dma((dm // hd,)), dma((2, layers, tok)), dma((2, layers, tok))],
            compiler_params=pltpu.CompilerParams(vmem_limit_bytes=PLACE_LIMIT),
        )(positions, res, k_cache.reshape(flat), v_cache.reshape(flat))
        k_out = k_out.reshape(k_cache.shape)
        v_out = v_out.reshape(v_cache.shape)
        return y, k_out, v_out

    return jax.shard_map(device_fn, mesh=mesh, in_specs=in_specs, out_specs=out_specs, check_vma=False)
```

```python
import functools
import math

import jax
import jax.numpy as jnp
from jax import lax
from jax.experimental import pallas as pl
from jax.experimental.pallas import tpu as pltpu
from jax.sharding import PartitionSpec as P

HEAD_DIM = 128
RMS_EPS = 1e-6
ROPE_THETA = 1000000.0
VMEM_LIMIT = 58400000
PLACE_LIMIT = 8 * 1024 * 1024
RES_BLOCKS = 4096

MESH = pl.DeviceIdType.MESH
F32 = jnp.float32
BF16 = jnp.bfloat16
NEG = float("-inf")


def rms(values, width):
    return values * lax.rsqrt(jnp.sum(values * values, axis=-1, keepdims=True) * (1.0 / width) + RMS_EPS)


def decode_kernel(cfg, pos_hbm, x_hbm, an_hbm, qn_hbm, kn_hbm, mn_hbm, wq_hbm, wk_hbm, wv_hbm, wo_hbm, wg_hbm, wu_hbm, wd_hbm, kc_hbm, vc_hbm,
                  res_hbm,
                  wq, wkv, wo, wof, wg, wu, wd, kc, vc, xg, qkvs, qkvi, og, x1g, x1r, pbuf, ybuf, x1f, qs, ks, vs, os_, kro, vro, cs, sn, slot_ref, pos_ref, an_ref, qn_ref, kn_ref, mn_ref, y_ref, krow_ref, vrow_ref,
                  z_recv, d_recv, p_recv, a_recv, down_recv, loc_sem, down_loc, in_sem, out_sem, diag_recv, diag_loc, ring_recv, of_recv, of_sib, send_sem):
    layers, zn, pool, tok = cfg["layers"], cfg["zn"], cfg["pool"], cfg["tok"]
    qh, kh, ny = cfg["qh"], cfg["kh"], cfg["ny"]
    dm = x_hbm.shape[1]
    nq = zn * tok
    ctile = dm // zn
    zh = zn // 2
    idx = lax.axis_index("dp")
    z, c = idx // 2, idx % 2
    part = lax.axis_index("part")
    sib = {"dp": 2 * z + (1 - c)}
    if pool == 4:
        px, py = (part // ny) % 2, (part % ny) % 2
        xnei = {"part": part + ny * (1 - 2 * px)}
        ynei = {"part": part + 1 - 2 * py}
    else:
        px, py = 0, 0
    quarter = px * 2 + py
    sub = c * pool + quarter
    subx = c * pool + (1 - px) * 2 + py
    suby = c * pool + px * 2 + 1 - py
    subd = c * pool + (1 - px) * 2 + 1 - py

    order = []
    for r in range(zn // 2, 0, -1):
        order.append(r)
        if r != zn - r:
            order.append(zn - r)

    def peer(r):
        return lax.rem(z + r, zn)

    def peer_id(zt):
        return {"dp": 2 * zt + c}

    barrier = pltpu.get_barrier_semaphore()
    for r in order:
        pl.semaphore_signal(barrier, inc=1, device_id=peer_id(peer(r)), device_id_type=MESH)
    pl.semaphore_signal(barrier, inc=1, device_id=sib, device_id_type=MESH)
    if pool == 4:
        pl.semaphore_signal(barrier, inc=1, device_id=xnei, device_id_type=MESH)
        pl.semaphore_signal(barrier, inc=1, device_id=ynei, device_id_type=MESH)

    sent = []

    def rcopy(src, dst, ss, rs, dev):
        sent.append(math.prod(src.shape) * src.dtype.itemsize)
        return pltpu.make_async_remote_copy(src_ref=src, dst_ref=dst, send_sem=ss, recv_sem=rs, device_id=dev, device_id_type=MESH)

    def wait_bytes(ref, sem):
        pltpu.make_async_copy(ref, ref, sem).wait()

    groups = {
        "q": (wq, 0, [(wq_hbm, 0)]),
        "kv": (wkv, 1, [(wk_hbm, 0), (wv_hbm, wkv.shape[-1] // 2)]),
        "o": (wo, 2, [(wo_hbm, 0)]),
        "g": (wg, 3, [(wg_hbm, 0)]),
        "u": (wu, 4, [(wu_hbm, 0)]),
    }

    full_o = {layers - 1} if pool == 4 else set()

    def skip(l, name):
        return l in full_o and name == "o"

    half_rows = wof.shape[3] // 2
    right, left = peer_id(peer(1)), peer_id(peer(zn - 1))

    def r_block(d, which=None):
        return wof.at[0, lax.rem(z + zn + d, zn), sub if which is None else which]

    def signed(d):
        return (d,) if d in (0, zh) else (d, -d)

    def of_own(l, d):
        if d == 0:
            wait_bytes(r_block(0), loc_sem.at[l, 2])
        elif d == zh:
            ring(l, zh)
        for b in signed(d):
            q = r_block(b)
            rcopy(q, q, send_sem, of_recv.at[0, d], xnei).start()
            rcopy(q, q, send_sem, of_recv.at[0, d], ynei).start()
            rcopy(q, q, send_sem, of_sib, sib).start()

    def of_relay(l, d):
        wait_bytes(wof.at[0, 0:len(signed(d)), 0:2], of_recv.at[0, d])
        for i, which, to in ((0, subx, ynei), (1, suby, xnei)):
            for b in signed(d):
                q = r_block(b, which)
                if (b > 0 if i == 0 else b <= 0):
                    rcopy(q, q, send_sem, of_recv.at[1, d], to).start()
                rcopy(q, q, send_sem, of_sib, sib).start()

    def of_last(l, d):
        wait_bytes(wof.at[0, 0:len(signed(d)), 0], of_recv.at[1, d])
        for b in signed(d):
            q = r_block(b, subd)
            rcopy(q, q, send_sem, of_sib, sib).start()

    def of_fin():
        wait_bytes(wof.at[0, :, 0:4], of_sib)

    def r_halves(d):
        blk = lax.rem(z + zn + d, zn)
        return wof.at[0, blk, sub, 0:half_rows], wof.at[0, blk, sub, half_rows:2 * half_rows]

    def ring(l, step):
        if step == 0:
            src = wo_hbm.at[l, pl.ds(pl.multiple_of(quarter * 2 * half_rows, 2 * half_rows), 2 * half_rows)]
            pltpu.make_async_copy(src, r_block(0), loc_sem.at[l, 2]).start()
            rcopy(src, r_block(0), send_sem, ring_recv.at[0, 0], right).start()
            rcopy(src, r_block(0), send_sem, ring_recv.at[1, 0], left).start()
        elif step < zh - 1:
            for i, d, to in ((0, -step, right), (1, step, left)):
                wait_bytes(r_block(d), ring_recv.at[i, step - 1])
                rcopy(r_block(d), r_block(d), send_sem, ring_recv.at[i, step], to).start()
        elif step == zh - 1:
            for i, d, to in ((0, -step, right), (1, step, left)):
                wait_bytes(r_block(d), ring_recv.at[i, step - 1])
                h = r_halves(d)[i]
                rcopy(h, h, send_sem, ring_recv.at[i, step], to).start()
        else:
            for i in range(2):
                wait_bytes(r_halves(zh)[i], ring_recv.at[i, zh - 1])

    direct = {(0, "q"), (0, "kv")} if pool == 4 else set()

    def pieces(l, name, zt, diag=False):
        buf, gi, srcs = groups[name]
        quart, to = (3 - quarter, subd) if diag else (quarter, sub)
        rows = buf.shape[3]
        out = []
        for src, off in srcs:
            width = src.shape[2] // zn
            s = src.at[l, pl.ds(pl.multiple_of(quart * rows, rows), rows), pl.ds(pl.multiple_of(zt * width, 128), width)]
            d = buf.at[l, z, to, :, pl.ds(off, width)]
            out.append((s, d))
        return out, gi

    def w_local(l, name):
        ps, gi = pieces(l, name, z)
        for s, d in ps:
            pltpu.make_async_copy(s, d, loc_sem.at[l, gi]).start()
        if (l, name) in direct:
            for s, d in pieces(l, name, z, True)[0]:
                pltpu.make_async_copy(s, d, diag_loc.at[l, gi]).start()

    def w_send(l, name):
        for r in order:
            zt = peer(r)
            ps, gi = pieces(l, name, zt)
            for s, d in ps:
                rcopy(s, d, send_sem, z_recv.at[l, gi], peer_id(zt)).start()

    def w_diag(l, name):
        if (l, name) in direct:
            for r in order:
                zt = peer(r)
                ps, gi = pieces(l, name, zt, True)
                for s, d in ps:
                    rcopy(s, d, send_sem, diag_recv.at[l, gi], peer_id(zt)).start()

    def w_s1(l, name):
        buf, gi, _ = groups[name]
        buf = buf.at[l]
        wait_bytes(buf.at[0:zn - 1, 0], z_recv.at[l, gi])
        wait_bytes(buf.at[0, 0], loc_sem.at[l, gi])
        q = buf.at[:, sub]
        if pool == 4:
            rcopy(q, q, send_sem, p_recv.at[l, gi, 0], xnei).start()
            rcopy(q, q, send_sem, p_recv.at[l, gi, 0], ynei).start()
        rcopy(q, q, send_sem, d_recv.at[l, gi], sib).start()

    def w_s2(l, name):
        if pool == 4:
            buf, gi, _ = groups[name]
            buf = buf.at[l]
            qx, qy = buf.at[:, subx], buf.at[:, suby]
            hx, hy = buf.at[0:zh, subx], buf.at[zh:zn, suby]
            wait_bytes(buf.at[:, 0:2], p_recv.at[l, gi, 0])
            if (l, name) not in direct:
                rcopy(hx, hx, send_sem, p_recv.at[l, gi, 1], ynei).start()
                rcopy(hy, hy, send_sem, p_recv.at[l, gi, 1], xnei).start()
            rcopy(qx, qx, send_sem, d_recv.at[l, gi], sib).start()
            rcopy(qy, qy, send_sem, d_recv.at[l, gi], sib).start()

    def w_s3(l, name):
        if pool == 4:
            buf, gi, _ = groups[name]
            buf = buf.at[l]
            q = buf.at[:, subd]
            if (l, name) in direct:
                wait_bytes(buf.at[0:zn - 1, 0], diag_recv.at[l, gi])
                wait_bytes(buf.at[0, 0], diag_loc.at[l, gi])
            else:
                wait_bytes(buf.at[:, subd], p_recv.at[l, gi, 1])
            rcopy(q, q, send_sem, d_recv.at[l, gi], sib).start()

    def w_fin(l, name):
        buf, gi, _ = groups[name]
        buf = buf.at[l]
        wait_bytes(buf.at[:, 0:pool], d_recv.at[l, gi])

    def spread(src_of, dst, l, ph):
        for r in order:
            zt = peer(r)
            rcopy(src_of(zt), dst, send_sem, a_recv.at[l, ph], peer_id(zt)).start()

    def arrived(buf, l, ph):
        if l is None:
            wait_bytes(buf.at[0:zn - 1], a_recv.at[layers - 1, ph])
        else:
            wait_bytes(buf.at[l, 0:zn - 1], a_recv.at[l, ph])

    end = layers - 1
    plan = {
        (0, "entry"): [(w_send, 0, "q"), (w_send, 0, "kv"), (w_diag, 0, "q"), (w_diag, 0, "kv")],
        (0, "x_wait"): [(w_s1, 0, "q"), (w_s1, 0, "kv"), (w_send, 0, "o"), (w_send, 0, "g"), (w_s2, 0, "q"), (w_s3, 0, "q"), (w_s2, 0, "kv"), (w_s3, 0, "kv")],
        (0, "qkv_sent"): [(w_send, 0, "u"), (ring, end, 0), (w_s1, 0, "o"), (of_own, end, 0), (w_s1, 0, "g")],
        (0, "o_sent"): [(w_s2, 0, "o"), (w_s1, 0, "u"), (ring, end, 1), (w_s3, 0, "o"), (w_s2, 0, "g"), (of_own, end, 1), (of_relay, end, 0)],
        (0, "x1_sent"): [(w_s2, 0, "u"), (ring, end, 2), (w_send, 1, "q"), (w_send, 1, "kv"), (w_s3, 0, "g"), (of_own, end, 2), (w_s3, 0, "u"), (of_relay, end, 1)],
        (0, "y_sent"): [(ring, end, 3), (w_send, 1, "g"), (w_s1, 1, "q"), (w_s1, 1, "kv"), (of_own, end, 3), (of_relay, end, 2)],
        (1, "x_sent"): [(w_s2, 1, "q"), (w_s2, 1, "kv"), (w_send, 1, "u"), (of_own, end, zh), (of_relay, end, 3), (w_s3, 1, "q"), (w_s3, 1, "kv"), (of_last, end, 0), (of_last, end, 1), (w_s1, 1, "g")],
        (1, "qkv_sent"): [(of_relay, end, zh), (w_s1, 1, "u"), (of_last, end, 2), (w_s2, 1, "g"), (of_last, end, 3), (of_last, end, zh)],
        (1, "x1_sent"): [(w_s2, 1, "u"), (w_s3, 1, "g"), (w_s3, 1, "u")],
    } if full_o else {
        (0, "entry"): [(w_send, 0, "q"), (w_send, 0, "kv"), (w_send, 0, "o"), (w_send, 0, "g"), (w_send, 0, "u")],
        (0, "x_wait"): [(w_s1, 0, "q"), (w_s1, 0, "kv")],
        (0, "qkv_sent"): [(w_s1, 0, "o"), (w_send, 1, "q"), (w_send, 1, "kv"), (w_send, 1, "o")],
        (0, "o_sent"): [(w_s1, 0, "g"), (w_s1, 0, "u")],
        (0, "x1_sent"): [(w_send, 1, "g"), (w_send, 1, "u"), (w_s1, 1, "q"), (w_s1, 1, "kv")],
        (0, "y_sent"): [(w_s1, 1, "o")],
        (1, "qkv_sent"): [(w_s1, 1, "g"), (w_s1, 1, "u")],
    }

    def background(l, point):
        for fn, wl, name in plan.get((l, point), ()):
            fn(wl, name)

    smalls = [(x_hbm, xg.at[0, z]), (pos_hbm, pos_ref), (an_hbm, an_ref), (qn_hbm, qn_ref), (kn_hbm, kn_ref), (mn_hbm, mn_ref)]
    small_copies = [pltpu.make_async_copy(s, d, in_sem.at[i]) for i, (s, d) in enumerate(smalls)]
    for cp in small_copies:
        cp.start()
    for l in range(layers):
        pltpu.make_async_copy(wd_hbm.at[l], wd.at[l, c], down_loc.at[l, 0]).start()
        for name in ("q", "kv", "o", "g", "u"):
            if not skip(l, name):
                w_local(l, name)
        pltpu.make_async_copy(kc_hbm.at[l], kc.at[l], down_loc.at[l, 1]).start()
        pltpu.make_async_copy(vc_hbm.at[l], vc.at[l], down_loc.at[l, 2]).start()

    cols = kc.shape[2]
    lane = lax.broadcasted_iota(jnp.int32, (qh, cols), 1)
    row = lax.broadcasted_iota(jnp.int32, (qh, cols), 0)
    mine = lax.rem(lane, kh) == lax.shift_right_logical(row, 1)
    slot_ref[...] = jnp.where(mine, lax.div(lane, kh), cols)

    pl.semaphore_wait(barrier, zn + (2 if pool == 4 else 0))

    background(0, "entry")
    small_copies[0].wait()
    spread(lambda zt: xg.at[0, z], xg.at[0, z], 0, 0)
    for l in range(layers):
        rcopy(wd_hbm.at[l], wd.at[l, c], send_sem, down_recv.at[l], sib).start()

    for cp in small_copies[1:]:
        cp.wait()
    row_id = lax.broadcasted_iota(jnp.int32, (tok, HEAD_DIM), 0)
    lane_id = lax.broadcasted_iota(jnp.int32, (tok, HEAD_DIM), 1)
    pos = jnp.zeros((tok, HEAD_DIM), jnp.int32)
    for n in range(tok):
        pos = jnp.where(row_id == n, pos_ref[n], pos)
    half = HEAD_DIM // 2
    pair = jnp.where(lane_id >= half, lane_id - half, lane_id).astype(F32)
    inv_freq = jnp.exp(pair * (-2.0 * math.log(ROPE_THETA) / HEAD_DIM))
    ang = pos.astype(F32) * inv_freq
    cs[...] = jnp.cos(ang)
    sin_tab = jnp.sin(ang)
    sn[...] = jnp.where(lane_id >= half, sin_tab, -sin_tab)

    outs = []

    def head_norm(v, gain):
        v = rms(v, HEAD_DIM) * gain
        return (v * cs[...] + pltpu.roll(v, half, 1) * sn[...]).astype(BF16).astype(F32)

    def gathered_x(l):
        return xg[l].astype(F32).reshape(nq, dm)

    def attention(l):
        qg = qn_ref[l:l + 1, :].astype(F32)
        kg = kn_ref[l:l + 1, :].astype(F32)
        for h in range(qh):
            v = qkvi[l, h // 2, :, (h % 2) * HEAD_DIM:(h % 2 + 1) * HEAD_DIM].astype(F32)
            qs[pl.ds(h, tok, stride=qh), :] = head_norm(v, qg)
        for h in range(kh):
            k = head_norm(qkvi[l, h, :, 2 * HEAD_DIM:3 * HEAD_DIM].astype(F32), kg)
            v = qkvi[l, h, :, 3 * HEAD_DIM:4 * HEAD_DIM].astype(F32)
            for g in range(2):
                ks[pl.ds(2 * h + g, tok, stride=qh), :] = k
                vs[pl.ds(2 * h + g, tok, stride=qh), :] = v
            kro[pl.ds(h, tok, stride=kh), :] = k
            vro[pl.ds(h, tok, stride=kh), :] = v
        krow_ref[l] = kro[...].astype(BF16)
        vrow_ref[l] = vro[...].astype(BF16)
        outs.append(pltpu.make_async_copy(krow_ref.at[l], res_hbm.at[1 + 2 * l], out_sem))
        outs.append(pltpu.make_async_copy(vrow_ref.at[l], res_hbm.at[2 + 2 * l], out_sem))
        outs[-2].start()
        outs[-1].start()
        slot = slot_ref[...]
        scale = HEAD_DIM ** -0.5
        for n0 in range(0, tok, 8):
            seqs = range(n0, n0 + 8)
            rows = [slice(n * qh, (n + 1) * qh) for n in seqs]
            q = [qs[r, :] for r in rows]
            s = [lax.dot_general(a.astype(BF16), kc[l, n], (((1,), (1,)), ((), ())), preferred_element_type=F32) * scale for a, n in zip(q, seqs)]
            s_new = [jnp.sum(a * ks[r, :], axis=-1, keepdims=True) * scale for a, r in zip(q, rows)]
            s = [jnp.where(slot < pos_ref[n], a, NEG) for a, n in zip(s, seqs)]
            m = [jnp.maximum(jnp.max(a, axis=-1, keepdims=True), b) for a, b in zip(s, s_new)]
            e = [jnp.exp(a - b) for a, b in zip(s, m)]
            e_new = [jnp.exp(a - b) for a, b in zip(s_new, m)]
            inv = [1.0 / (jnp.sum(a, axis=-1, keepdims=True) + b) for a, b in zip(e, e_new)]
            p = [(a * b).astype(BF16) for a, b in zip(e, inv)]
            p_new = [(a * b).astype(BF16).astype(F32) for a, b in zip(e_new, inv)]
            for a, b, r, n in zip(p, p_new, rows, seqs):
                os_[r, :] = jnp.dot(a, vc[l, n], preferred_element_type=F32) + b * vs[r, :]
        for h in range(qh):
            og[l, z, :, h * HEAD_DIM:(h + 1) * HEAD_DIM] = os_[pl.ds(h, tok, stride=qh), :].astype(BF16)

    def own_rows(l):
        of_fin()
        r = jnp.dot(og[l, z], wof[0].reshape(og.shape[-1], dm), preferred_element_type=F32)
        x1r[z] = (xg[l, z].astype(F32) + r).astype(BF16)
        spread(lambda zt: x1r.at[z], x1r.at[z], l, 3)
        background(l, "x1_sent")
        wait_bytes(wd.at[l, 0], down_loc.at[l, 0])
        wait_bytes(wd.at[l, 0], down_recv.at[l])
        w_fin(l, "g")
        w_fin(l, "u")
        arrived(x1r, None, 3)
        return x1r[...].astype(F32).reshape(nq, dm)

    def gathered_rows(l):
        spread(lambda zt: og.at[l, z], og.at[l, z], l, 2)
        background(l, "o_sent")
        w_fin(l, "o")
        arrived(og, l, 2)
        o_all = og[l].astype(F32).reshape(nq, og.shape[-1]).astype(BF16)
        r = jnp.dot(o_all, wo[l].reshape(og.shape[-1], ctile), preferred_element_type=F32)
        xc = xg[l, :, :, pl.ds(pl.multiple_of(z * ctile, ctile), ctile)].astype(F32).reshape(nq, ctile)
        x1g[l, z] = (xc + r).astype(BF16)
        spread(lambda zt: x1g.at[l, z], x1g.at[l, z], l, 3)
        background(l, "x1_sent")
        wait_bytes(wd.at[l, 0], down_loc.at[l, 0])
        wait_bytes(wd.at[l, 0], down_recv.at[l])
        w_fin(l, "g")
        w_fin(l, "u")
        arrived(x1g, l, 3)
        background(l, "x1_in")
        return jnp.concatenate([x1g[l, zz].astype(F32) for zz in range(zn)], axis=-1)

    for l in range(layers):
        last = l == layers - 1
        background(l, "x_wait")
        arrived(xg, l, 0)
        h = (rms(gathered_x(l), dm) * an_ref[l:l + 1, :].astype(F32)).astype(BF16)
        background(l, "x_in")
        w_fin(l, "q")
        w_fin(l, "kv")
        for name, lo in (("q", 0), ("kv", wq.shape[-1])):
            buf = groups[name][0]
            cols = buf.shape[-1]
            r = jnp.dot(h, buf[l].reshape(dm, cols), preferred_element_type=F32)
            qkvs[l, :, :, lo:lo + cols] = r.reshape(zn, tok, cols).astype(BF16)
        spread(lambda zt: qkvs.at[l, zt], qkvi.at[l, z], l, 1)
        qkvi[l, z] = qkvs[l, z]
        background(l, "qkv_sent")
        if l == 0:
            for k in range(layers):
                wait_bytes(kc.at[k], down_loc.at[k, 1])
                wait_bytes(vc.at[k], down_loc.at[k, 2])
        arrived(qkvi, l, 1)
        background(l, "qkv_in")
        attention(l)
        x1 = own_rows(l) if l in full_o else gathered_rows(l)
        x1f[...] = x1
        h2 = (rms(x1, dm) * mn_ref[l:l + 1, :].astype(F32)).astype(BF16)
        ffc = wg.shape[-1]
        g = jnp.dot(h2, wg[l].reshape(dm, ffc), preferred_element_type=F32)
        u = jnp.dot(h2, wu[l].reshape(dm, ffc), preferred_element_type=F32)
        a = (g * jax.nn.sigmoid(g) * u).astype(BF16)
        pr = jnp.dot(a, wd[l].reshape(ffc, dm), preferred_element_type=F32)
        pbuf[l] = pr.reshape(zn, tok, dm)
        spread(lambda zt: pbuf.at[l, zt], ybuf.at[l, z], l, 4)
        ybuf[l, z] = pbuf[l, z]
        background(l, "y_sent")
        arrived(ybuf, l, 4)
        total = ybuf[l, 0]
        for zz in range(1, zn):
            total = total + ybuf[l, zz]
        y = x1f[pl.ds(pl.multiple_of(z * tok, tok), tok), :] + total
        if last:
            y_ref[...] = jnp.concatenate([y[:, t * HEAD_DIM:(t + 1) * HEAD_DIM] for t in range(dm // HEAD_DIM)], axis=0).astype(BF16)
            outs.append(pltpu.make_async_copy(y_ref, res_hbm.at[0], out_sem))
            outs[-1].start()
        else:
            xg[l + 1, z] = y.astype(BF16)
            spread(lambda zt: xg.at[l + 1, z], xg.at[l + 1, z], l + 1, 0)
            background(l + 1, "x_sent")

    rows = sum(sent) // (res_hbm.shape[2] * 2)
    part_rows = math.gcd(rows, res_hbm.shape[1])
    wait_bytes(res_hbm.at[0:rows // part_rows, 0:part_rows], send_sem)
    wait_bytes(res_hbm.at[0:len(outs)], out_sem)


def place_rows(layers, tok, kh, pos_hbm, res_hbm, kin, vin, y_out, kout, vout, pos_ref, res, in_sem, y_sem, bulk_sem, row_sem):
    small = [pltpu.make_async_copy(pos_hbm, pos_ref, in_sem.at[0]), pltpu.make_async_copy(res_hbm.at[0:1 + 2 * layers], res, in_sem.at[1])]
    for cp in small:
        cp.start()
    pairs = ((kin, kout), (vin, vout))
    bulk = [[[pltpu.make_async_copy(src.at[l, n], dst.at[l, n], bulk_sem.at[i, l, n]) for n in range(tok)] for l in range(layers)] for i, (src, dst) in enumerate(pairs)]
    for l in range(layers):
        for n in range(tok):
            for i in range(2):
                bulk[i][l][n].start()
    for cp in small:
        cp.wait()
    done = [pltpu.make_async_copy(res.at[0, pl.ds(t * tok, tok)], y_out.at[:, pl.ds(t * HEAD_DIM, HEAD_DIM)], y_sem.at[t]) for t in range(y_out.shape[1] // HEAD_DIM)]
    for cp in done:
        cp.start()
    for l in range(layers):
        for n in range(tok):
            at = pl.ds(pl.multiple_of(pos_ref[n] * kh, kh), kh)
            for i, (_, dst) in enumerate(pairs):
                bulk[i][l][n].wait()
                cp = pltpu.make_async_copy(res.at[1 + 2 * l + i, pl.ds(n * kh, kh)], dst.at[l, n, at], row_sem.at[i, l, n])
                cp.start()
                done.append(cp)
    for cp in done:
        cp.wait()


def solution(mesh):
    batch_axes = ("part", "dp")
    act_spec = P(batch_axes, None)
    cache_spec = P(None, batch_axes, None, None, None)
    mat_spec = P(None, "dp", None)
    gain_spec = P(None, None)
    in_specs = (act_spec, P(batch_axes), cache_spec, cache_spec, gain_spec, mat_spec, mat_spec, mat_spec, gain_spec, gain_spec, mat_spec, gain_spec, mat_spec, mat_spec, mat_spec)
    out_specs = (act_spec, cache_spec, cache_spec)
    zn = mesh.shape["dp"] // 2
    ny = math.isqrt(mesh.shape["part"])
    pool = 4 if ny * ny == mesh.shape["part"] and ny % 2 == 0 else 1

    def device_fn(x, positions, k_cache, v_cache, attn_norm, w_q, w_k, w_v, q_norm, k_norm, w_o, mlp_norm, w_gate, w_up, w_down):
        layers, tok, slots, kh, hd = k_cache.shape
        dm = x.shape[1]
        qw, kw, ff = w_q.shape[2], w_k.shape[2], w_gate.shape[2]
        qh = qw // hd
        nq = 2 * pool
        qkvc = (qw + 2 * kw) // zn
        cfg = dict(layers=layers, zn=zn, pool=pool, ny=ny, tok=tok, qh=qh, kh=kh)
        hb = pl.BlockSpec(memory_space=pltpu.HBM)
        dma = pltpu.SemaphoreType.DMA
        flat = (layers, tok, slots * kh, hd)
        scratch = [
            pltpu.VMEM((layers, zn, nq, w_q.shape[1] // pool, qw // zn), BF16),
            pltpu.VMEM((layers, zn, nq, w_k.shape[1] // pool, 2 * kw // zn), BF16),
            pltpu.VMEM((layers, zn, nq, w_o.shape[1] // pool, dm // zn), BF16),
            pltpu.VMEM((1, zn, nq, w_o.shape[1] // pool, dm), BF16),
            pltpu.VMEM((layers, zn, nq, w_gate.shape[1] // pool, ff // zn), BF16),
            pltpu.VMEM((layers, zn, nq, w_up.shape[1] // pool, ff // zn), BF16),
            pltpu.VMEM((layers, 2, w_down.shape[1], dm), BF16),
            pltpu.VMEM(flat, BF16),
            pltpu.VMEM(flat, BF16),
            pltpu.VMEM((layers, zn, tok, dm), BF16),
            pltpu.VMEM((layers, zn, tok, qkvc), BF16),
            pltpu.VMEM((layers, zn, tok, qkvc), BF16),
            pltpu.VMEM((layers, zn, tok, qw), BF16),
            pltpu.VMEM((layers, zn, zn * tok, dm // zn), BF16),
            pltpu.VMEM((zn, tok, dm), BF16),
            pltpu.VMEM((layers, zn, tok, dm), F32),
            pltpu.VMEM((layers, zn, tok, dm), F32),
            pltpu.VMEM((zn * tok, dm), F32),
            pltpu.VMEM((tok * qh, hd), F32),
            pltpu.VMEM((tok * qh, hd), F32),
            pltpu.VMEM((tok * qh, hd), F32),
            pltpu.VMEM((tok * qh, hd), F32),
            pltpu.VMEM((tok * kh, hd), F32),
            pltpu.VMEM((tok * kh, hd), F32),
            pltpu.VMEM((tok, hd), F32),
            pltpu.VMEM((tok, hd), F32),
            pltpu.VMEM((qh, slots * kh), jnp.int32),
            pltpu.SMEM((tok,), jnp.int32),
            pltpu.VMEM((layers, dm), BF16),
            pltpu.VMEM((layers, hd), BF16),
            pltpu.VMEM((layers, hd), BF16),
            pltpu.VMEM((layers, dm), BF16),
            pltpu.VMEM((tok * kh, hd), BF16),
            pltpu.VMEM((layers, tok * kh, hd), BF16),
            pltpu.VMEM((layers, tok * kh, hd), BF16),
            dma((layers, 5)), dma((layers, 5)), dma((layers, 5, 2)), dma((layers, 5)), dma((layers,)), dma((layers, 5)), dma((layers, 3)), dma((6,)), dma,
            dma((1, 2)), dma((1, 2)), dma((2, zn // 2)), dma((2, zn // 2 + 1)), dma, dma,
        ]
        res = pl.pallas_call(
            functools.partial(decode_kernel, cfg),
            name="decode",
            out_shape=jax.ShapeDtypeStruct((RES_BLOCKS, tok * kh, hd), BF16),
            in_specs=[hb] * 15,
            out_specs=hb,
            scratch_shapes=scratch,
            compiler_params=pltpu.CompilerParams(collective_id=0, has_side_effects=True, vmem_limit_bytes=VMEM_LIMIT),
        )(positions, x, attn_norm, q_norm, k_norm, mlp_norm, w_q, w_k, w_v, w_o, w_gate, w_up, w_down, k_cache.reshape(flat), v_cache.reshape(flat))
        anys = pl.BlockSpec(memory_space=pl.ANY)
        rows = (1 + 2 * layers, tok * kh, hd)
        y, k_out, v_out = pl.pallas_call(
            functools.partial(place_rows, layers, tok, kh),
            name="place",
            out_shape=(jax.ShapeDtypeStruct((tok, dm), BF16), jax.ShapeDtypeStruct(flat, BF16), jax.ShapeDtypeStruct(flat, BF16)),
            in_specs=[anys] * 4,
            out_specs=(anys,) * 3,
            scratch_shapes=[pltpu.SMEM((tok,), jnp.int32), pltpu.VMEM(rows, BF16), dma((2,)), dma((dm // hd,)), dma((2, layers, tok)), dma((2, layers, tok))],
            compiler_params=pltpu.CompilerParams(vmem_limit_bytes=PLACE_LIMIT),
        )(positions, res, k_cache.reshape(flat), v_cache.reshape(flat))
        k_out = k_out.reshape(k_cache.shape)
        v_out = v_out.reshape(v_cache.shape)
        return y, k_out, v_out

    return jax.shard_map(device_fn, mesh=mesh, in_specs=in_specs, out_specs=out_specs, check_vma=False)
```

```python
import functools
import math

import jax
import jax.numpy as jnp
from jax import lax
from jax.experimental import pallas as pl
from jax.experimental.pallas import tpu as pltpu
from jax.sharding import PartitionSpec as P

HEAD_DIM = 128
RMS_EPS = 1e-6
ROPE_THETA = 1000000.0
VMEM_LIMIT = 58400000
PLACE_LIMIT = 8 * 1024 * 1024
RES_BLOCKS = 4096

MESH = pl.DeviceIdType.MESH
F32 = jnp.float32
BF16 = jnp.bfloat16
NEG = float("-inf")


def rms(values, width):
    return values * lax.rsqrt(jnp.sum(values * values, axis=-1, keepdims=True) * (1.0 / width) + RMS_EPS)


def decode_kernel(cfg, pos_hbm, x_hbm, an_hbm, qn_hbm, kn_hbm, mn_hbm, wq_hbm, wk_hbm, wv_hbm, wo_hbm, wg_hbm, wu_hbm, wd_hbm, kc_hbm, vc_hbm,
                  res_hbm,
                  wq, wkv, wo, wof, wg, wu, wd, kc, vc, xg, qkvs, qkvi, og, x1g, x1r, pbuf, ybuf, x1f, qs, ks, vs, os_, kro, vro, cs, sn, slot_ref, pos_ref, an_ref, qn_ref, kn_ref, mn_ref, y_ref, krow_ref, vrow_ref,
                  z_recv, d_recv, p_recv, a_recv, down_recv, of_loc, cache_sem, in_sem, out_sem, diag_recv, ring_recv, of_recv, of_sib, send_sem):
    layers, zn, pool, tok = cfg["layers"], cfg["zn"], cfg["pool"], cfg["tok"]
    qh, kh, ny = cfg["qh"], cfg["kh"], cfg["ny"]
    dm = x_hbm.shape[1]
    nq = zn * tok
    ctile = dm // zn
    zh = zn // 2
    idx = lax.axis_index("dp")
    z, c = idx // 2, idx % 2
    part = lax.axis_index("part")
    sib = {"dp": 2 * z + (1 - c)}
    if pool == 4:
        px, py = (part // ny) % 2, (part % ny) % 2
        xnei = {"part": part + ny * (1 - 2 * px)}
        ynei = {"part": part + 1 - 2 * py}
    else:
        px, py = 0, 0
    quarter = px * 2 + py
    sub = c * pool + quarter
    subx = c * pool + (1 - px) * 2 + py
    suby = c * pool + px * 2 + 1 - py
    subd = c * pool + (1 - px) * 2 + 1 - py

    order = []
    for r in range(zn // 2, 0, -1):
        order.append(r)
        if r != zn - r:
            order.append(zn - r)

    def peer(r):
        return lax.rem(z + r, zn)

    def peer_id(zt):
        return {"dp": 2 * zt + c}

    barrier = pltpu.get_barrier_semaphore()
    for r in order:
        pl.semaphore_signal(barrier, inc=1, device_id=peer_id(peer(r)), device_id_type=MESH)
    pl.semaphore_signal(barrier, inc=1, device_id=sib, device_id_type=MESH)
    if pool == 4:
        pl.semaphore_signal(barrier, inc=1, device_id=xnei, device_id_type=MESH)
        pl.semaphore_signal(barrier, inc=1, device_id=ynei, device_id_type=MESH)

    sent = []

    def rcopy(src, dst, ss, rs, dev):
        sent.append(math.prod(src.shape) * src.dtype.itemsize)
        return pltpu.make_async_remote_copy(src_ref=src, dst_ref=dst, send_sem=ss, recv_sem=rs, device_id=dev, device_id_type=MESH)

    def wait_bytes(ref, sem):
        pltpu.make_async_copy(ref, ref, sem).wait()

    groups = {
        "q": (wq, 0, [(wq_hbm, 0)]),
        "kv": (wkv, 1, [(wk_hbm, 0), (wv_hbm, wkv.shape[-1] // 2)]),
        "o": (wo, 2, [(wo_hbm, 0)]),
        "g": (wg, 3, [(wg_hbm, 0)]),
        "u": (wu, 4, [(wu_hbm, 0)]),
    }

    full_o = {layers - 1} if pool == 4 else set()

    def skip(l, name):
        return l in full_o and name == "o"

    half_rows = wof.shape[3] // 2
    right, left = peer_id(peer(1)), peer_id(peer(zn - 1))

    def r_block(d, which=None):
        return wof.at[0, lax.rem(z + zn + d, zn), sub if which is None else which]

    def signed(d):
        return (d,) if d in (0, zh) else (d, -d)

    def of_own(l, d):
        if d == 0:
            wait_bytes(r_block(0), of_loc)
        elif d == zh:
            ring(l, zh)
        for b in signed(d):
            q = r_block(b)
            rcopy(q, q, send_sem, of_recv.at[0, d], xnei).start()
            rcopy(q, q, send_sem, of_recv.at[0, d], ynei).start()
            rcopy(q, q, send_sem, of_sib, sib).start()

    def of_relay(l, d):
        wait_bytes(wof.at[0, 0:len(signed(d)), 0:2], of_recv.at[0, d])
        for i, which, to in ((0, subx, ynei), (1, suby, xnei)):
            for b in signed(d):
                q = r_block(b, which)
                if (b > 0 if i == 0 else b <= 0):
                    rcopy(q, q, send_sem, of_recv.at[1, d], to).start()
                rcopy(q, q, send_sem, of_sib, sib).start()

    def of_last(l, d):
        wait_bytes(wof.at[0, 0:len(signed(d)), 0], of_recv.at[1, d])
        for b in signed(d):
            q = r_block(b, subd)
            rcopy(q, q, send_sem, of_sib, sib).start()

    def of_fin():
        wait_bytes(wof.at[0, :, 0:4], of_sib)

    def r_halves(d):
        blk = lax.rem(z + zn + d, zn)
        return wof.at[0, blk, sub, 0:half_rows], wof.at[0, blk, sub, half_rows:2 * half_rows]

    def ring(l, step):
        if step == 0:
            src = wo_hbm.at[l, pl.ds(pl.multiple_of(quarter * 2 * half_rows, 2 * half_rows), 2 * half_rows)]
            pltpu.make_async_copy(src, r_block(0), of_loc).start()
            rcopy(src, r_block(0), send_sem, ring_recv.at[0, 0], right).start()
            rcopy(src, r_block(0), send_sem, ring_recv.at[1, 0], left).start()
        elif step < zh - 1:
            for i, d, to in ((0, -step, right), (1, step, left)):
                wait_bytes(r_block(d), ring_recv.at[i, step - 1])
                rcopy(r_block(d), r_block(d), send_sem, ring_recv.at[i, step], to).start()
        elif step == zh - 1:
            for i, d, to in ((0, -step, right), (1, step, left)):
                wait_bytes(r_block(d), ring_recv.at[i, step - 1])
                h = r_halves(d)[i]
                rcopy(h, h, send_sem, ring_recv.at[i, step], to).start()
        else:
            for i in range(2):
                wait_bytes(r_halves(zh)[i], ring_recv.at[i, zh - 1])

    direct = {(0, "q"), (0, "kv")} if pool == 4 else set()

    def pieces(l, name, zt, diag=False):
        buf, gi, srcs = groups[name]
        quart, to = (3 - quarter, subd) if diag else (quarter, sub)
        rows = buf.shape[3]
        out = []
        for src, off in srcs:
            width = src.shape[2] // zn
            s = src.at[l, pl.ds(pl.multiple_of(quart * rows, rows), rows), pl.ds(pl.multiple_of(zt * width, 128), width)]
            d = buf.at[l, z, to, :, pl.ds(off, width)]
            out.append((s, d))
        return out, gi

    def w_local(l, name):
        ps, gi = pieces(l, name, z)
        for s, d in ps:
            pltpu.make_async_copy(s, d, z_recv.at[l, gi]).start()
        if (l, name) in direct:
            for s, d in pieces(l, name, z, True)[0]:
                pltpu.make_async_copy(s, d, diag_recv.at[l, gi]).start()

    def w_send(l, name):
        for r in order:
            zt = peer(r)
            ps, gi = pieces(l, name, zt)
            for s, d in ps:
                rcopy(s, d, send_sem, z_recv.at[l, gi], peer_id(zt)).start()

    def w_diag(l, name):
        if (l, name) in direct:
            for r in order:
                zt = peer(r)
                ps, gi = pieces(l, name, zt, True)
                for s, d in ps:
                    rcopy(s, d, send_sem, diag_recv.at[l, gi], peer_id(zt)).start()

    def w_s1(l, name):
        buf, gi, _ = groups[name]
        buf = buf.at[l]
        wait_bytes(buf.at[:, 0], z_recv.at[l, gi])
        q = buf.at[:, sub]
        if pool == 4:
            rcopy(q, q, send_sem, p_recv.at[l, gi, 0], xnei).start()
            rcopy(q, q, send_sem, p_recv.at[l, gi, 0], ynei).start()
        rcopy(q, q, send_sem, d_recv.at[l, gi], sib).start()

    def w_s2(l, name):
        if pool == 4:
            buf, gi, _ = groups[name]
            buf = buf.at[l]
            qx, qy = buf.at[:, subx], buf.at[:, suby]
            hx, hy = buf.at[0:zh, subx], buf.at[zh:zn, suby]
            wait_bytes(buf.at[:, 0:2], p_recv.at[l, gi, 0])
            if (l, name) not in direct:
                rcopy(hx, hx, send_sem, p_recv.at[l, gi, 1], ynei).start()
                rcopy(hy, hy, send_sem, p_recv.at[l, gi, 1], xnei).start()
            rcopy(qx, qx, send_sem, d_recv.at[l, gi], sib).start()
            rcopy(qy, qy, send_sem, d_recv.at[l, gi], sib).start()

    def w_s3(l, name):
        if pool == 4:
            buf, gi, _ = groups[name]
            buf = buf.at[l]
            q = buf.at[:, subd]
            if (l, name) in direct:
                wait_bytes(buf.at[:, 0], diag_recv.at[l, gi])
            else:
                wait_bytes(buf.at[:, subd], p_recv.at[l, gi, 1])
            rcopy(q, q, send_sem, d_recv.at[l, gi], sib).start()

    def w_fin(l, name):
        buf, gi, _ = groups[name]
        buf = buf.at[l]
        wait_bytes(buf.at[:, 0:pool], d_recv.at[l, gi])

    def spread(src_of, dst, l, ph):
        for r in order:
            zt = peer(r)
            rcopy(src_of(zt), dst, send_sem, a_recv.at[l, ph], peer_id(zt)).start()

    def arrived(buf, l, ph):
        if l is None:
            wait_bytes(buf.at[0:zn - 1], a_recv.at[layers - 1, ph])
        else:
            wait_bytes(buf.at[l, 0:zn - 1], a_recv.at[l, ph])

    end = layers - 1
    plan = {
        (0, "entry"): [(w_send, 0, "q"), (w_send, 0, "kv"), (w_diag, 0, "q"), (w_diag, 0, "kv")],
        (0, "x_wait"): [(w_s1, 0, "q"), (w_s1, 0, "kv"), (w_send, 0, "o"), (w_send, 0, "g"), (w_s2, 0, "q"), (w_s3, 0, "q"), (w_s2, 0, "kv"), (w_s3, 0, "kv")],
        (0, "qkv_sent"): [(w_send, 0, "u"), (ring, end, 0), (w_s1, 0, "o"), (of_own, end, 0), (w_s1, 0, "g")],
        (0, "o_sent"): [(w_s2, 0, "o"), (w_s1, 0, "u"), (ring, end, 1), (w_s3, 0, "o"), (w_s2, 0, "g"), (of_own, end, 1), (of_relay, end, 0)],
        (0, "x1_sent"): [(w_s2, 0, "u"), (ring, end, 2), (w_send, 1, "q"), (w_send, 1, "kv"), (w_s3, 0, "g"), (of_own, end, 2), (w_s3, 0, "u"), (of_relay, end, 1)],
        (0, "y_sent"): [(ring, end, 3), (w_send, 1, "g"), (w_s1, 1, "q"), (w_s1, 1, "kv"), (of_own, end, 3), (of_relay, end, 2)],
        (1, "x_sent"): [(w_s2, 1, "q"), (w_s2, 1, "kv"), (w_send, 1, "u"), (of_own, end, zh), (of_relay, end, 3), (w_s3, 1, "q"), (w_s3, 1, "kv"), (of_last, end, 0), (of_last, end, 1), (w_s1, 1, "g")],
        (1, "qkv_sent"): [(of_relay, end, zh), (w_s1, 1, "u"), (of_last, end, 2), (w_s2, 1, "g"), (of_last, end, 3), (of_last, end, zh)],
        (1, "att_done"): [(w_s2, 1, "u")],
        (1, "x1_sent"): [(w_s3, 1, "g"), (w_s3, 1, "u")],
    } if full_o else {
        (0, "entry"): [(w_send, 0, "q"), (w_send, 0, "kv"), (w_send, 0, "o"), (w_send, 0, "g"), (w_send, 0, "u")],
        (0, "x_wait"): [(w_s1, 0, "q"), (w_s1, 0, "kv")],
        (0, "qkv_sent"): [(w_s1, 0, "o"), (w_send, 1, "q"), (w_send, 1, "kv"), (w_send, 1, "o")],
        (0, "o_sent"): [(w_s1, 0, "g"), (w_s1, 0, "u")],
        (0, "x1_sent"): [(w_send, 1, "g"), (w_send, 1, "u"), (w_s1, 1, "q"), (w_s1, 1, "kv")],
        (0, "y_sent"): [(w_s1, 1, "o")],
        (1, "qkv_sent"): [(w_s1, 1, "g"), (w_s1, 1, "u")],
    }

    def background(l, point):
        for fn, wl, name in plan.get((l, point), ()):
            fn(wl, name)

    smalls = [(x_hbm, xg.at[0, z]), (pos_hbm, pos_ref), (an_hbm, an_ref), (qn_hbm, qn_ref), (kn_hbm, kn_ref), (mn_hbm, mn_ref)]
    small_copies = [pltpu.make_async_copy(s, d, in_sem.at[i]) for i, (s, d) in enumerate(smalls)]
    for cp in small_copies:
        cp.start()
    for l in range(layers):
        pltpu.make_async_copy(wd_hbm.at[l], wd.at[l, c], down_recv.at[l]).start()
        for name in ("q", "kv", "o", "g", "u"):
            if not skip(l, name):
                w_local(l, name)
        pltpu.make_async_copy(kc_hbm.at[l], kc.at[l], cache_sem.at[0]).start()
        pltpu.make_async_copy(vc_hbm.at[l], vc.at[l], cache_sem.at[1]).start()

    cols = kc.shape[2]
    lane = lax.broadcasted_iota(jnp.int32, (qh, cols), 1)
    row = lax.broadcasted_iota(jnp.int32, (qh, cols), 0)
    mine = lax.rem(lane, kh) == lax.shift_right_logical(row, 1)
    slot_ref[...] = jnp.where(mine, lax.div(lane, kh), cols)

    pl.semaphore_wait(barrier, zn + (2 if pool == 4 else 0))

    background(0, "entry")
    small_copies[0].wait()
    spread(lambda zt: xg.at[0, z], xg.at[0, z], 0, 0)
    for l in range(layers):
        rcopy(wd_hbm.at[l], wd.at[l, c], send_sem, down_recv.at[l], sib).start()

    for cp in small_copies[1:]:
        cp.wait()
    row_id = lax.broadcasted_iota(jnp.int32, (tok, HEAD_DIM), 0)
    lane_id = lax.broadcasted_iota(jnp.int32, (tok, HEAD_DIM), 1)
    pos = jnp.zeros((tok, HEAD_DIM), jnp.int32)
    for n in range(tok):
        pos = jnp.where(row_id == n, pos_ref[n], pos)
    half = HEAD_DIM // 2
    pair = jnp.where(lane_id >= half, lane_id - half, lane_id).astype(F32)
    inv_freq = jnp.exp(pair * (-2.0 * math.log(ROPE_THETA) / HEAD_DIM))
    ang = pos.astype(F32) * inv_freq
    cs[...] = jnp.cos(ang)
    sin_tab = jnp.sin(ang)
    sn[...] = jnp.where(lane_id >= half, sin_tab, -sin_tab)

    outs = []

    def head_norm(v, gain):
        v = rms(v, HEAD_DIM) * gain
        return (v * cs[...] + pltpu.roll(v, half, 1) * sn[...]).astype(BF16).astype(F32)

    def gathered_x(l):
        return xg[l].astype(F32).reshape(nq, dm)

    def attention(l):
        qg = qn_ref[l:l + 1, :].astype(F32)
        kg = kn_ref[l:l + 1, :].astype(F32)
        for h in range(qh):
            v = qkvi[l, h // 2, :, (h % 2) * HEAD_DIM:(h % 2 + 1) * HEAD_DIM].astype(F32)
            qs[pl.ds(h, tok, stride=qh), :] = head_norm(v, qg)
        for h in range(kh):
            k = head_norm(qkvi[l, h, :, 2 * HEAD_DIM:3 * HEAD_DIM].astype(F32), kg)
            v = qkvi[l, h, :, 3 * HEAD_DIM:4 * HEAD_DIM].astype(F32)
            for g in range(2):
                ks[pl.ds(2 * h + g, tok, stride=qh), :] = k
                vs[pl.ds(2 * h + g, tok, stride=qh), :] = v
            kro[pl.ds(h, tok, stride=kh), :] = k
            vro[pl.ds(h, tok, stride=kh), :] = v
        krow_ref[l] = kro[...].astype(BF16)
        vrow_ref[l] = vro[...].astype(BF16)
        outs.append(pltpu.make_async_copy(krow_ref.at[l], res_hbm.at[1 + 2 * l], out_sem))
        outs.append(pltpu.make_async_copy(vrow_ref.at[l], res_hbm.at[2 + 2 * l], out_sem))
        outs[-2].start()
        outs[-1].start()
        slot = slot_ref[...]
        scale = HEAD_DIM ** -0.5
        for n0 in range(0, tok, 8):
            seqs = range(n0, n0 + 8)
            rows = [slice(n * qh, (n + 1) * qh) for n in seqs]
            q = [qs[r, :] for r in rows]
            s = [lax.dot_general(a.astype(BF16), kc[l, n], (((1,), (1,)), ((), ())), preferred_element_type=F32) * scale for a, n in zip(q, seqs)]
            s_new = [jnp.sum(a * ks[r, :], axis=-1, keepdims=True) * scale for a, r in zip(q, rows)]
            s = [jnp.where(slot < pos_ref[n], a, NEG) for a, n in zip(s, seqs)]
            m = [jnp.maximum(jnp.max(a, axis=-1, keepdims=True), b) for a, b in zip(s, s_new)]
            e = [jnp.exp(a - b) for a, b in zip(s, m)]
            e_new = [jnp.exp(a - b) for a, b in zip(s_new, m)]
            inv = [1.0 / (jnp.sum(a, axis=-1, keepdims=True) + b) for a, b in zip(e, e_new)]
            p = [(a * b).astype(BF16) for a, b in zip(e, inv)]
            p_new = [(a * b).astype(BF16).astype(F32) for a, b in zip(e_new, inv)]
            for a, b, r, n in zip(p, p_new, rows, seqs):
                os_[r, :] = jnp.dot(a, vc[l, n], preferred_element_type=F32) + b * vs[r, :]
        for h in range(qh):
            og[l, z, :, h * HEAD_DIM:(h + 1) * HEAD_DIM] = os_[pl.ds(h, tok, stride=qh), :].astype(BF16)

    def own_rows(l):
        background(l, "att_done")
        of_fin()
        r = jnp.dot(og[l, z], wof[0].reshape(og.shape[-1], dm), preferred_element_type=F32)
        x1r[z] = (xg[l, z].astype(F32) + r).astype(BF16)
        spread(lambda zt: x1r.at[z], x1r.at[z], l, 3)
        background(l, "x1_sent")
        wait_bytes(wd.at[l], down_recv.at[l])
        w_fin(l, "g")
        w_fin(l, "u")
        arrived(x1r, None, 3)
        return x1r[...].astype(F32).reshape(nq, dm)

    def gathered_rows(l):
        spread(lambda zt: og.at[l, z], og.at[l, z], l, 2)
        background(l, "o_sent")
        w_fin(l, "o")
        arrived(og, l, 2)
        o_all = og[l].astype(F32).reshape(nq, og.shape[-1]).astype(BF16)
        r = jnp.dot(o_all, wo[l].reshape(og.shape[-1], ctile), preferred_element_type=F32)
        xc = xg[l, :, :, pl.ds(pl.multiple_of(z * ctile, ctile), ctile)].astype(F32).reshape(nq, ctile)
        x1g[l, z] = (xc + r).astype(BF16)
        spread(lambda zt: x1g.at[l, z], x1g.at[l, z], l, 3)
        background(l, "x1_sent")
        wait_bytes(wd.at[l], down_recv.at[l])
        w_fin(l, "g")
        w_fin(l, "u")
        arrived(x1g, l, 3)
        background(l, "x1_in")
        return jnp.concatenate([x1g[l, zz].astype(F32) for zz in range(zn)], axis=-1)

    for l in range(layers):
        last = l == layers - 1
        background(l, "x_wait")
        arrived(xg, l, 0)
        h = (rms(gathered_x(l), dm) * an_ref[l:l + 1, :].astype(F32)).astype(BF16)
        background(l, "x_in")
        w_fin(l, "q")
        w_fin(l, "kv")
        for name, lo in (("q", 0), ("kv", wq.shape[-1])):
            buf = groups[name][0]
            cols = buf.shape[-1]
            r = jnp.dot(h, buf[l].reshape(dm, cols), preferred_element_type=F32)
            qkvs[l, :, :, lo:lo + cols] = r.reshape(zn, tok, cols).astype(BF16)
        spread(lambda zt: qkvs.at[l, zt], qkvi.at[l, z], l, 1)
        qkvi[l, z] = qkvs[l, z]
        background(l, "qkv_sent")
        if l == 0:
            wait_bytes(kc, cache_sem.at[0])
            wait_bytes(vc, cache_sem.at[1])
        arrived(qkvi, l, 1)
        background(l, "qkv_in")
        attention(l)
        x1 = own_rows(l) if l in full_o else gathered_rows(l)
        x1f[...] = x1
        h2 = (rms(x1, dm) * mn_ref[l:l + 1, :].astype(F32)).astype(BF16)
        ffc = wg.shape[-1]
        g = jnp.dot(h2, wg[l].reshape(dm, ffc), preferred_element_type=F32)
        u = jnp.dot(h2, wu[l].reshape(dm, ffc), preferred_element_type=F32)
        a = (g * jax.nn.sigmoid(g) * u).astype(BF16)
        pr = jnp.dot(a, wd[l].reshape(ffc, dm), preferred_element_type=F32)
        pbuf[l] = pr.reshape(zn, tok, dm)
        spread(lambda zt: pbuf.at[l, zt], ybuf.at[l, z], l, 4)
        ybuf[l, z] = pbuf[l, z]
        background(l, "y_sent")
        arrived(ybuf, l, 4)
        total = ybuf[l, 0]
        for zz in range(1, zn):
            total = total + ybuf[l, zz]
        y = x1f[pl.ds(pl.multiple_of(z * tok, tok), tok), :] + total
        if last:
            y_ref[...] = jnp.concatenate([y[:, t * HEAD_DIM:(t + 1) * HEAD_DIM] for t in range(dm // HEAD_DIM)], axis=0).astype(BF16)
            outs.append(pltpu.make_async_copy(y_ref, res_hbm.at[0], out_sem))
            outs[-1].start()
        else:
            xg[l + 1, z] = y.astype(BF16)
            spread(lambda zt: xg.at[l + 1, z], xg.at[l + 1, z], l + 1, 0)
            background(l + 1, "x_sent")

    rows = sum(sent) // (res_hbm.shape[2] * 2)
    part_rows = math.gcd(rows, res_hbm.shape[1])
    wait_bytes(res_hbm.at[0:rows // part_rows, 0:part_rows], send_sem)
    wait_bytes(res_hbm.at[0:len(outs)], out_sem)


def place_rows(layers, tok, kh, pos_hbm, res_hbm, kin, vin, y_out, kout, vout, pos_ref, res, in_sem, bulk_sem, out_sem):
    small = [pltpu.make_async_copy(pos_hbm, pos_ref, in_sem.at[0]), pltpu.make_async_copy(res_hbm.at[0:1 + 2 * layers], res, in_sem.at[1])]
    for cp in small:
        cp.start()
    pairs = ((kin, kout), (vin, vout))
    for l in range(layers):
        for n in range(tok):
            for src, dst in pairs:
                pltpu.make_async_copy(src.at[l, n], dst.at[l, n], bulk_sem.at[l, n // 4]).start()
    for cp in small:
        cp.wait()
    for t in range(y_out.shape[1] // HEAD_DIM):
        pltpu.make_async_copy(res.at[0, pl.ds(t * tok, tok)], y_out.at[:, pl.ds(t * HEAD_DIM, HEAD_DIM)], out_sem).start()
    for l in range(layers):
        for n in range(tok):
            at = pl.ds(pl.multiple_of(pos_ref[n] * kh, kh), kh)
            if n % 4 == 0:
                done = kout.at[l]
                pltpu.make_async_copy(done, done, bulk_sem.at[l, n // 4]).wait()
            for i, (_, dst) in enumerate(pairs):
                pltpu.make_async_copy(res.at[1 + 2 * l + i, pl.ds(n * kh, kh)], dst.at[l, n, at], out_sem).start()
    pltpu.make_async_copy(res, res, out_sem).wait()


def solution(mesh):
    batch_axes = ("part", "dp")
    act_spec = P(batch_axes, None)
    cache_spec = P(None, batch_axes, None, None, None)
    mat_spec = P(None, "dp", None)
    gain_spec = P(None, None)
    in_specs = (act_spec, P(batch_axes), cache_spec, cache_spec, gain_spec, mat_spec, mat_spec, mat_spec, gain_spec, gain_spec, mat_spec, gain_spec, mat_spec, mat_spec, mat_spec)
    out_specs = (act_spec, cache_spec, cache_spec)
    zn = mesh.shape["dp"] // 2
    ny = math.isqrt(mesh.shape["part"])
    pool = 4 if ny * ny == mesh.shape["part"] and ny % 2 == 0 else 1

    def device_fn(x, positions, k_cache, v_cache, attn_norm, w_q, w_k, w_v, q_norm, k_norm, w_o, mlp_norm, w_gate, w_up, w_down):
        layers, tok, slots, kh, hd = k_cache.shape
        dm = x.shape[1]
        qw, kw, ff = w_q.shape[2], w_k.shape[2], w_gate.shape[2]
        qh = qw // hd
        nq = 2 * pool
        qkvc = (qw + 2 * kw) // zn
        cfg = dict(layers=layers, zn=zn, pool=pool, ny=ny, tok=tok, qh=qh, kh=kh)
        hb = pl.BlockSpec(memory_space=pltpu.HBM)
        dma = pltpu.SemaphoreType.DMA
        flat = (layers, tok, slots * kh, hd)
        scratch = [
            pltpu.VMEM((layers, zn, nq, w_q.shape[1] // pool, qw // zn), BF16),
            pltpu.VMEM((layers, zn, nq, w_k.shape[1] // pool, 2 * kw // zn), BF16),
            pltpu.VMEM((layers, zn, nq, w_o.shape[1] // pool, dm // zn), BF16),
            pltpu.VMEM((1, zn, nq, w_o.shape[1] // pool, dm), BF16),
            pltpu.VMEM((layers, zn, nq, w_gate.shape[1] // pool, ff // zn), BF16),
            pltpu.VMEM((layers, zn, nq, w_up.shape[1] // pool, ff // zn), BF16),
            pltpu.VMEM((layers, 2, w_down.shape[1], dm), BF16),
            pltpu.VMEM(flat, BF16),
            pltpu.VMEM(flat, BF16),
            pltpu.VMEM((layers, zn, tok, dm), BF16),
            pltpu.VMEM((layers, zn, tok, qkvc), BF16),
            pltpu.VMEM((layers, zn, tok, qkvc), BF16),
            pltpu.VMEM((layers, zn, tok, qw), BF16),
            pltpu.VMEM((layers, zn, zn * tok, dm // zn), BF16),
            pltpu.VMEM((zn, tok, dm), BF16),
            pltpu.VMEM((layers, zn, tok, dm), F32),
            pltpu.VMEM((layers, zn, tok, dm), F32),
            pltpu.VMEM((zn * tok, dm), F32),
            pltpu.VMEM((tok * qh, hd), F32),
            pltpu.VMEM((tok * qh, hd), F32),
            pltpu.VMEM((tok * qh, hd), F32),
            pltpu.VMEM((tok * qh, hd), F32),
            pltpu.VMEM((tok * kh, hd), F32),
            pltpu.VMEM((tok * kh, hd), F32),
            pltpu.VMEM((tok, hd), F32),
            pltpu.VMEM((tok, hd), F32),
            pltpu.VMEM((qh, slots * kh), jnp.int32),
            pltpu.SMEM((tok,), jnp.int32),
            pltpu.VMEM((layers, dm), BF16),
            pltpu.VMEM((layers, hd), BF16),
            pltpu.VMEM((layers, hd), BF16),
            pltpu.VMEM((layers, dm), BF16),
            pltpu.VMEM((tok * kh, hd), BF16),
            pltpu.VMEM((layers, tok * kh, hd), BF16),
            pltpu.VMEM((layers, tok * kh, hd), BF16),
            dma((layers, 5)), dma((layers, 5)), dma((layers, 5, 2)), dma((layers, 5)), dma((layers,)), dma, dma((2,)), dma((6,)), dma,
            dma((1, 2)), dma((2, zn // 2)), dma((2, zn // 2 + 1)), dma, dma,
        ]
        res = pl.pallas_call(
            functools.partial(decode_kernel, cfg),
            name="decode",
            out_shape=jax.ShapeDtypeStruct((RES_BLOCKS, tok * kh, hd), BF16),
            in_specs=[hb] * 15,
            out_specs=hb,
            scratch_shapes=scratch,
            compiler_params=pltpu.CompilerParams(collective_id=0, has_side_effects=True, vmem_limit_bytes=VMEM_LIMIT),
        )(positions, x, attn_norm, q_norm, k_norm, mlp_norm, w_q, w_k, w_v, w_o, w_gate, w_up, w_down, k_cache.reshape(flat), v_cache.reshape(flat))
        anys = pl.BlockSpec(memory_space=pl.ANY)
        rows = (1 + 2 * layers, tok * kh, hd)
        y, k_out, v_out = pl.pallas_call(
            functools.partial(place_rows, layers, tok, kh),
            name="place",
            out_shape=(jax.ShapeDtypeStruct((tok, dm), BF16), jax.ShapeDtypeStruct(flat, BF16), jax.ShapeDtypeStruct(flat, BF16)),
            in_specs=[anys] * 4,
            out_specs=(anys,) * 3,
            scratch_shapes=[pltpu.SMEM((tok,), jnp.int32), pltpu.VMEM(rows, BF16), dma((2,)), dma((layers, tok // 4)), dma],
            compiler_params=pltpu.CompilerParams(vmem_limit_bytes=PLACE_LIMIT),
        )(positions, res, k_cache.reshape(flat), v_cache.reshape(flat))
        k_out = k_out.reshape(k_cache.shape)
        v_out = v_out.reshape(v_cache.shape)
        return y, k_out, v_out

    return jax.shard_map(device_fn, mesh=mesh, in_specs=in_specs, out_specs=out_specs, check_vma=False)
```

```python
import functools
import math

import jax
import jax.numpy as jnp
from jax import lax
from jax.experimental import pallas as pl
from jax.experimental.pallas import tpu as pltpu
from jax.sharding import PartitionSpec as P

HEAD_DIM = 128
RMS_EPS = 1e-6
ROPE_THETA = 1000000.0
VMEM_LIMIT = 58400000
PLACE_LIMIT = 8 * 1024 * 1024
RES_BLOCKS = 4096

MESH = pl.DeviceIdType.MESH
F32 = jnp.float32
BF16 = jnp.bfloat16
NEG = float("-inf")


def rms(values, width):
    return values * lax.rsqrt(jnp.sum(values * values, axis=-1, keepdims=True) * (1.0 / width) + RMS_EPS)


def decode_kernel(cfg, pos_hbm, x_hbm, an_hbm, qn_hbm, kn_hbm, mn_hbm, wq_hbm, wk_hbm, wv_hbm, wo_hbm, wg_hbm, wu_hbm, wd_hbm, kc_hbm, vc_hbm,
                  res_hbm,
                  wq, wkv, wo, wof, wg, wu, wd, kc, vc, xg, qkvs, qkvi, og, x1g, x1r, pbuf, ybuf, x1f, qs, ks, vs, os_, kro, vro, cs, sn, slot_ref, pos_ref, an_ref, qn_ref, kn_ref, mn_ref, y_ref, krow_ref, vrow_ref,
                  z_recv, d_recv, p_recv, a_recv, down_recv, of_loc, cache_sem, in_sem, out_sem, diag_recv, ring_recv, of_recv, of_sib, send_sem):
    layers, zn, pool, tok = cfg["layers"], cfg["zn"], cfg["pool"], cfg["tok"]
    qh, kh, ny = cfg["qh"], cfg["kh"], cfg["ny"]
    dm = x_hbm.shape[1]
    nq = zn * tok
    ctile = dm // zn
    zh = zn // 2
    idx = lax.axis_index("dp")
    z, c = idx // 2, idx % 2
    part = lax.axis_index("part")
    sib = {"dp": 2 * z + (1 - c)}
    if pool == 4:
        px, py = (part // ny) % 2, (part % ny) % 2
        xnei = {"part": part + ny * (1 - 2 * px)}
        ynei = {"part": part + 1 - 2 * py}
    else:
        px, py = 0, 0
    quarter = px * 2 + py
    sub = c * pool + quarter
    subx = c * pool + (1 - px) * 2 + py
    suby = c * pool + px * 2 + 1 - py
    subd = c * pool + (1 - px) * 2 + 1 - py

    order = []
    for r in range(zn // 2, 0, -1):
        order.append(r)
        if r != zn - r:
            order.append(zn - r)

    def peer(r):
        return lax.rem(z + r, zn)

    def peer_id(zt):
        return {"dp": 2 * zt + c}

    barrier = pltpu.get_barrier_semaphore()
    for r in order:
        pl.semaphore_signal(barrier, inc=1, device_id=peer_id(peer(r)), device_id_type=MESH)
    pl.semaphore_signal(barrier, inc=1, device_id=sib, device_id_type=MESH)
    if pool == 4:
        pl.semaphore_signal(barrier, inc=1, device_id=xnei, device_id_type=MESH)
        pl.semaphore_signal(barrier, inc=1, device_id=ynei, device_id_type=MESH)

    sent = []

    def rcopy(src, dst, ss, rs, dev):
        sent.append(math.prod(src.shape) * src.dtype.itemsize)
        return pltpu.make_async_remote_copy(src_ref=src, dst_ref=dst, send_sem=ss, recv_sem=rs, device_id=dev, device_id_type=MESH)

    def wait_bytes(ref, sem):
        pltpu.make_async_copy(ref, ref, sem).wait()

    groups = {
        "q": (wq, 0, [(wq_hbm, 0)]),
        "kv": (wkv, 1, [(wk_hbm, 0), (wv_hbm, wkv.shape[-1] // 2)]),
        "o": (wo, 2, [(wo_hbm, 0)]),
        "g": (wg, 3, [(wg_hbm, 0)]),
        "u": (wu, 4, [(wu_hbm, 0)]),
    }

    full_o = {layers - 1} if pool == 4 else set()

    def skip(l, name):
        return l in full_o and name == "o"

    half_rows = wof.shape[3] // 2
    right, left = peer_id(peer(1)), peer_id(peer(zn - 1))

    def r_block(d, which=None):
        return wof.at[0, lax.rem(z + zn + d, zn), sub if which is None else which]

    def signed(d):
        return (d,) if d in (0, zh) else (d, -d)

    def of_own(l, d):
        if d == 0:
            wait_bytes(r_block(0), of_loc)
        elif d == zh:
            ring(l, zh)
        for b in signed(d):
            q = r_block(b)
            rcopy(q, q, send_sem, of_recv.at[0, d], xnei).start()
            rcopy(q, q, send_sem, of_recv.at[0, d], ynei).start()
            rcopy(q, q, send_sem, of_sib, sib).start()

    def of_relay(l, d):
        wait_bytes(wof.at[0, 0:len(signed(d)), 0:2], of_recv.at[0, d])
        for i, which, to in ((0, subx, ynei), (1, suby, xnei)):
            for b in signed(d):
                q = r_block(b, which)
                if (b > 0 if i == 0 else b <= 0):
                    rcopy(q, q, send_sem, of_recv.at[1, d], to).start()
                rcopy(q, q, send_sem, of_sib, sib).start()

    def of_last(l, d):
        wait_bytes(wof.at[0, 0:len(signed(d)), 0], of_recv.at[1, d])
        for b in signed(d):
            q = r_block(b, subd)
            rcopy(q, q, send_sem, of_sib, sib).start()

    def of_fin():
        wait_bytes(wof.at[0, :, 0:4], of_sib)

    def r_halves(d):
        blk = lax.rem(z + zn + d, zn)
        return wof.at[0, blk, sub, 0:half_rows], wof.at[0, blk, sub, half_rows:2 * half_rows]

    def ring(l, step):
        if step == 0:
            src = wo_hbm.at[l, pl.ds(pl.multiple_of(quarter * 2 * half_rows, 2 * half_rows), 2 * half_rows)]
            pltpu.make_async_copy(src, r_block(0), of_loc).start()
            rcopy(src, r_block(0), send_sem, ring_recv.at[0, 0], right).start()
            rcopy(src, r_block(0), send_sem, ring_recv.at[1, 0], left).start()
        elif step < zh - 1:
            for i, d, to in ((0, -step, right), (1, step, left)):
                wait_bytes(r_block(d), ring_recv.at[i, step - 1])
                rcopy(r_block(d), r_block(d), send_sem, ring_recv.at[i, step], to).start()
        elif step == zh - 1:
            for i, d, to in ((0, -step, right), (1, step, left)):
                wait_bytes(r_block(d), ring_recv.at[i, step - 1])
                h = r_halves(d)[i]
                rcopy(h, h, send_sem, ring_recv.at[i, step], to).start()
        else:
            for i in range(2):
                wait_bytes(r_halves(zh)[i], ring_recv.at[i, zh - 1])

    direct = {(0, "q"), (0, "kv")} if pool == 4 else set()

    def pieces(l, name, zt, diag=False):
        buf, gi, srcs = groups[name]
        quart, to = (3 - quarter, subd) if diag else (quarter, sub)
        rows = buf.shape[3]
        out = []
        for src, off in srcs:
            width = src.shape[2] // zn
            s = src.at[l, pl.ds(pl.multiple_of(quart * rows, rows), rows), pl.ds(pl.multiple_of(zt * width, 128), width)]
            d = buf.at[l, z, to, :, pl.ds(off, width)]
            out.append((s, d))
        return out, gi

    def w_local(l, name):
        ps, gi = pieces(l, name, z)
        for s, d in ps:
            pltpu.make_async_copy(s, d, z_recv.at[l, gi]).start()
        if (l, name) in direct:
            for s, d in pieces(l, name, z, True)[0]:
                pltpu.make_async_copy(s, d, diag_recv.at[l, gi]).start()

    def w_send(l, name):
        for r in order:
            zt = peer(r)
            ps, gi = pieces(l, name, zt)
            for s, d in ps:
                rcopy(s, d, send_sem, z_recv.at[l, gi], peer_id(zt)).start()

    def w_diag(l, name):
        if (l, name) in direct:
            for r in order:
                zt = peer(r)
                ps, gi = pieces(l, name, zt, True)
                for s, d in ps:
                    rcopy(s, d, send_sem, diag_recv.at[l, gi], peer_id(zt)).start()

    def w_s1(l, name):
        buf, gi, _ = groups[name]
        buf = buf.at[l]
        wait_bytes(buf.at[:, 0], z_recv.at[l, gi])
        q = buf.at[:, sub]
        if pool == 4:
            rcopy(q, q, send_sem, p_recv.at[l, gi, 0], xnei).start()
            rcopy(q, q, send_sem, p_recv.at[l, gi, 0], ynei).start()
        rcopy(q, q, send_sem, d_recv.at[l, gi], sib).start()

    def w_s2(l, name):
        if pool == 4:
            buf, gi, _ = groups[name]
            buf = buf.at[l]
            qx, qy = buf.at[:, subx], buf.at[:, suby]
            hx, hy = buf.at[0:zh, subx], buf.at[zh:zn, suby]
            wait_bytes(buf.at[:, 0:2], p_recv.at[l, gi, 0])
            if (l, name) not in direct:
                rcopy(hx, hx, send_sem, p_recv.at[l, gi, 1], ynei).start()
                rcopy(hy, hy, send_sem, p_recv.at[l, gi, 1], xnei).start()
            rcopy(qx, qx, send_sem, d_recv.at[l, gi], sib).start()
            rcopy(qy, qy, send_sem, d_recv.at[l, gi], sib).start()

    def w_s3(l, name):
        if pool == 4:
            buf, gi, _ = groups[name]
            buf = buf.at[l]
            q = buf.at[:, subd]
            if (l, name) in direct:
                wait_bytes(buf.at[:, 0], diag_recv.at[l, gi])
            else:
                wait_bytes(buf.at[:, subd], p_recv.at[l, gi, 1])
            rcopy(q, q, send_sem, d_recv.at[l, gi], sib).start()

    def w_fin(l, name):
        buf, gi, _ = groups[name]
        buf = buf.at[l]
        wait_bytes(buf.at[:, 0:pool], d_recv.at[l, gi])

    def spread(src_of, dst, l, ph):
        for r in order:
            zt = peer(r)
            rcopy(src_of(zt), dst, send_sem, a_recv.at[l, ph], peer_id(zt)).start()

    def arrived(buf, l, ph):
        if l is None:
            wait_bytes(buf.at[0:zn - 1], a_recv.at[layers - 1, ph])
        else:
            wait_bytes(buf.at[l, 0:zn - 1], a_recv.at[l, ph])

    end = layers - 1
    plan = {
        (0, "entry"): [(w_send, 0, "q"), (w_send, 0, "kv"), (w_diag, 0, "q"), (w_diag, 0, "kv")],
        (0, "x_wait"): [(w_s1, 0, "q"), (w_s1, 0, "kv"), (w_send, 0, "o"), (w_send, 0, "g"), (w_s2, 0, "q"), (w_s3, 0, "q"), (w_s2, 0, "kv"), (w_s3, 0, "kv")],
        (0, "qkv_sent"): [(w_send, 0, "u"), (ring, end, 0), (w_s1, 0, "o"), (of_own, end, 0), (w_s1, 0, "g")],
        (0, "o_sent"): [(w_s2, 0, "o"), (w_s1, 0, "u"), (ring, end, 1), (w_s3, 0, "o"), (w_s2, 0, "g"), (of_own, end, 1), (of_relay, end, 0)],
        (0, "x1_sent"): [(w_s2, 0, "u"), (ring, end, 2), (w_send, 1, "q"), (w_send, 1, "kv"), (w_s3, 0, "g"), (of_own, end, 2), (w_s3, 0, "u"), (of_relay, end, 1)],
        (0, "y_sent"): [(ring, end, 3), (w_send, 1, "g"), (w_s1, 1, "q"), (w_s1, 1, "kv"), (of_own, end, 3), (of_relay, end, 2)],
        (1, "x_sent"): [(w_s2, 1, "q"), (w_s2, 1, "kv"), (w_send, 1, "u"), (of_own, end, zh), (of_relay, end, 3), (w_s3, 1, "q"), (w_s3, 1, "kv"), (of_last, end, 0), (of_last, end, 1), (w_s1, 1, "g")],
        (1, "qkv_sent"): [(of_relay, end, zh), (w_s1, 1, "u"), (of_last, end, 2), (w_s2, 1, "g"), (of_last, end, 3), (of_last, end, zh)],
        (1, "att_done"): [(w_s2, 1, "u")],
        (1, "x1_sent"): [(w_s3, 1, "g"), (w_s3, 1, "u")],
    } if full_o else {
        (0, "entry"): [(w_send, 0, "q"), (w_send, 0, "kv"), (w_send, 0, "o"), (w_send, 0, "g"), (w_send, 0, "u")],
        (0, "x_wait"): [(w_s1, 0, "q"), (w_s1, 0, "kv")],
        (0, "qkv_sent"): [(w_s1, 0, "o"), (w_send, 1, "q"), (w_send, 1, "kv"), (w_send, 1, "o")],
        (0, "o_sent"): [(w_s1, 0, "g"), (w_s1, 0, "u")],
        (0, "x1_sent"): [(w_send, 1, "g"), (w_send, 1, "u"), (w_s1, 1, "q"), (w_s1, 1, "kv")],
        (0, "y_sent"): [(w_s1, 1, "o")],
        (1, "qkv_sent"): [(w_s1, 1, "g"), (w_s1, 1, "u")],
    }

    def background(l, point):
        for fn, wl, name in plan.get((l, point), ()):
            fn(wl, name)

    smalls = [(x_hbm, xg.at[0, z]), (pos_hbm, pos_ref), (an_hbm, an_ref), (qn_hbm, qn_ref), (kn_hbm, kn_ref), (mn_hbm, mn_ref)]
    small_copies = [pltpu.make_async_copy(s, d, in_sem.at[i]) for i, (s, d) in enumerate(smalls)]
    for cp in small_copies:
        cp.start()
    for l in range(layers):
        pltpu.make_async_copy(wd_hbm.at[l], wd.at[l, c], down_recv.at[l]).start()
        for name in ("q", "kv", "o", "g", "u"):
            if not skip(l, name):
                w_local(l, name)
        pltpu.make_async_copy(kc_hbm.at[l], kc.at[l], cache_sem.at[0]).start()
        pltpu.make_async_copy(vc_hbm.at[l], vc.at[l], cache_sem.at[1]).start()

    cols = kc.shape[2]
    lane = lax.broadcasted_iota(jnp.int32, (qh, cols), 1)
    row = lax.broadcasted_iota(jnp.int32, (qh, cols), 0)
    mine = lax.rem(lane, kh) == lax.shift_right_logical(row, 1)
    slot_ref[...] = jnp.where(mine, lax.div(lane, kh), cols)

    pl.semaphore_wait(barrier, zn + (2 if pool == 4 else 0))

    background(0, "entry")
    small_copies[0].wait()
    spread(lambda zt: xg.at[0, z], xg.at[0, z], 0, 0)
    for l in range(layers):
        rcopy(wd_hbm.at[l], wd.at[l, c], send_sem, down_recv.at[l], sib).start()

    for cp in small_copies[1:]:
        cp.wait()
    row_id = lax.broadcasted_iota(jnp.int32, (tok, HEAD_DIM), 0)
    lane_id = lax.broadcasted_iota(jnp.int32, (tok, HEAD_DIM), 1)
    pos = jnp.zeros((tok, HEAD_DIM), jnp.int32)
    for n in range(tok):
        pos = jnp.where(row_id == n, pos_ref[n], pos)
    half = HEAD_DIM // 2
    pair = jnp.where(lane_id >= half, lane_id - half, lane_id).astype(F32)
    inv_freq = jnp.exp(pair * (-2.0 * math.log(ROPE_THETA) / HEAD_DIM))
    ang = pos.astype(F32) * inv_freq
    cs[...] = jnp.cos(ang)
    sin_tab = jnp.sin(ang)
    sn[...] = jnp.where(lane_id >= half, sin_tab, -sin_tab)

    outs = []

    def head_norm(v, gain):
        v = rms(v, HEAD_DIM) * gain
        return (v * cs[...] + pltpu.roll(v, half, 1) * sn[...]).astype(BF16).astype(F32)

    def gathered_x(l):
        return xg[l].astype(F32).reshape(nq, dm)

    def attention(l):
        qg = qn_ref[l:l + 1, :].astype(F32)
        kg = kn_ref[l:l + 1, :].astype(F32)
        for h in range(qh):
            v = qkvi[l, h // 2, :, (h % 2) * HEAD_DIM:(h % 2 + 1) * HEAD_DIM].astype(F32)
            qs[pl.ds(h, tok, stride=qh), :] = head_norm(v, qg)
        for h in range(kh):
            k = head_norm(qkvi[l, h, :, 2 * HEAD_DIM:3 * HEAD_DIM].astype(F32), kg)
            v = qkvi[l, h, :, 3 * HEAD_DIM:4 * HEAD_DIM].astype(F32)
            for g in range(2):
                ks[pl.ds(2 * h + g, tok, stride=qh), :] = k
                vs[pl.ds(2 * h + g, tok, stride=qh), :] = v
            kro[pl.ds(h, tok, stride=kh), :] = k
            vro[pl.ds(h, tok, stride=kh), :] = v
        slot = slot_ref[...]
        scale = HEAD_DIM ** -0.5
        for n0 in range(0, tok, 8):
            seqs = range(n0, n0 + 8)
            rows = [slice(n * qh, (n + 1) * qh) for n in seqs]
            q = [qs[r, :] for r in rows]
            s = [lax.dot_general(a.astype(BF16), kc[l, n], (((1,), (1,)), ((), ())), preferred_element_type=F32) * scale for a, n in zip(q, seqs)]
            s_new = [jnp.sum(a * ks[r, :], axis=-1, keepdims=True) * scale for a, r in zip(q, rows)]
            s = [jnp.where(slot < pos_ref[n], a, NEG) for a, n in zip(s, seqs)]
            m = [jnp.maximum(jnp.max(a, axis=-1, keepdims=True), b) for a, b in zip(s, s_new)]
            e = [jnp.exp(a - b) for a, b in zip(s, m)]
            e_new = [jnp.exp(a - b) for a, b in zip(s_new, m)]
            inv = [1.0 / (jnp.sum(a, axis=-1, keepdims=True) + b) for a, b in zip(e, e_new)]
            p = [(a * b).astype(BF16) for a, b in zip(e, inv)]
            p_new = [(a * b).astype(BF16).astype(F32) for a, b in zip(e_new, inv)]
            for a, b, r, n in zip(p, p_new, rows, seqs):
                os_[r, :] = jnp.dot(a, vc[l, n], preferred_element_type=F32) + b * vs[r, :]
        for h in range(qh):
            og[l, z, :, h * HEAD_DIM:(h + 1) * HEAD_DIM] = os_[pl.ds(h, tok, stride=qh), :].astype(BF16)

    def flush_rows(l):
        krow_ref[l] = kro[...].astype(BF16)
        vrow_ref[l] = vro[...].astype(BF16)
        outs.append(pltpu.make_async_copy(krow_ref.at[l], res_hbm.at[1 + 2 * l], out_sem))
        outs.append(pltpu.make_async_copy(vrow_ref.at[l], res_hbm.at[2 + 2 * l], out_sem))
        outs[-2].start()
        outs[-1].start()

    def own_rows(l):
        background(l, "att_done")
        of_fin()
        r = jnp.dot(og[l, z], wof[0].reshape(og.shape[-1], dm), preferred_element_type=F32)
        x1r[z] = (xg[l, z].astype(F32) + r).astype(BF16)
        spread(lambda zt: x1r.at[z], x1r.at[z], l, 3)
        flush_rows(l)
        background(l, "x1_sent")
        wait_bytes(wd.at[l], down_recv.at[l])
        w_fin(l, "g")
        w_fin(l, "u")
        arrived(x1r, None, 3)
        return x1r[...].astype(F32).reshape(nq, dm)

    def gathered_rows(l):
        spread(lambda zt: og.at[l, z], og.at[l, z], l, 2)
        flush_rows(l)
        background(l, "o_sent")
        w_fin(l, "o")
        arrived(og, l, 2)
        o_all = og[l].astype(F32).reshape(nq, og.shape[-1]).astype(BF16)
        r = jnp.dot(o_all, wo[l].reshape(og.shape[-1], ctile), preferred_element_type=F32)
        xc = xg[l, :, :, pl.ds(pl.multiple_of(z * ctile, ctile), ctile)].astype(F32).reshape(nq, ctile)
        x1g[l, z] = (xc + r).astype(BF16)
        spread(lambda zt: x1g.at[l, z], x1g.at[l, z], l, 3)
        background(l, "x1_sent")
        wait_bytes(wd.at[l], down_recv.at[l])
        w_fin(l, "g")
        w_fin(l, "u")
        arrived(x1g, l, 3)
        background(l, "x1_in")
        return jnp.concatenate([x1g[l, zz].astype(F32) for zz in range(zn)], axis=-1)

    for l in range(layers):
        last = l == layers - 1
        background(l, "x_wait")
        arrived(xg, l, 0)
        h = (rms(gathered_x(l), dm) * an_ref[l:l + 1, :].astype(F32)).astype(BF16)
        background(l, "x_in")
        w_fin(l, "q")
        w_fin(l, "kv")
        for name, lo in (("q", 0), ("kv", wq.shape[-1])):
            buf = groups[name][0]
            cols = buf.shape[-1]
            r = jnp.dot(h, buf[l].reshape(dm, cols), preferred_element_type=F32)
            qkvs[l, :, :, lo:lo + cols] = r.reshape(zn, tok, cols).astype(BF16)
        spread(lambda zt: qkvs.at[l, zt], qkvi.at[l, z], l, 1)
        qkvi[l, z] = qkvs[l, z]
        background(l, "qkv_sent")
        if l == 0:
            wait_bytes(kc, cache_sem.at[0])
            wait_bytes(vc, cache_sem.at[1])
        arrived(qkvi, l, 1)
        background(l, "qkv_in")
        attention(l)
        x1 = own_rows(l) if l in full_o else gathered_rows(l)
        x1f[...] = x1
        h2 = (rms(x1, dm) * mn_ref[l:l + 1, :].astype(F32)).astype(BF16)
        ffc = wg.shape[-1]
        g = jnp.dot(h2, wg[l].reshape(dm, ffc), preferred_element_type=F32)
        u = jnp.dot(h2, wu[l].reshape(dm, ffc), preferred_element_type=F32)
        a = (g * jax.nn.sigmoid(g) * u).astype(BF16)
        pr = jnp.dot(a, wd[l].reshape(ffc, dm), preferred_element_type=F32)
        pbuf[l] = pr.reshape(zn, tok, dm)
        spread(lambda zt: pbuf.at[l, zt], ybuf.at[l, z], l, 4)
        ybuf[l, z] = pbuf[l, z]
        background(l, "y_sent")
        arrived(ybuf, l, 4)
        total = ybuf[l, 0]
        for zz in range(1, zn):
            total = total + ybuf[l, zz]
        y = x1f[pl.ds(pl.multiple_of(z * tok, tok), tok), :] + total
        if last:
            y_ref[...] = jnp.concatenate([y[:, t * HEAD_DIM:(t + 1) * HEAD_DIM] for t in range(dm // HEAD_DIM)], axis=0).astype(BF16)
            outs.append(pltpu.make_async_copy(y_ref, res_hbm.at[0], out_sem))
            outs[-1].start()
        else:
            xg[l + 1, z] = y.astype(BF16)
            spread(lambda zt: xg.at[l + 1, z], xg.at[l + 1, z], l + 1, 0)
            background(l + 1, "x_sent")

    rows = sum(sent) // (res_hbm.shape[2] * 2)
    part_rows = math.gcd(rows, res_hbm.shape[1])
    wait_bytes(res_hbm.at[0:rows // part_rows, 0:part_rows], send_sem)
    wait_bytes(res_hbm.at[0:len(outs)], out_sem)


def place_rows(layers, tok, kh, pos_hbm, res_hbm, kin, vin, y_out, kout, vout, pos_ref, res, in_sem, bulk_sem, out_sem):
    small = [pltpu.make_async_copy(pos_hbm, pos_ref, in_sem.at[0]), pltpu.make_async_copy(res_hbm.at[0:1 + 2 * layers], res, in_sem.at[1])]
    for cp in small:
        cp.start()
    pairs = ((kin, kout), (vin, vout))
    for l in range(layers):
        for n in range(tok):
            for src, dst in pairs:
                pltpu.make_async_copy(src.at[l, n], dst.at[l, n], bulk_sem.at[l, n // 4]).start()
    for cp in small:
        cp.wait()
    for t in range(y_out.shape[1] // HEAD_DIM):
        pltpu.make_async_copy(res.at[0, pl.ds(t * tok, tok)], y_out.at[:, pl.ds(t * HEAD_DIM, HEAD_DIM)], out_sem).start()
    for l in range(layers):
        for n in range(tok):
            at = pl.ds(pl.multiple_of(pos_ref[n] * kh, kh), kh)
            if n % 4 == 0:
                done = kout.at[l]
                pltpu.make_async_copy(done, done, bulk_sem.at[l, n // 4]).wait()
            for i, (_, dst) in enumerate(pairs):
                pltpu.make_async_copy(res.at[1 + 2 * l + i, pl.ds(n * kh, kh)], dst.at[l, n, at], out_sem).start()
    pltpu.make_async_copy(res, res, out_sem).wait()


def solution(mesh):
    batch_axes = ("part", "dp")
    act_spec = P(batch_axes, None)
    cache_spec = P(None, batch_axes, None, None, None)
    mat_spec = P(None, "dp", None)
    gain_spec = P(None, None)
    in_specs = (act_spec, P(batch_axes), cache_spec, cache_spec, gain_spec, mat_spec, mat_spec, mat_spec, gain_spec, gain_spec, mat_spec, gain_spec, mat_spec, mat_spec, mat_spec)
    out_specs = (act_spec, cache_spec, cache_spec)
    zn = mesh.shape["dp"] // 2
    ny = math.isqrt(mesh.shape["part"])
    pool = 4 if ny * ny == mesh.shape["part"] and ny % 2 == 0 else 1

    def device_fn(x, positions, k_cache, v_cache, attn_norm, w_q, w_k, w_v, q_norm, k_norm, w_o, mlp_norm, w_gate, w_up, w_down):
        layers, tok, slots, kh, hd = k_cache.shape
        dm = x.shape[1]
        qw, kw, ff = w_q.shape[2], w_k.shape[2], w_gate.shape[2]
        qh = qw // hd
        nq = 2 * pool
        qkvc = (qw + 2 * kw) // zn
        cfg = dict(layers=layers, zn=zn, pool=pool, ny=ny, tok=tok, qh=qh, kh=kh)
        hb = pl.BlockSpec(memory_space=pltpu.HBM)
        dma = pltpu.SemaphoreType.DMA
        flat = (layers, tok, slots * kh, hd)
        scratch = [
            pltpu.VMEM((layers, zn, nq, w_q.shape[1] // pool, qw // zn), BF16),
            pltpu.VMEM((layers, zn, nq, w_k.shape[1] // pool, 2 * kw // zn), BF16),
            pltpu.VMEM((layers, zn, nq, w_o.shape[1] // pool, dm // zn), BF16),
            pltpu.VMEM((1, zn, nq, w_o.shape[1] // pool, dm), BF16),
            pltpu.VMEM((layers, zn, nq, w_gate.shape[1] // pool, ff // zn), BF16),
            pltpu.VMEM((layers, zn, nq, w_up.shape[1] // pool, ff // zn), BF16),
            pltpu.VMEM((layers, 2, w_down.shape[1], dm), BF16),
            pltpu.VMEM(flat, BF16),
            pltpu.VMEM(flat, BF16),
            pltpu.VMEM((layers, zn, tok, dm), BF16),
            pltpu.VMEM((layers, zn, tok, qkvc), BF16),
            pltpu.VMEM((layers, zn, tok, qkvc), BF16),
            pltpu.VMEM((layers, zn, tok, qw), BF16),
            pltpu.VMEM((layers, zn, zn * tok, dm // zn), BF16),
            pltpu.VMEM((zn, tok, dm), BF16),
            pltpu.VMEM((layers, zn, tok, dm), F32),
            pltpu.VMEM((layers, zn, tok, dm), F32),
            pltpu.VMEM((zn * tok, dm), F32),
            pltpu.VMEM((tok * qh, hd), F32),
            pltpu.VMEM((tok * qh, hd), F32),
            pltpu.VMEM((tok * qh, hd), F32),
            pltpu.VMEM((tok * qh, hd), F32),
            pltpu.VMEM((tok * kh, hd), F32),
            pltpu.VMEM((tok * kh, hd), F32),
            pltpu.VMEM((tok, hd), F32),
            pltpu.VMEM((tok, hd), F32),
            pltpu.VMEM((qh, slots * kh), jnp.int32),
            pltpu.SMEM((tok,), jnp.int32),
            pltpu.VMEM((layers, dm), BF16),
            pltpu.VMEM((layers, hd), BF16),
            pltpu.VMEM((layers, hd), BF16),
            pltpu.VMEM((layers, dm), BF16),
            pltpu.VMEM((tok * kh, hd), BF16),
            pltpu.VMEM((layers, tok * kh, hd), BF16),
            pltpu.VMEM((layers, tok * kh, hd), BF16),
            dma((layers, 5)), dma((layers, 5)), dma((layers, 5, 2)), dma((layers, 5)), dma((layers,)), dma, dma((2,)), dma((6,)), dma,
            dma((1, 2)), dma((2, zn // 2)), dma((2, zn // 2 + 1)), dma, dma,
        ]
        res = pl.pallas_call(
            functools.partial(decode_kernel, cfg),
            name="decode",
            out_shape=jax.ShapeDtypeStruct((RES_BLOCKS, tok * kh, hd), BF16),
            in_specs=[hb] * 15,
            out_specs=hb,
            scratch_shapes=scratch,
            compiler_params=pltpu.CompilerParams(collective_id=0, has_side_effects=True, vmem_limit_bytes=VMEM_LIMIT),
        )(positions, x, attn_norm, q_norm, k_norm, mlp_norm, w_q, w_k, w_v, w_o, w_gate, w_up, w_down, k_cache.reshape(flat), v_cache.reshape(flat))
        anys = pl.BlockSpec(memory_space=pl.ANY)
        rows = (1 + 2 * layers, tok * kh, hd)
        y, k_out, v_out = pl.pallas_call(
            functools.partial(place_rows, layers, tok, kh),
            name="place",
            out_shape=(jax.ShapeDtypeStruct((tok, dm), BF16), jax.ShapeDtypeStruct(flat, BF16), jax.ShapeDtypeStruct(flat, BF16)),
            in_specs=[anys] * 4,
            out_specs=(anys,) * 3,
            scratch_shapes=[pltpu.SMEM((tok,), jnp.int32), pltpu.VMEM(rows, BF16), dma((2,)), dma((layers, tok // 4)), dma],
            compiler_params=pltpu.CompilerParams(vmem_limit_bytes=PLACE_LIMIT),
        )(positions, res, k_cache.reshape(flat), v_cache.reshape(flat))
        k_out = k_out.reshape(k_cache.shape)
        v_out = v_out.reshape(v_cache.shape)
        return y, k_out, v_out

    return jax.shard_map(device_fn, mesh=mesh, in_specs=in_specs, out_specs=out_specs, check_vma=False)
```
